8 devices in a mesh: data: 2 (over z, y), stage: 4 (over x, core).
Axes of the slice: x: 2, y: 2, z: 1, core: 2. Of those that a mesh axis runs over, the one named last changes fastest.
Arguments:
- inputs: bfloat16 [128, 64, 2048], P('data'), parts along dimension 0
- targets: bfloat16 [128, 64, 2048], P('data'), parts along dimension 0
- lengths: int32 [128], P('data'), parts along dimension 0
- w_in: bfloat16 [4, 2048, 8192], P('stage')
- w_rec: bfloat16 [4, 2048, 8192], P('stage')
- gate_bias: float32 [4, 8192], P('stage')
- h_init: float32 [4, 128, 2048], P('stage', 'data'), parts along dimension 1
- c_init: float32 [4, 128, 2048], P('stage', 'data'), parts along dimension 1
Outputs:
- output 1: float32 [2], P('data'), parts along dimension 0
- output 2: float32 [8, 2048, 8192], P(('data', 'stage')), parts along dimension 0
- output 3: float32 [8, 2048, 8192], P(('data', 'stage')), parts along dimension 0
- output 4: float32 [8, 8192], P(('data', 'stage')), parts along dimension 0
- output 5: float32 [4, 128, 2048], P('stage', 'data'), parts along dimension 1
- output 6: float32 [4, 128, 2048], P('stage', 'data'), parts along dimension 1
There are 2 independent parts. The reference program is written for one: setup_inputs(seed, part) draws one part's arguments, and reference() takes and returns one part's arrays. A program takes and returns all parts, laid end to end along the dimension named above; an argument that names none is the same for every part.
All inputs are finite; a program needn't handle non-finite values.
Results may differ from the reference program's by a relative error of at most 0.00682419.
Values are sent between devices in bfloat16 or wider.
A program may use at most 1 GiB of HBM per device.

```python
import jax
import jax.numpy as jnp
from jax import lax

HIDDEN = 2048
LAYERS = 4
BATCH_ROWS = 64
TIME_STEPS = 64


def draw_lengths(key_len):
    shortest = TIME_STEPS // 4
    middle = jax.random.randint(key_len, (BATCH_ROWS - 2,), shortest, TIME_STEPS + 1, jnp.int32)
    raw_len = jnp.concatenate([jnp.array([TIME_STEPS, shortest], jnp.int32), middle])
    return -jnp.sort(-raw_len)


def setup_inputs(seed: int = 0, part: int = 0) -> dict:
    shared_keys = jax.random.split(jax.random.key(seed), 3)
    part_keys = jax.random.split(jax.random.fold_in(jax.random.key(seed + 1), part), 5)
    w_scale = HIDDEN ** -0.5
    w_in = (jax.random.normal(shared_keys[0], (LAYERS, HIDDEN, 4 * HIDDEN), jnp.float32) * w_scale).astype(jnp.bfloat16)
    w_rec = (jax.random.normal(shared_keys[1], (LAYERS, HIDDEN, 4 * HIDDEN), jnp.float32) * w_scale).astype(jnp.bfloat16)
    forget_shift = jnp.repeat(jnp.array([0.0, 1.0, 0.0, 0.0], jnp.float32), HIDDEN)
    gate_bias = 0.5 * jax.random.normal(shared_keys[2], (LAYERS, 4 * HIDDEN), jnp.float32) + forget_shift
    inputs = jax.random.normal(part_keys[0], (BATCH_ROWS, TIME_STEPS, HIDDEN), jnp.float32).astype(jnp.bfloat16)
    targets = (0.5 * jax.random.normal(part_keys[1], (BATCH_ROWS, TIME_STEPS, HIDDEN), jnp.float32)).astype(jnp.bfloat16)
    h_init = 0.5 * jax.random.normal(part_keys[2], (LAYERS, BATCH_ROWS, HIDDEN), jnp.float32)
    c_init = jax.random.normal(part_keys[3], (LAYERS, BATCH_ROWS, HIDDEN), jnp.float32)
    lengths = draw_lengths(part_keys[4])
    return {"inputs": inputs, "targets": targets, "lengths": lengths, "w_in": w_in, "w_rec": w_rec,
            "gate_bias": gate_bias, "h_init": h_init, "c_init": c_init}


def cell_gates(pre_act):
    sig_if = jax.nn.sigmoid(pre_act[:, :2 * HIDDEN])
    cell_in = jnp.tanh(pre_act[:, 2 * HIDDEN:3 * HIDDEN])
    out_gate = jax.nn.sigmoid(pre_act[:, 3 * HIDDEN:])
    return jnp.concatenate([sig_if, cell_in, out_gate], axis=-1)


def layer_forward(seq_in, w_in, w_rec, gate_bias, h_start, c_start, active):
    in_proj = jnp.dot(seq_in.reshape(TIME_STEPS * BATCH_ROWS, HIDDEN), w_in, preferred_element_type=jnp.float32)
    in_proj = in_proj.reshape(TIME_STEPS, BATCH_ROWS, 4 * HIDDEN) + gate_bias

    def time_step(carry_in, step_in):
        h_prev, c_prev = carry_in
        proj_t, mask_t = step_in
        gate_vals = cell_gates(proj_t + jnp.dot(h_prev, w_rec, preferred_element_type=jnp.float32))
        c_new = gate_vals[:, HIDDEN:2 * HIDDEN] * c_prev + gate_vals[:, :HIDDEN] * gate_vals[:, 2 * HIDDEN:3 * HIDDEN]
        h_new = (gate_vals[:, 3 * HIDDEN:] * jnp.tanh(c_new)).astype(jnp.bfloat16)
        c_next = jnp.where(mask_t, c_new, c_prev)
        h_next = jnp.where(mask_t, h_new, h_prev)
        return (h_next, c_next), (h_next, gate_vals, c_next)

    last_state, saved_seq = lax.scan(time_step, (h_start.astype(jnp.bfloat16), c_start), (in_proj, active))
    return saved_seq


def layer_backward(seq_in, seq_out, gate_vals, cell_seq, w_in, w_rec, h_start, c_start, active, d_out):
    h_prevs = jnp.concatenate([h_start.astype(jnp.bfloat16)[None], seq_out[:-1]], axis=0)
    c_prevs = jnp.concatenate([c_start[None], cell_seq[:-1]], axis=0)

    def time_step(carry_in, step_in):
        d_hid, d_cell, d_bias = carry_in
        gates_t, c_prev, c_now, d_out_t, mask_t = step_in
        in_gate = gates_t[:, :HIDDEN]
        forget = gates_t[:, HIDDEN:2 * HIDDEN]
        cell_in = gates_t[:, 2 * HIDDEN:3 * HIDDEN]
        out_gate = gates_t[:, 3 * HIDDEN:]
        d_total = d_hid + d_out_t
        tanh_c = jnp.tanh(c_now)
        d_c_new = d_cell + d_total * out_gate * (1.0 - tanh_c * tanh_c)
        d_pre = jnp.concatenate([
            d_c_new * cell_in * in_gate * (1.0 - in_gate),
            d_c_new * c_prev * forget * (1.0 - forget),
            d_c_new * in_gate * (1.0 - cell_in * cell_in),
            d_total * tanh_c * out_gate * (1.0 - out_gate)], axis=-1)
        d_pre = jnp.where(mask_t, d_pre, 0.0)
        d_low = d_pre.astype(jnp.bfloat16)
        d_h_prev = jnp.where(mask_t, jnp.dot(d_low, w_rec.T, preferred_element_type=jnp.float32), d_total)
        d_c_prev = jnp.where(mask_t, d_c_new * forget, d_cell)
        return (d_h_prev, d_c_prev, d_bias + jnp.sum(d_pre, axis=0)), d_low

    zero_state = jnp.zeros((BATCH_ROWS, HIDDEN), jnp.float32)
    init_carry = (zero_state, zero_state, jnp.zeros((4 * HIDDEN,), jnp.float32))
    (d_h_init, d_c_init, grad_bias), d_lows = lax.scan(time_step, init_carry, (gate_vals, c_prevs, cell_seq, d_out, active), reverse=True)
    flat_d = d_lows.reshape(TIME_STEPS * BATCH_ROWS, 4 * HIDDEN)
    grad_in = jnp.dot(seq_in.reshape(TIME_STEPS * BATCH_ROWS, HIDDEN).T, flat_d, preferred_element_type=jnp.float32)
    grad_rec = jnp.dot(h_prevs.reshape(TIME_STEPS * BATCH_ROWS, HIDDEN).T, flat_d, preferred_element_type=jnp.float32)
    d_seq = jnp.dot(flat_d, w_in.T, preferred_element_type=jnp.float32).astype(jnp.bfloat16)
    return d_seq.reshape(TIME_STEPS, BATCH_ROWS, HIDDEN), grad_in, grad_rec, grad_bias, d_h_init, d_c_init


def reference(inputs, targets, lengths, w_in, w_rec, gate_bias, h_init, c_init):
    active = jnp.arange(TIME_STEPS)[:, None, None] < lengths[None, :, None]
    seq_first = jnp.transpose(inputs, (1, 0, 2))

    def fwd_layer(seq_in, params):
        seq_out, gate_vals, cell_seq = layer_forward(seq_in, params[0], params[1], params[2], params[3], params[4], active)
        return seq_out, seq_in

    top_seq, layer_ins = lax.scan(fwd_layer, seq_first, (w_in, w_rec, gate_bias, h_init, c_init))
    n_active = jnp.sum(lengths).astype(jnp.float32)
    top_err = jnp.where(active, top_seq.astype(jnp.float32) - jnp.transpose(targets, (1, 0, 2)).astype(jnp.float32), 0.0)
    loss_val = jnp.sum(top_err * top_err) / (2.0 * n_active)

    def bwd_layer(d_out, params):
        seq_out, gate_vals, cell_seq = layer_forward(params[0], params[1], params[2], params[3], params[4], params[5], active)
        result = layer_backward(params[0], seq_out, gate_vals, cell_seq, params[1], params[2], params[4], params[5], active, d_out)
        return result[0].astype(jnp.float32), result[1:]

    last_grad, grads = lax.scan(bwd_layer, top_err / n_active, (layer_ins, w_in, w_rec, gate_bias, h_init, c_init), reverse=True)
    return (loss_val.reshape(1), grads[0], grads[1], grads[2], grads[3], grads[4])
```

```python
import functools

import jax
import jax.numpy as jnp
from jax import lax
from jax.experimental import pallas as pl
from jax.experimental.pallas import tpu as pltpu
from jax.sharding import PartitionSpec as P

MESH = pl.DeviceIdType.MESH
NB = 8
WIN = 4
VMEM_LIMIT = 67043328
f32 = jnp.float32
bf16 = jnp.bfloat16


def sigmoid(x):
    return 0.5 * jnp.tanh(0.5 * x) + 0.5


def copy_of(src, dst, sem):
    return pltpu.make_async_copy(src, dst, sem)


def entry_barrier(stage, n_stages):
    barrier = pltpu.get_barrier_semaphore()
    for other in (lax.rem(stage + 1, n_stages), lax.rem(stage + n_stages - 1, n_stages)):
        pl.semaphore_signal(barrier, inc=1, device_id={"stage": other}, device_id_type=MESH)
    pl.semaphore_wait(barrier, 2)


def forward_kernel(n_stages, steps, rows, hidden,
                   seq_ref, w_in, w_rec, bias, h_start, c_start, lens,
                   useq, hseq, gates, cseq,
                   wr, wi, uring, zin, gst, cst, hst,
                   wr_sem, wi_sem, u_sem, g_sem, c_sem, h_sem, send_sem, recv_sem):
    bw = hidden // NB
    half = NB // 2
    stage = lax.axis_index("stage")
    first = stage == 0
    sends = stage < n_stages - 1
    entry_barrier(stage, n_stages)

    def wr_copies():
        return [copy_of(w_rec.at[0, :, pl.ds(g * hidden + j * bw, bw)], wr.at[j, :, pl.ds(g * bw, bw)], wr_sem.at[j, g])
                for j in range(NB) for g in range(4)]

    def wi_copies(blk, slot):
        return [copy_of(w_in.at[0, :, pl.ds(pl.multiple_of(g * hidden + blk * bw, 128), bw)],
                        wi.at[slot, :, pl.ds(g * bw, bw)], wi_sem.at[slot, g]) for g in range(4)]

    def u_copy(t):
        slot = lax.rem(t, WIN + 1)
        return copy_of(useq.at[t], uring.at[slot], u_sem.at[0])

    def g_copy(t, hf):
        return copy_of(gst.at[pl.ds(hf * half, half)], gates.at[t, pl.ds(hf * half, half)], g_sem.at[hf])

    def c_copy(slot, t):
        return copy_of(cst.at[slot], cseq.at[t], c_sem.at[slot])

    def h_copy(slot, t):
        return copy_of(hst.at[slot], hseq.at[t], h_sem.at[slot])

    def send(slot, t):
        return pltpu.make_async_remote_copy(
            src_ref=hst.at[slot], dst_ref=useq.at[t], send_sem=send_sem.at[slot], recv_sem=recv_sem.at[t],
            device_id={"stage": lax.rem(stage + 1, n_stages)}, device_id_type=MESH)

    def block_a(t):
        return half + lax.rem(t + WIN, WIN)

    def block_b(t):
        return lax.rem(t + WIN, WIN)

    def fetch_u(t):
        @pl.when(t < steps)
        def _():
            @pl.when(jnp.logical_not(first))
            def _():
                send(0, t).wait_recv()
            u_copy(t).start()

    def await_u(t):
        @pl.when(t < steps)
        def _():
            u_copy(t).wait()

    def project(blk, t0, slot):
        u = jnp.concatenate([uring[lax.rem(t0 + i + 2 * (WIN + 1), WIN + 1)] for i in range(WIN)], axis=0)
        z = jnp.dot(u, wi[slot], preferred_element_type=f32) + bias[pl.ds(blk, 1), :]
        for i in range(WIN):
            zin[blk, lax.rem(t0 + i + 2 * WIN, WIN)] = z[i * rows:(i + 1) * rows]

    def recur(t, hf):
        cur, nxt = lax.rem(t, 2), lax.rem(t + 1, 2)
        live = lens[...] > t
        h = hst[cur]
        for j in range(hf * half, (hf + 1) * half):
            cols = slice(j * bw, (j + 1) * bw)
            z = jnp.dot(h, wr[j], preferred_element_type=f32) + zin[j, lax.rem(t, WIN)]
            gi = sigmoid(z[:, :bw])
            gf = sigmoid(z[:, bw:2 * bw])
            gg = jnp.tanh(z[:, 2 * bw:3 * bw])
            go = sigmoid(z[:, 3 * bw:])
            c_prev = cst[cur, :, cols]
            c_new = gf * c_prev + gi * gg
            h_new = go * jnp.tanh(c_new)
            cst[nxt, :, cols] = jnp.where(live, c_new, c_prev)
            hst[nxt, :, cols] = jnp.where(live, h_new, h[:, cols].astype(f32)).astype(bf16)
            gst[j, :, :bw] = gi
            gst[j, :, bw:2 * bw] = gf
            gst[j, :, 2 * bw:3 * bw] = gg
            gst[j, :, 3 * bw:] = go

    for c in wi_copies(block_b(-WIN), 1):
        c.start()
    for c in wr_copies():
        c.start()
    hst[0] = h_start[...].astype(bf16)
    cst[0] = c_start[...]
    c_copy(0, 0).start()
    h_copy(0, 0).start()

    def warm(v, _):
        t = v - WIN
        fetch_u(t + WIN)

        @pl.when(v > 0)
        def _():
            for c in wi_copies(block_a(t), 0):
                c.wait()
            for c in wi_copies(block_b(t), 1):
                c.start()
            project(block_a(t), t, 0)

        for c in wi_copies(block_b(t), 1):
            c.wait()
        await_u(t + WIN)
        for c in wi_copies(block_a(t + 1), 0):
            c.start()
        project(block_b(t), t + 1, 1)
        return 0

    lax.fori_loop(0, WIN, warm, 0)
    for c in wr_copies():
        c.wait()

    def step(t, _):
        nxt = lax.rem(t + 1, 2)
        fetch_u(t + WIN)
        for c in wi_copies(block_a(t), 0):
            c.wait()
        for c in wi_copies(block_b(t), 1):
            c.start()

        @pl.when(t >= 1)
        def _():
            c_copy(nxt, t).wait()
            h_copy(nxt, t).wait()
            g_copy(t, 0).wait()

        @pl.when(jnp.logical_and(t >= 2, sends))
        def _():
            send(nxt, t).wait_send()

        recur(t, 0)
        project(block_a(t), t, 0)

        g_copy(t, 0).start()
        for c in wi_copies(block_b(t), 1):
            c.wait()

        @pl.when(t + 1 < steps)
        def _():
            for c in wi_copies(block_a(t + 1), 0):
                c.start()

        await_u(t + WIN)

        @pl.when(t >= 1)
        def _():
            g_copy(t, 1).wait()

        recur(t, 1)
        project(block_b(t), t + 1, 1)

        g_copy(t, 1).start()
        c_copy(nxt, t + 1).start()
        h_copy(nxt, t + 1).start()

        @pl.when(sends)
        def _():
            send(nxt, t).start()

        return 0

    lax.fori_loop(0, steps, step, 0)
    for hf in range(2):
        g_copy(0, hf).wait()
        c_copy(hf, 0).wait()
        h_copy(hf, 0).wait()

        @pl.when(sends)
        def _():
            send(hf, 0).wait_send()


def run_forward(n_stages, seq, w_in, w_rec, bias, h_start, c_start, lens):
    steps, rows, hidden = seq.shape
    bw = hidden // NB
    any_spec = pl.BlockSpec(memory_space=pl.ANY)
    vmem_spec = pl.BlockSpec(memory_space=pltpu.VMEM)
    dma = pltpu.SemaphoreType.DMA
    return pl.pallas_call(
        functools.partial(forward_kernel, n_stages, steps, rows, hidden),
        out_shape=(jax.ShapeDtypeStruct((steps, rows, hidden), bf16),
                   jax.ShapeDtypeStruct((steps + 1, rows, hidden), bf16),
                   jax.ShapeDtypeStruct((steps, NB, rows, 4 * bw), f32),
                   jax.ShapeDtypeStruct((steps + 1, rows, hidden), f32)),
        in_specs=[any_spec, any_spec, any_spec, vmem_spec, vmem_spec, vmem_spec, vmem_spec],
        out_specs=(any_spec,) * 4,
        input_output_aliases={0: 0},
        scratch_shapes=[
            pltpu.VMEM((NB, hidden, 4 * bw), bf16),
            pltpu.VMEM((2, hidden, 4 * bw), bf16),
            pltpu.VMEM((WIN + 1, rows, hidden), bf16),
            pltpu.VMEM((NB, WIN, rows, 4 * bw), f32),
            pltpu.VMEM((NB, rows, 4 * bw), f32),
            pltpu.VMEM((2, rows, hidden), f32),
            pltpu.VMEM((2, rows, hidden), bf16),
            dma((NB, 4)), dma((2, 4)), dma((1,)), dma((2,)), dma((2,)), dma((2,)), dma((2,)), dma((steps,)),
        ],
        compiler_params=pltpu.CompilerParams(collective_id=0, has_side_effects=True, vmem_limit_bytes=VMEM_LIMIT),
        name="lstm_forward",
    )(seq, w_in, w_rec, bias, h_start, c_start, lens)


def backward_kernel(n_stages, steps, rows, hidden,
                    hseq, tseq, gates, cseq, w_in, w_rec, lens, scale,
                    drecv, dz_out, dh_out, dc_out, db_out, loss_out,
                    wt, wi, wtmp, gin, cring, dbuf, ybuf, dzr, dh, dc, dbacc, lossacc, duacc, dust,
                    wt_sem, wi_sem, g_sem, c_sem, d_sem, y_sem, dz_sem, out_sem, send_sem, recv_sem):
    bw = hidden // NB
    half = NB // 2
    hw = half * bw
    quarter = hidden // WIN
    ring = WIN + 1
    pad = WIN - 1
    stage = lax.axis_index("stage")
    top = stage == n_stages - 1
    sends = stage > 0
    entry_barrier(stage, n_stages)

    def wt_copy(p, slot):
        j, g = p // 4, lax.rem(p, 4)
        return copy_of(w_rec.at[0, :, pl.ds(pl.multiple_of(g * hidden + j * bw, 128), bw)], wtmp.at[slot], wt_sem.at[slot])

    def part_of(t):
        return lax.rem(t + WIN, WIN)

    def wi_copies(t, hf):
        first_row = pl.multiple_of(part_of(t) * quarter, 8)
        return [copy_of(w_in.at[0, pl.ds(first_row, quarter), pl.ds(g * hidden + hf * hw, hw)],
                        wi.at[hf, :, pl.ds(g * hw, hw)], wi_sem.at[hf, g]) for g in range(4)]

    def g_copy(t, hf):
        return copy_of(gates.at[t, pl.ds(hf * half, half)], gin.at[pl.ds(hf * half, half)], g_sem.at[hf])

    def c_copy(i):
        slot = lax.rem(i, 3)
        return copy_of(cseq.at[i], cring.at[slot], c_sem.at[slot])

    def own_copies(t):
        return [copy_of(hseq.at[t + 1, :, pl.ds(q * quarter, quarter)], dbuf.at[q], d_sem.at[q]) for q in range(WIN)]

    def y_copy(t):
        return copy_of(tseq.at[t], ybuf, y_sem.at[0])

    def recv_copies(t):
        return [copy_of(drecv.at[q, t + pad], dbuf.at[q], d_sem.at[q]) for q in range(WIN)]

    def dz_copies(t):
        slot = lax.rem(t, ring)
        return [copy_of(dzr.at[slot, hf, :, pl.ds(g * hw, hw)], dz_out.at[t, :, pl.ds(g * hidden + hf * hw, hw)],
                        dz_sem.at[slot, 4 * hf + g]) for hf in range(2) for g in range(4)]

    def send(t):
        return pltpu.make_async_remote_copy(
            src_ref=dust.at[0], dst_ref=drecv.at[part_of(t), pl.ds(t + pad, WIN)],
            send_sem=send_sem.at[0], recv_sem=recv_sem.at[t + pad],
            device_id={"stage": lax.rem(stage + n_stages - 1, n_stages)}, device_id_type=MESH)

    def fetch_d(t):
        @pl.when(top)
        def _():
            for c in own_copies(t):
                c.start()
            y_copy(t).start()

        @pl.when(jnp.logical_not(top))
        def _():
            send(t - pad).wait_recv()
            for c in recv_copies(t):
                c.start()

    def await_d(t):
        for c in recv_copies(t):
            c.wait()

        @pl.when(top)
        def _():
            y_copy(t).wait()

    def input_grad(t, hf):
        d = jnp.concatenate([dzr[lax.rem(t + i + ring, ring), hf] for i in range(WIN)], axis=0)
        du = lax.dot_general(d, wi[hf], (((1,), (1,)), ((), ())), preferred_element_type=f32)
        if hf == 0:
            duacc[...] = du
        else:
            du = (du + duacc[...]).astype(bf16)
            for i in range(WIN):
                dust[0, i] = du[i * rows:(i + 1) * rows]

    def fold(x):
        return x.reshape(rows // 8, 8, x.shape[-1]).sum(axis=0)

    def recur(t, hf):
        cur, nxt = lax.rem(t, 2), lax.rem(t + 1, 2)
        live = lens[...] > t
        sc = scale[0:1, :]
        total = None
        for j in range(hf * half, (hf + 1) * half):
            cols = slice(j * bw, (j + 1) * bw)
            q, off = j * bw // quarter, j * bw % quarter
            gi, gf = gin[j, :, :bw], gin[j, :, bw:2 * bw]
            gg, go = gin[j, :, 2 * bw:3 * bw], gin[j, :, 3 * bw:]
            err = jnp.where(live, dbuf[q, :, off:off + bw].astype(f32) - ybuf[:, cols].astype(f32), 0.0)
            lossacc[:, cols] += fold(err * err)
            d_total = dh[cur, :, cols] + err * sc
            c_prev = cring[lax.rem(t, 3), :, cols]
            tanh_c = jnp.tanh(cring[lax.rem(t + 1, 3), :, cols])
            dc_old = dc[:, cols]
            d_c = dc_old + d_total * go * (1.0 - tanh_c * tanh_c)
            parts = (d_c * gg * gi * (1.0 - gi),
                     d_c * c_prev * gf * (1.0 - gf),
                     d_c * gi * (1.0 - gg * gg),
                     d_total * tanh_c * go * (1.0 - go))
            low = []
            for g in range(4):
                dz = jnp.where(live, parts[g], 0.0)
                dbacc[j, :, g * bw:(g + 1) * bw] += fold(dz)
                dz = dz.astype(bf16)
                at = g * hw + (j - hf * half) * bw
                dzr[lax.rem(t, ring), hf, :, at:at + bw] = dz
                low.append(dz)
            dc[:, cols] = jnp.where(live, d_c * gf, dc_old)
            keep = jnp.where(live, 0.0, d_total)
            if hf == 0:
                dh[nxt, :, cols] = keep
            else:
                dh[nxt, :, cols] += keep
            r = jnp.dot(jnp.concatenate(low, axis=1), wt[j], preferred_element_type=f32)
            total = r if total is None else total + r
        if hf == 0:
            dh[nxt, :, :hw] += total[:, :hw]
            dh[nxt, :, hw:] = total[:, hw:]
        else:
            dh[nxt] += total

    last = steps - 1
    for c in wi_copies(last, 0):
        c.start()
    wt_copy(0, 0).start()
    g_copy(last, 0).start()
    c_copy(last + 1).start()
    c_copy(last).start()
    dh[...] = jnp.zeros_like(dh)
    dc[...] = jnp.zeros_like(dc)
    dbacc[...] = jnp.zeros_like(dbacc)
    lossacc[...] = jnp.zeros_like(lossacc)
    ybuf[...] = jnp.zeros_like(ybuf)
    for i in range(ring):
        dzr[i] = jnp.zeros_like(dzr[i])

    def load_wt(p, _):
        slot = lax.rem(p, 2)

        @pl.when(p + 1 < 4 * NB)
        def _():
            wt_copy(p + 1, 1 - slot).start()

        wt_copy(p, slot).wait()
        j, g = p // 4, lax.rem(p, 4)
        wt[j, pl.ds(pl.multiple_of(g * bw, 8), bw), :] = wtmp[slot].T
        return 0

    lax.fori_loop(0, 4 * NB, load_wt, 0)

    @pl.when(jnp.logical_not(top))
    def _():
        for i in range(pad):
            send(last - i).wait_recv()

    fetch_d(last)
    c_copy(last + 1).wait()

    def step(v, _):
        t = last - v
        await_d(t)
        g_copy(t, 0).wait()
        c_copy(t).wait()
        for c in wi_copies(t, 0):
            c.wait()

        @pl.when(v >= ring)
        def _():
            for c in dz_copies(t + ring):
                c.wait()

        g_copy(t, 1).start()
        for c in wi_copies(t, 1):
            c.start()

        @pl.when(t >= 1)
        def _():
            c_copy(t - 1).start()

        recur(t, 0)
        input_grad(t, 0)

        g_copy(t, 1).wait()
        for c in wi_copies(t, 1):
            c.wait()

        @pl.when(jnp.logical_and(v >= 1, sends))
        def _():
            send(t + 1).wait_send()

        for c in wi_copies(t - 1, 0):
            c.start()

        @pl.when(t >= 1)
        def _():
            g_copy(t - 1, 0).start()

        recur(t, 1)
        input_grad(t, 1)
        for c in dz_copies(t):
            c.start()

        @pl.when(sends)
        def _():
            send(t).start()

        @pl.when(t >= 1)
        def _():
            fetch_d(t - 1)

        return 0

    lax.fori_loop(0, steps, step, 0)

    for i in range(ring):
        for c in dz_copies(i):
            c.wait()
    outs = [copy_of(dh.at[1], dh_out, out_sem.at[0]), copy_of(dc, dc_out, out_sem.at[1]),
            copy_of(dbacc, db_out, out_sem.at[2]), copy_of(lossacc, loss_out, out_sem.at[3])]
    for c in outs:
        c.start()
    for c in wi_copies(-1, 0):
        c.wait()

    @pl.when(sends)
    def _():
        for c in wi_copies(-1, 0):
            c.start()

        def drain(v, _):
            t = -1 - v
            for c in wi_copies(t, 0):
                c.wait()
            for c in wi_copies(t, 1):
                c.start()
            input_grad(t, 0)
            for c in wi_copies(t, 1):
                c.wait()

            @pl.when(v < pad - 1)
            def _():
                for c in wi_copies(t - 1, 0):
                    c.start()

            send(t + 1).wait_send()
            input_grad(t, 1)
            send(t).start()
            return 0

        lax.fori_loop(0, pad, drain, 0)
        send(-pad).wait_send()

    for c in outs:
        c.wait()


def run_backward(n_stages, hseq, tseq, gates, cseq, w_in, w_rec, lens, scale):
    steps, rows, hidden = tseq.shape
    bw = hidden // NB
    quarter = hidden // WIN
    any_spec = pl.BlockSpec(memory_space=pl.ANY)
    vmem_spec = pl.BlockSpec(memory_space=pltpu.VMEM)
    dma = pltpu.SemaphoreType.DMA
    return pl.pallas_call(
        functools.partial(backward_kernel, n_stages, steps, rows, hidden),
        out_shape=(jax.ShapeDtypeStruct((WIN, steps + 2 * (WIN - 1), rows, quarter), bf16),
                   jax.ShapeDtypeStruct((steps, rows, 4 * hidden), bf16),
                   jax.ShapeDtypeStruct((rows, hidden), f32),
                   jax.ShapeDtypeStruct((rows, hidden), f32),
                   jax.ShapeDtypeStruct((NB, 8, 4 * bw), f32),
                   jax.ShapeDtypeStruct((8, hidden), f32)),
        in_specs=[any_spec] * 6 + [vmem_spec] * 2,
        out_specs=(any_spec,) * 6,
        scratch_shapes=[
            pltpu.VMEM((NB, 4 * bw, hidden), bf16),
            pltpu.VMEM((2, quarter, 2 * hidden), bf16),
            pltpu.VMEM((2, hidden, bw), bf16),
            pltpu.VMEM((NB, rows, 4 * bw), f32),
            pltpu.VMEM((3, rows, hidden), f32),
            pltpu.VMEM((WIN, rows, quarter), bf16),
            pltpu.VMEM((rows, hidden), bf16),
            pltpu.VMEM((WIN + 1, 2, rows, 2 * hidden), bf16),
            pltpu.VMEM((2, rows, hidden), f32),
            pltpu.VMEM((rows, hidden), f32),
            pltpu.VMEM((NB, 8, 4 * bw), f32),
            pltpu.VMEM((8, hidden), f32),
            pltpu.VMEM((WIN * rows, quarter), f32),
            pltpu.VMEM((1, WIN, rows, quarter), bf16),
            dma((2,)), dma((2, 4)), dma((2,)), dma((3,)), dma((WIN,)), dma((1,)), dma((WIN + 1, 8)), dma((4,)), dma((1,)),
            dma((steps + WIN - 1,)),
        ],
        compiler_params=pltpu.CompilerParams(collective_id=1, has_side_effects=True, vmem_limit_bytes=VMEM_LIMIT),
        name="lstm_backward",
    )(hseq, tseq, gates, cseq, w_in, w_rec, lens, scale)


def solution(mesh):
    n_stages = mesh.shape["stage"]

    def local_program(inputs, targets, lengths, w_in, w_rec, gate_bias, h_init, c_init):
        rows, steps, hidden = inputs.shape
        bw = hidden // NB
        is_last = lax.axis_index("stage") == n_stages - 1
        n_active = jnp.sum(lengths).astype(f32)
        lens = jnp.broadcast_to(lengths[:, None], (rows, bw))
        bias = gate_bias.reshape(4, NB, bw).transpose(1, 0, 2).reshape(NB, 4 * bw)
        seq = jnp.transpose(inputs, (1, 0, 2))
        useq, hseq, gates, cseq = run_forward(n_stages, seq, w_in, w_rec, bias, h_init[0], c_init[0], lens)
        tseq = jnp.transpose(targets, (1, 0, 2))
        scale = jnp.broadcast_to(jnp.where(is_last, 1.0 / n_active, 1.0), (8, bw))
        _, dz, dh0, dc0, db, sq = run_backward(n_stages, hseq, tseq, gates, cseq, w_in, w_rec, lens, scale)
        loss = lax.psum(jnp.where(is_last, jnp.sum(sq), 0.0), "stage") / (2.0 * n_active)
        dz = dz.reshape(steps * rows, 4 * hidden)
        dims = (((0,), (0,)), ((), ()))
        grad_in = lax.dot_general(useq.reshape(steps * rows, hidden), dz, dims, preferred_element_type=f32)
        h_prev = hseq.reshape((steps + 1) * rows, hidden)[:steps * rows]
        grad_rec = lax.dot_general(h_prev, dz, dims, preferred_element_type=f32)
        grad_bias = db.sum(axis=1).reshape(NB, 4, bw).transpose(1, 0, 2).reshape(1, 4 * hidden)
        return loss.reshape(1), grad_in[None], grad_rec[None], grad_bias, dh0[None], dc0[None]

    row_spec = P("data", None, None)
    layer_spec = P("stage", None, None)
    state_spec = P("stage", "data", None)
    grad_spec = P(("data", "stage"), None, None)
    return jax.shard_map(local_program, mesh=mesh,
                         in_specs=(row_spec, row_spec, P("data"), layer_spec, layer_spec, P("stage", None), state_spec, state_spec),
                         out_specs=(P("data"), grad_spec, grad_spec, P(("data", "stage"), None), state_spec, state_spec),
                         check_vma=False)
```

```python
import functools

import jax
import jax.numpy as jnp
from jax import lax
from jax.experimental import pallas as pl
from jax.experimental.pallas import tpu as pltpu
from jax.sharding import PartitionSpec as P

MESH = pl.DeviceIdType.MESH
NB = 8
WIN = 4
VMEM_LIMIT = 67043328
f32 = jnp.float32
bf16 = jnp.bfloat16


def sigmoid(x):
    return 0.5 * jnp.tanh(0.5 * x) + 0.5


def copy_of(src, dst, sem):
    return pltpu.make_async_copy(src, dst, sem)


def entry_barrier(stage, n_stages):
    barrier = pltpu.get_barrier_semaphore()
    for other in (lax.rem(stage + 1, n_stages), lax.rem(stage + n_stages - 1, n_stages)):
        pl.semaphore_signal(barrier, inc=1, device_id={"stage": other}, device_id_type=MESH)
    pl.semaphore_wait(barrier, 2)


def forward_kernel(n_stages, steps, rows, hidden,
                   seq_ref, w_in, w_rec, bias, h_start, c_start, lens,
                   useq, hseq, gates, cseq,
                   wr, wi, uring, zin, gst, cst, hst,
                   wr_sem, wi_sem, u_sem, g_sem, c_sem, h_sem, send_sem, recv_sem):
    bw = hidden // NB
    half = NB // 2
    hw = half * bw
    stage = lax.axis_index("stage")
    first = stage == 0
    sends = stage < n_stages - 1
    entry_barrier(stage, n_stages)

    def wr_copies():
        return [copy_of(w_rec.at[0, :, pl.ds(g * hidden + j * bw, bw)], wr.at[j, :, pl.ds(g * bw, bw)], wr_sem.at[j, g])
                for j in range(NB) for g in range(4)]

    def wi_copy(blk, slot):
        first_col = lax.rem(blk, 4) * hidden + blk // 4 * hw
        return copy_of(w_in.at[0, :, pl.ds(pl.multiple_of(first_col, 128), hw)], wi.at[slot], wi_sem.at[slot])

    def u_copy(t):
        slot = lax.rem(t, WIN + 1)
        return copy_of(useq.at[t], uring.at[slot], u_sem.at[0])

    def g_copy(t, hf):
        return copy_of(gst.at[pl.ds(hf * half, half)], gates.at[t, pl.ds(hf * half, half)], g_sem.at[hf])

    def c_copy(slot, t):
        return copy_of(cst.at[slot], cseq.at[t], c_sem.at[slot])

    def h_copy(slot, t):
        return copy_of(hst.at[slot], hseq.at[t], h_sem.at[slot])

    def send(slot, t):
        return pltpu.make_async_remote_copy(
            src_ref=hst.at[slot], dst_ref=useq.at[t], send_sem=send_sem.at[slot], recv_sem=recv_sem.at[t],
            device_id={"stage": lax.rem(stage + 1, n_stages)}, device_id_type=MESH)

    def block_a(t):
        return half + lax.rem(t + WIN, WIN)

    def block_b(t):
        return lax.rem(t + WIN, WIN)

    def fetch_u(t):
        @pl.when(t < steps)
        def _():
            @pl.when(jnp.logical_not(first))
            def _():
                send(0, t).wait_recv()
            u_copy(t).start()

    def await_u(t):
        @pl.when(t < steps)
        def _():
            u_copy(t).wait()

    def project(blk, t0, slot):
        u = jnp.concatenate([uring[lax.rem(t0 + i + 2 * (WIN + 1), WIN + 1)] for i in range(WIN)], axis=0)
        z = jnp.dot(u, wi[slot], preferred_element_type=f32) + bias[pl.ds(blk, 1), :]
        for i in range(WIN):
            zin[blk, lax.rem(t0 + i + 2 * WIN, WIN)] = z[i * rows:(i + 1) * rows]

    def recur(t, hf):
        cur, nxt = lax.rem(t, 2), lax.rem(t + 1, 2)
        live = lens[...] > t
        h = hst[cur]
        for j in range(hf * half, (hf + 1) * half):
            cols = slice(j * bw, (j + 1) * bw)
            z = jnp.dot(h, wr[j], preferred_element_type=f32)
            at = (j - hf * half) * bw
            zi, zf, zg, zo = (z[:, g * bw:(g + 1) * bw] + zin[4 * hf + g, lax.rem(t, WIN), :, at:at + bw] for g in range(4))
            gi = sigmoid(zi)
            gf = sigmoid(zf)
            gg = jnp.tanh(zg)
            go = sigmoid(zo)
            c_prev = cst[cur, :, cols]
            c_new = gf * c_prev + gi * gg
            h_new = go * jnp.tanh(c_new)
            cst[nxt, :, cols] = jnp.where(live, c_new, c_prev)
            hst[nxt, :, cols] = jnp.where(live, h_new, h[:, cols].astype(f32)).astype(bf16)
            gst[j, :, :bw] = gi
            gst[j, :, bw:2 * bw] = gf
            gst[j, :, 2 * bw:3 * bw] = gg
            gst[j, :, 3 * bw:] = go

    wi_copy(block_b(-WIN), 1).start()
    for c in wr_copies():
        c.start()
    hst[0] = h_start[...].astype(bf16)
    cst[0] = c_start[...]
    c_copy(0, 0).start()
    h_copy(0, 0).start()

    def warm(v, _):
        t = v - WIN
        fetch_u(t + WIN)

        @pl.when(v > 0)
        def _():
            wi_copy(block_a(t), 0).wait()
            wi_copy(block_b(t), 1).start()
            project(block_a(t), t, 0)

        wi_copy(block_b(t), 1).wait()
        await_u(t + WIN)
        wi_copy(block_a(t + 1), 0).start()
        project(block_b(t), t + 1, 1)
        return 0

    lax.fori_loop(0, WIN, warm, 0)
    for c in wr_copies():
        c.wait()

    def step(t, _):
        nxt = lax.rem(t + 1, 2)
        fetch_u(t + WIN)
        wi_copy(block_a(t), 0).wait()
        wi_copy(block_b(t), 1).start()

        @pl.when(t >= 1)
        def _():
            c_copy(nxt, t).wait()
            h_copy(nxt, t).wait()
            g_copy(t, 0).wait()

        @pl.when(jnp.logical_and(t >= 2, sends))
        def _():
            send(nxt, t).wait_send()

        recur(t, 0)
        project(block_a(t), t, 0)

        g_copy(t, 0).start()
        wi_copy(block_b(t), 1).wait()

        @pl.when(t + 1 < steps)
        def _():
            wi_copy(block_a(t + 1), 0).start()

        await_u(t + WIN)

        @pl.when(t >= 1)
        def _():
            g_copy(t, 1).wait()

        recur(t, 1)
        project(block_b(t), t + 1, 1)

        g_copy(t, 1).start()
        c_copy(nxt, t + 1).start()
        h_copy(nxt, t + 1).start()

        @pl.when(sends)
        def _():
            send(nxt, t).start()

        return 0

    lax.fori_loop(0, steps, step, 0)
    for hf in range(2):
        g_copy(0, hf).wait()
        c_copy(hf, 0).wait()
        h_copy(hf, 0).wait()

        @pl.when(sends)
        def _():
            send(hf, 0).wait_send()


def run_forward(n_stages, seq, w_in, w_rec, bias, h_start, c_start, lens):
    steps, rows, hidden = seq.shape
    bw = hidden // NB
    any_spec = pl.BlockSpec(memory_space=pl.ANY)
    vmem_spec = pl.BlockSpec(memory_space=pltpu.VMEM)
    dma = pltpu.SemaphoreType.DMA
    return pl.pallas_call(
        functools.partial(forward_kernel, n_stages, steps, rows, hidden),
        out_shape=(jax.ShapeDtypeStruct((steps, rows, hidden), bf16),
                   jax.ShapeDtypeStruct((steps + 1, rows, hidden), bf16),
                   jax.ShapeDtypeStruct((steps, NB, rows, 4 * bw), f32),
                   jax.ShapeDtypeStruct((steps + 1, rows, hidden), f32)),
        in_specs=[any_spec, any_spec, any_spec, vmem_spec, vmem_spec, vmem_spec, vmem_spec],
        out_specs=(any_spec,) * 4,
        input_output_aliases={0: 0},
        scratch_shapes=[
            pltpu.VMEM((NB, hidden, 4 * bw), bf16),
            pltpu.VMEM((2, hidden, 4 * bw), bf16),
            pltpu.VMEM((WIN + 1, rows, hidden), bf16),
            pltpu.VMEM((NB, WIN, rows, 4 * bw), f32),
            pltpu.VMEM((NB, rows, 4 * bw), f32),
            pltpu.VMEM((2, rows, hidden), f32),
            pltpu.VMEM((2, rows, hidden), bf16),
            dma((NB, 4)), dma((2,)), dma((1,)), dma((2,)), dma((2,)), dma((2,)), dma((2,)), dma((steps,)),
        ],
        compiler_params=pltpu.CompilerParams(collective_id=0, has_side_effects=True, vmem_limit_bytes=VMEM_LIMIT),
        name="lstm_forward",
    )(seq, w_in, w_rec, bias, h_start, c_start, lens)


def backward_kernel(n_stages, steps, rows, hidden,
                    hseq, tseq, gates, cseq, w_in, w_rec, lens, scale,
                    drecv, dz_out, dh_out, dc_out, db_out, loss_out,
                    wt, wi, wtmp, gin, cring, dbuf, ybuf, dzr, dh, dc, dbacc, lossacc, duacc, dust,
                    wt_sem, wi_sem, g_sem, c_sem, d_sem, y_sem, dz_sem, out_sem, send_sem, recv_sem):
    bw = hidden // NB
    half = NB // 2
    hw = half * bw
    quarter = hidden // WIN
    ring = WIN + 1
    pad = WIN - 1
    stage = lax.axis_index("stage")
    top = stage == n_stages - 1
    sends = stage > 0
    entry_barrier(stage, n_stages)

    def wt_copy(p, slot):
        j, g = p // 4, lax.rem(p, 4)
        return copy_of(w_rec.at[0, :, pl.ds(pl.multiple_of(g * hidden + j * bw, 128), bw)], wtmp.at[slot], wt_sem.at[slot])

    def part_of(t):
        return lax.rem(t + WIN, WIN)

    def wi_copies(t, hf):
        first_row = pl.multiple_of(part_of(t) * quarter, 8)
        return [copy_of(w_in.at[0, pl.ds(first_row, quarter), pl.ds(g * hidden + hf * hw, hw)],
                        wi.at[hf, :, pl.ds(g * hw, hw)], wi_sem.at[hf, g]) for g in range(4)]

    def g_copy(t, hf):
        return copy_of(gates.at[t, pl.ds(hf * half, half)], gin.at[pl.ds(hf * half, half)], g_sem.at[hf])

    def c_copy(i):
        slot = lax.rem(i, 3)
        return copy_of(cseq.at[i], cring.at[slot], c_sem.at[slot])

    def own_copies(t):
        return [copy_of(hseq.at[t + 1, :, pl.ds(q * quarter, quarter)], dbuf.at[lax.rem(t, 2), q], d_sem.at[q]) for q in range(WIN)]

    def y_copy(t):
        return copy_of(tseq.at[t], ybuf.at[lax.rem(t, 2)], y_sem.at[0])

    def recv_copies(t):
        return [copy_of(drecv.at[q, t + pad], dbuf.at[lax.rem(t, 2), q], d_sem.at[q]) for q in range(WIN)]

    def dz_copies(t):
        slot = lax.rem(t, ring)
        return [copy_of(dzr.at[slot, hf, :, pl.ds(g * hw, hw)], dz_out.at[t, :, pl.ds(g * hidden + hf * hw, hw)],
                        dz_sem.at[slot, 4 * hf + g]) for hf in range(2) for g in range(4)]

    def send(t):
        return pltpu.make_async_remote_copy(
            src_ref=dust.at[0], dst_ref=drecv.at[part_of(t), pl.ds(t + pad, WIN)],
            send_sem=send_sem.at[0], recv_sem=recv_sem.at[t + pad],
            device_id={"stage": lax.rem(stage + n_stages - 1, n_stages)}, device_id_type=MESH)

    def fetch_d(t):
        @pl.when(top)
        def _():
            for c in own_copies(t):
                c.start()
            y_copy(t).start()

        @pl.when(jnp.logical_not(top))
        def _():
            send(t - pad).wait_recv()
            for c in recv_copies(t):
                c.start()

    def await_d(t):
        for c in recv_copies(t):
            c.wait()

        @pl.when(top)
        def _():
            y_copy(t).wait()

    def input_grad(t, hf):
        d = jnp.concatenate([dzr[lax.rem(t + i + ring, ring), hf] for i in range(WIN)], axis=0)
        du = lax.dot_general(d, wi[hf], (((1,), (1,)), ((), ())), preferred_element_type=f32)
        if hf == 0:
            duacc[...] = du
        else:
            du = (du + duacc[...]).astype(bf16)
            for i in range(WIN):
                dust[0, i] = du[i * rows:(i + 1) * rows]

    def fold(x):
        return x.reshape(rows // 8, 8, x.shape[-1]).sum(axis=0)

    def recur(t, hf):
        cur, nxt = lax.rem(t, 2), lax.rem(t + 1, 2)
        slot = cur
        live = lens[...] > t
        sc = scale[0:1, :bw]
        total = None
        for j in range(hf * half, (hf + 1) * half):
            cols = slice(j * bw, (j + 1) * bw)
            q, off = j * bw // quarter, j * bw % quarter
            gi, gf = gin[j, :, :bw], gin[j, :, bw:2 * bw]
            gg, go = gin[j, :, 2 * bw:3 * bw], gin[j, :, 3 * bw:]
            err = jnp.where(live, dbuf[slot, q, :, off:off + bw].astype(f32) - ybuf[slot, :, cols].astype(f32), 0.0)
            lossacc[:, cols] += fold(err * err)
            d_total = dh[cur, :, cols] + err * sc
            c_prev = cring[lax.rem(t, 3), :, cols]
            tanh_c = jnp.tanh(cring[lax.rem(t + 1, 3), :, cols])
            dc_old = dc[:, cols]
            d_c = dc_old + d_total * go * (1.0 - tanh_c * tanh_c)
            parts = (d_c * gg * gi * (1.0 - gi),
                     d_c * c_prev * gf * (1.0 - gf),
                     d_c * gi * (1.0 - gg * gg),
                     d_total * tanh_c * go * (1.0 - go))
            low = []
            for g in range(4):
                dz = jnp.where(live, parts[g], 0.0)
                dbacc[j, :, g * bw:(g + 1) * bw] += fold(dz)
                dz = dz.astype(bf16)
                at = g * hw + (j - hf * half) * bw
                dzr[lax.rem(t, ring), hf, :, at:at + bw] = dz
                low.append(dz)
            dc[:, cols] = jnp.where(live, d_c * gf, dc_old)
            keep = jnp.where(live, 0.0, d_total)
            if hf == 0:
                dh[nxt, :, cols] = keep
            else:
                dh[nxt, :, cols] += keep
            r = jnp.dot(jnp.concatenate(low, axis=1), wt[j], preferred_element_type=f32)
            total = r if total is None else total + r
        if hf == 0:
            dh[nxt, :, :hw] += total[:, :hw]
            dh[nxt, :, hw:] = total[:, hw:]
        else:
            dh[nxt] += total

    last = steps - 1
    for c in wi_copies(last, 0):
        c.start()
    wt_copy(0, 0).start()
    g_copy(last, 0).start()
    c_copy(last + 1).start()
    c_copy(last).start()
    dh[...] = jnp.zeros_like(dh)
    dc[...] = jnp.zeros_like(dc)
    dbacc[...] = jnp.zeros_like(dbacc)
    lossacc[...] = jnp.zeros_like(lossacc)
    ybuf[...] = jnp.zeros_like(ybuf)
    for i in range(ring):
        dzr[i] = jnp.zeros_like(dzr[i])

    def load_wt(p, _):
        slot = lax.rem(p, 2)

        @pl.when(p + 1 < 4 * NB)
        def _():
            wt_copy(p + 1, 1 - slot).start()

        wt_copy(p, slot).wait()
        j, g = p // 4, lax.rem(p, 4)
        wt[j, pl.ds(pl.multiple_of(g * bw, 8), bw), :] = wtmp[slot].T
        return 0

    lax.fori_loop(0, 4 * NB, load_wt, 0)

    @pl.when(jnp.logical_not(top))
    def _():
        for i in range(pad):
            send(last - i).wait_recv()

    fetch_d(last)
    c_copy(last + 1).wait()

    def step(v, _):
        t = last - v
        await_d(t)
        g_copy(t, 0).wait()
        c_copy(t).wait()
        for c in wi_copies(t, 0):
            c.wait()

        @pl.when(v >= ring)
        def _():
            for c in dz_copies(t + ring):
                c.wait()

        g_copy(t, 1).start()
        for c in wi_copies(t, 1):
            c.start()

        @pl.when(t >= 1)
        def _():
            c_copy(t - 1).start()

        recur(t, 0)
        input_grad(t, 0)

        g_copy(t, 1).wait()
        for c in wi_copies(t, 1):
            c.wait()

        @pl.when(jnp.logical_and(v >= 1, sends))
        def _():
            send(t + 1).wait_send()

        for c in wi_copies(t - 1, 0):
            c.start()

        @pl.when(t >= 1)
        def _():
            g_copy(t - 1, 0).start()
            fetch_d(t - 1)

        recur(t, 1)
        input_grad(t, 1)
        for c in dz_copies(t):
            c.start()

        @pl.when(sends)
        def _():
            send(t).start()

        return 0

    lax.fori_loop(0, steps, step, 0)

    for i in range(ring):
        for c in dz_copies(i):
            c.wait()
    outs = [copy_of(dh.at[1], dh_out, out_sem.at[0]), copy_of(dc, dc_out, out_sem.at[1]),
            copy_of(dbacc, db_out, out_sem.at[2]), copy_of(lossacc, loss_out, out_sem.at[3])]
    for c in outs:
        c.start()
    for c in wi_copies(-1, 0):
        c.wait()

    @pl.when(sends)
    def _():
        for c in wi_copies(-1, 0):
            c.start()

        def drain(v, _):
            t = -1 - v
            for c in wi_copies(t, 0):
                c.wait()
            for c in wi_copies(t, 1):
                c.start()
            input_grad(t, 0)
            for c in wi_copies(t, 1):
                c.wait()

            @pl.when(v < pad - 1)
            def _():
                for c in wi_copies(t - 1, 0):
                    c.start()

            send(t + 1).wait_send()
            input_grad(t, 1)
            send(t).start()
            return 0

        lax.fori_loop(0, pad, drain, 0)
        send(-pad).wait_send()

    for c in outs:
        c.wait()


def run_backward(n_stages, hseq, tseq, gates, cseq, w_in, w_rec, lens, scale):
    steps, rows, hidden = tseq.shape
    bw = hidden // NB
    quarter = hidden // WIN
    any_spec = pl.BlockSpec(memory_space=pl.ANY)
    vmem_spec = pl.BlockSpec(memory_space=pltpu.VMEM)
    dma = pltpu.SemaphoreType.DMA
    return pl.pallas_call(
        functools.partial(backward_kernel, n_stages, steps, rows, hidden),
        out_shape=(jax.ShapeDtypeStruct((WIN, steps + 2 * (WIN - 1), rows, quarter), bf16),
                   jax.ShapeDtypeStruct((steps, rows, 4 * hidden), bf16),
                   jax.ShapeDtypeStruct((rows, hidden), f32),
                   jax.ShapeDtypeStruct((rows, hidden), f32),
                   jax.ShapeDtypeStruct((NB, 8, 4 * bw), f32),
                   jax.ShapeDtypeStruct((8, hidden), f32)),
        in_specs=[any_spec] * 6 + [vmem_spec] * 2,
        out_specs=(any_spec,) * 6,
        scratch_shapes=[
            pltpu.VMEM((NB, 4 * bw, hidden), bf16),
            pltpu.VMEM((2, quarter, 2 * hidden), bf16),
            pltpu.VMEM((2, hidden, bw), bf16),
            pltpu.VMEM((NB, rows, 4 * bw), f32),
            pltpu.VMEM((3, rows, hidden), f32),
            pltpu.VMEM((2, WIN, rows, quarter), bf16),
            pltpu.VMEM((2, rows, hidden), bf16),
            pltpu.VMEM((WIN + 1, 2, rows, 2 * hidden), bf16),
            pltpu.VMEM((2, rows, hidden), f32),
            pltpu.VMEM((rows, hidden), f32),
            pltpu.VMEM((NB, 8, 4 * bw), f32),
            pltpu.VMEM((8, hidden), f32),
            pltpu.VMEM((WIN * rows, quarter), f32),
            pltpu.VMEM((1, WIN, rows, quarter), bf16),
            dma((2,)), dma((2, 4)), dma((2,)), dma((3,)), dma((WIN,)), dma((1,)), dma((WIN + 1, 8)), dma((4,)), dma((1,)),
            dma((steps + WIN - 1,)),
        ],
        compiler_params=pltpu.CompilerParams(collective_id=1, has_side_effects=True, vmem_limit_bytes=VMEM_LIMIT),
        name="lstm_backward",
    )(hseq, tseq, gates, cseq, w_in, w_rec, lens, scale)


def solution(mesh):
    n_stages = mesh.shape["stage"]

    def local_program(inputs, targets, lengths, w_in, w_rec, gate_bias, h_init, c_init):
        rows, steps, hidden = inputs.shape
        bw = hidden // NB
        is_last = lax.axis_index("stage") == n_stages - 1
        n_active = jnp.sum(lengths).astype(f32)
        lens = jnp.broadcast_to(lengths[:, None], (rows, bw))
        bias = gate_bias.reshape(4, 2, hidden // 2).transpose(1, 0, 2).reshape(8, hidden // 2)
        seq = jnp.transpose(inputs, (1, 0, 2))
        useq, hseq, gates, cseq = run_forward(n_stages, seq, w_in, w_rec, bias, h_init[0], c_init[0], lens)
        tseq = jnp.transpose(targets, (1, 0, 2))
        scale = jnp.broadcast_to(jnp.where(is_last, 1.0 / n_active, 1.0), (8, 2 * bw))
        _, dz, dh0, dc0, db, sq = run_backward(n_stages, hseq, tseq, gates, cseq, w_in, w_rec, lens, scale)
        loss = lax.psum(jnp.where(is_last, jnp.sum(sq), 0.0), "stage") / (2.0 * n_active)
        dz = dz.reshape(steps * rows, 4 * hidden)
        dims = (((0,), (0,)), ((), ()))
        grad_in = lax.dot_general(useq.reshape(steps * rows, hidden), dz, dims, preferred_element_type=f32)
        h_prev = hseq.reshape((steps + 1) * rows, hidden)[:steps * rows]
        grad_rec = lax.dot_general(h_prev, dz, dims, preferred_element_type=f32)
        grad_bias = db.sum(axis=1).reshape(NB, 4, bw).transpose(1, 0, 2).reshape(1, 4 * hidden)
        return loss.reshape(1), grad_in[None], grad_rec[None], grad_bias, dh0[None], dc0[None]

    row_spec = P("data", None, None)
    layer_spec = P("stage", None, None)
    state_spec = P("stage", "data", None)
    grad_spec = P(("data", "stage"), None, None)
    return jax.shard_map(local_program, mesh=mesh,
                         in_specs=(row_spec, row_spec, P("data"), layer_spec, layer_spec, P("stage", None), state_spec, state_spec),
                         out_specs=(P("data"), grad_spec, grad_spec, P(("data", "stage"), None), state_spec, state_spec),
                         check_vma=False)
```

```python
import functools

import jax
import jax.numpy as jnp
from jax import lax
from jax.experimental import pallas as pl
from jax.experimental.pallas import tpu as pltpu
from jax.sharding import PartitionSpec as P

MESH = pl.DeviceIdType.MESH
NB = 8
WIN = 4
GROUP = 16
VMEM_LIMIT = 67043328
f32 = jnp.float32
bf16 = jnp.bfloat16


def sigmoid(x):
    return 0.5 * jnp.tanh(0.5 * x) + 0.5


def copy_of(src, dst, sem):
    return pltpu.make_async_copy(src, dst, sem)


def entry_barrier(stage, n_stages):
    barrier = pltpu.get_barrier_semaphore()
    for step in range(1, n_stages):
        pl.semaphore_signal(barrier, inc=1, device_id={"stage": lax.rem(stage + step, n_stages)}, device_id_type=MESH)
    pl.semaphore_wait(barrier, n_stages - 1)


def prepare_kernel(n_stages, inputs, targets, useq, tseq, src, dst, in_sem, out_sem):
    rows, steps, _ = inputs.shape
    stage = lax.axis_index("stage")
    n_slots = src.shape[0]
    n_cols = steps // GROUP
    units = rows // GROUP * n_cols

    def turn(x, y):
        def load(i):
            slot = lax.rem(i, n_slots)
            return copy_of(x.at[pl.ds(pl.multiple_of(i // n_cols * GROUP, GROUP), GROUP),
                                pl.ds(pl.multiple_of(lax.rem(i, n_cols) * GROUP, GROUP), GROUP)], src.at[slot], in_sem.at[slot])

        def save(i):
            slot = lax.rem(i, n_slots)
            return copy_of(dst.at[slot], y.at[i // n_cols, pl.ds(lax.rem(i, n_cols) * GROUP, GROUP)], out_sem.at[slot])

        for i in range(min(n_slots, units)):
            load(i).start()

        def unit(i, _):
            slot = lax.rem(i, n_slots)
            load(i).wait()

            @pl.when(i >= n_slots)
            def _():
                save(i).wait()

            dst[slot] = jnp.swapaxes(src[slot], 0, 1)
            save(i).start()

            @pl.when(i + n_slots < units)
            def _():
                load(i + n_slots).start()

            return 0

        lax.fori_loop(0, units, unit, 0)
        for i in range(max(0, units - n_slots), units):
            save(i).wait()

    @pl.when(stage == 0)
    def _():
        turn(inputs, useq)

    @pl.when(stage == n_stages - 1)
    def _():
        turn(targets, tseq)


def run_prepare(n_stages, inputs, targets):
    rows, steps, hidden = inputs.shape
    any_spec = pl.BlockSpec(memory_space=pl.ANY)
    dma = pltpu.SemaphoreType.DMA
    out = jax.ShapeDtypeStruct((rows // GROUP, steps, GROUP, hidden), bf16)
    return pl.pallas_call(
        functools.partial(prepare_kernel, n_stages),
        out_shape=(out, out), in_specs=[any_spec] * 2, out_specs=(any_spec,) * 2,
        scratch_shapes=[pltpu.VMEM((4, GROUP, GROUP, hidden), bf16), pltpu.VMEM((4, GROUP, GROUP, hidden), bf16),
                        dma((4,)), dma((4,))],
        compiler_params=pltpu.CompilerParams(vmem_limit_bytes=VMEM_LIMIT),
        name="lstm_prepare",
    )(inputs, targets)


def forward_kernel(n_stages, steps, rows, hidden,
                   seq_ref, w_in, w_rec, bias, h_start, c_start, lens,
                   useq, hseq, gates, cseq,
                   wr, wi, uring, zin, gst, cst, hst,
                   wr_sem, wi_sem, u_sem, g_sem, c_sem, h_sem, send_sem, recv_sem):
    bw = hidden // NB
    half = NB // 2
    hw = half * bw
    stage = lax.axis_index("stage")
    first = stage == 0
    sends = stage < n_stages - 1
    entry_barrier(stage, n_stages)

    def wr_copies():
        return [copy_of(w_rec.at[0, :, pl.ds(g * hidden + j * bw, bw)], wr.at[j, :, pl.ds(g * bw, bw)], wr_sem.at[j, g])
                for j in range(NB) for g in range(4)]

    def wi_copy(blk, slot):
        first_col = lax.rem(blk, 4) * hidden + blk // 4 * hw
        return copy_of(w_in.at[0, :, pl.ds(pl.multiple_of(first_col, 128), hw)], wi.at[slot], wi_sem.at[slot])

    def u_copy(t):
        slot = lax.rem(t, WIN + 1)
        return copy_of(useq.at[:, t], uring.at[slot], u_sem.at[0])

    def g_copy(t, hf):
        return copy_of(gst.at[pl.ds(hf * half, half)], gates.at[t, pl.ds(hf * half, half)], g_sem.at[hf])

    def c_copy(slot, t):
        return copy_of(cst.at[slot], cseq.at[t], c_sem.at[slot])

    def h_copy(slot, t):
        return copy_of(hst.at[slot], hseq.at[:, t], h_sem.at[slot])

    def send(slot, t):
        return pltpu.make_async_remote_copy(
            src_ref=hst.at[slot], dst_ref=useq.at[:, t], send_sem=send_sem.at[slot], recv_sem=recv_sem.at[t],
            device_id={"stage": lax.rem(stage + 1, n_stages)}, device_id_type=MESH)

    def block_a(t):
        return half + lax.rem(t + WIN, WIN)

    def block_b(t):
        return lax.rem(t + WIN, WIN)

    def fetch_u(t):
        @pl.when(t < steps)
        def _():
            @pl.when(jnp.logical_not(first))
            def _():
                send(0, t).wait_recv()
            u_copy(t).start()

    def await_u(t):
        @pl.when(t < steps)
        def _():
            u_copy(t).wait()

    def project(blk, t0, slot):
        u = jnp.concatenate([uring[lax.rem(t0 + i + 2 * (WIN + 1), WIN + 1)].reshape(rows, hidden) for i in range(WIN)], axis=0)
        z = jnp.dot(u, wi[slot], preferred_element_type=f32) + bias[pl.ds(blk, 1), :]
        for i in range(WIN):
            zin[blk, lax.rem(t0 + i + 2 * WIN, WIN)] = z[i * rows:(i + 1) * rows]

    def recur(t, hf):
        cur, nxt = lax.rem(t, 2), lax.rem(t + 1, 2)
        live = lens[...] > t
        h = hst[cur].reshape(rows, hidden)
        h_twice = jnp.concatenate([h, h], axis=0)
        for j in range(hf * half, (hf + 1) * half):
            cols = slice(j * bw, (j + 1) * bw)
            z = jnp.dot(h_twice, wr[j], preferred_element_type=f32)
            z = jnp.maximum(z[:rows], z[rows:])
            at = (j - hf * half) * bw
            zi, zf, zg, zo = (z[:, g * bw:(g + 1) * bw] + zin[4 * hf + g, lax.rem(t, WIN), :, at:at + bw] for g in range(4))
            gi = sigmoid(zi)
            gf = sigmoid(zf)
            gg = jnp.tanh(zg)
            go = sigmoid(zo)
            c_prev = cst[cur, :, cols]
            c_new = gf * c_prev + gi * gg
            h_new = go * jnp.tanh(c_new)
            cst[nxt, :, cols] = jnp.where(live, c_new, c_prev)
            hst[nxt, :, :, cols] = jnp.where(live, h_new, h[:, cols].astype(f32)).astype(bf16).reshape(rows // GROUP, GROUP, bw)
            gst[j, :, :bw] = gi
            gst[j, :, bw:2 * bw] = gf
            gst[j, :, 2 * bw:3 * bw] = gg
            gst[j, :, 3 * bw:] = go

    wi_copy(block_b(-WIN), 1).start()
    for c in wr_copies():
        c.start()
    hst[0] = h_start[...].astype(bf16).reshape(rows // GROUP, GROUP, hidden)
    cst[0] = c_start[...]
    c_copy(0, 0).start()
    h_copy(0, 0).start()

    def warm(v, _):
        t = v - WIN
        fetch_u(t + WIN)

        @pl.when(v > 0)
        def _():
            wi_copy(block_a(t), 0).wait()
            wi_copy(block_b(t), 1).start()
            project(block_a(t), t, 0)

        wi_copy(block_b(t), 1).wait()
        await_u(t + WIN)
        wi_copy(block_a(t + 1), 0).start()
        project(block_b(t), t + 1, 1)
        return 0

    lax.fori_loop(0, WIN, warm, 0)
    for c in wr_copies():
        c.wait()

    def step(t, _):
        nxt = lax.rem(t + 1, 2)
        fetch_u(t + WIN)
        wi_copy(block_a(t), 0).wait()
        wi_copy(block_b(t), 1).start()

        @pl.when(t >= 1)
        def _():
            c_copy(nxt, t).wait()
            h_copy(nxt, t).wait()
            g_copy(t, 0).wait()

        @pl.when(jnp.logical_and(t >= 2, sends))
        def _():
            send(nxt, t).wait_send()

        recur(t, 0)
        project(block_a(t), t, 0)

        g_copy(t, 0).start()
        wi_copy(block_b(t), 1).wait()

        @pl.when(t + 1 < steps)
        def _():
            wi_copy(block_a(t + 1), 0).start()

        await_u(t + WIN)

        @pl.when(t >= 1)
        def _():
            g_copy(t, 1).wait()

        recur(t, 1)
        project(block_b(t), t + 1, 1)

        g_copy(t, 1).start()
        c_copy(nxt, t + 1).start()
        h_copy(nxt, t + 1).start()

        @pl.when(sends)
        def _():
            send(nxt, t).start()

        return 0

    lax.fori_loop(0, steps, step, 0)
    for hf in range(2):
        g_copy(0, hf).wait()
        c_copy(hf, 0).wait()
        h_copy(hf, 0).wait()

        @pl.when(sends)
        def _():
            send(hf, 0).wait_send()


def run_forward(n_stages, seq, w_in, w_rec, bias, h_start, c_start, lens):
    n_groups, steps, _, hidden = seq.shape
    rows = n_groups * GROUP
    bw = hidden // NB
    any_spec = pl.BlockSpec(memory_space=pl.ANY)
    vmem_spec = pl.BlockSpec(memory_space=pltpu.VMEM)
    dma = pltpu.SemaphoreType.DMA
    return pl.pallas_call(
        functools.partial(forward_kernel, n_stages, steps, rows, hidden),
        out_shape=(jax.ShapeDtypeStruct((n_groups, steps, GROUP, hidden), bf16),
                   jax.ShapeDtypeStruct((n_groups, steps + 1, GROUP, hidden), bf16),
                   jax.ShapeDtypeStruct((steps, NB, rows, 4 * bw), f32),
                   jax.ShapeDtypeStruct((steps + 1, rows, hidden), f32)),
        in_specs=[any_spec, any_spec, any_spec, vmem_spec, vmem_spec, vmem_spec, vmem_spec],
        out_specs=(any_spec,) * 4,
        input_output_aliases={0: 0},
        scratch_shapes=[
            pltpu.VMEM((NB, hidden, 4 * bw), bf16),
            pltpu.VMEM((2, hidden, 4 * bw), bf16),
            pltpu.VMEM((WIN + 1, n_groups, GROUP, hidden), bf16),
            pltpu.VMEM((NB, WIN, rows, 4 * bw), f32),
            pltpu.VMEM((NB, rows, 4 * bw), f32),
            pltpu.VMEM((2, rows, hidden), f32),
            pltpu.VMEM((2, n_groups, GROUP, hidden), bf16),
            dma((NB, 4)), dma((2,)), dma((1,)), dma((2,)), dma((2,)), dma((2,)), dma((2,)), dma((steps,)),
        ],
        compiler_params=pltpu.CompilerParams(collective_id=0, has_side_effects=True, vmem_limit_bytes=VMEM_LIMIT),
        name="lstm_forward",
    )(seq, w_in, w_rec, bias, h_start, c_start, lens)


def backward_kernel(n_stages, steps, rows, hidden,
                    hseq, tseq, gates, cseq, w_in, w_rec, lens, scale,
                    drecv, dz_out, dh_out, dc_out, db_out, loss_out,
                    wt, wi, wtmp, gin, cring, dbuf, ybuf, dzr, dh, dc, dbacc, lossacc, duacc, dust, lsend, lrecv,
                    wt_sem, wi_sem, g_sem, c_sem, d_sem, y_sem, dz_sem, out_sem, send_sem, recv_sem, lsend_sem, lrecv_sem):
    bw = hidden // NB
    n_groups = rows // GROUP
    half = NB // 2
    hw = half * bw
    quarter = hidden // WIN
    ring = WIN + 1
    pad = WIN - 1
    stage = lax.axis_index("stage")
    top = stage == n_stages - 1
    sends = stage > 0
    entry_barrier(stage, n_stages)

    def wt_copy(p, slot):
        j, g = p // 4, lax.rem(p, 4)
        return copy_of(w_rec.at[0, :, pl.ds(pl.multiple_of(g * hidden + j * bw, 128), bw)], wtmp.at[slot], wt_sem.at[slot])

    def part_of(t):
        return lax.rem(t + WIN, WIN)

    def wi_copies(t, hf):
        first_row = pl.multiple_of(part_of(t) * quarter, 8)
        return [copy_of(w_in.at[0, pl.ds(first_row, quarter), pl.ds(g * hidden + hf * hw, hw)],
                        wi.at[hf, :, pl.ds(g * hw, hw)], wi_sem.at[hf, g]) for g in range(4)]

    def g_copy(t, hf):
        return copy_of(gates.at[t, pl.ds(hf * half, half)], gin.at[pl.ds(hf * half, half)], g_sem.at[hf])

    def c_copy(i):
        slot = lax.rem(i, 3)
        return copy_of(cseq.at[i], cring.at[slot], c_sem.at[slot])

    def own_copies(t):
        return [copy_of(hseq.at[:, t + 1, :, pl.ds(q * quarter, quarter)], dbuf.at[lax.rem(t, 2), q], d_sem.at[q]) for q in range(WIN)]

    def y_copy(t):
        return copy_of(tseq.at[:, t], ybuf.at[lax.rem(t, 2)], y_sem.at[0])

    def recv_copies(t):
        return [copy_of(drecv.at[q, t + pad], dbuf.at[lax.rem(t, 2), q], d_sem.at[q]) for q in range(WIN)]

    def dz_copies(t):
        slot = lax.rem(t, ring)
        return [copy_of(dzr.at[slot, hf, :, :, pl.ds(g * hw, hw)], dz_out.at[:, t, :, pl.ds(g * hidden + hf * hw, hw)],
                        dz_sem.at[slot, 4 * hf + g]) for hf in range(2) for g in range(4)]

    def send(t):
        return pltpu.make_async_remote_copy(
            src_ref=dust.at[0], dst_ref=drecv.at[part_of(t), pl.ds(t + pad, WIN)],
            send_sem=send_sem.at[0], recv_sem=recv_sem.at[t + pad],
            device_id={"stage": lax.rem(stage + n_stages - 1, n_stages)}, device_id_type=MESH)

    def fetch_d(t):
        @pl.when(top)
        def _():
            for c in own_copies(t):
                c.start()
            y_copy(t).start()

        @pl.when(jnp.logical_not(top))
        def _():
            send(t - pad).wait_recv()
            for c in recv_copies(t):
                c.start()

    def await_d(t):
        for c in recv_copies(t):
            c.wait()

        @pl.when(top)
        def _():
            y_copy(t).wait()

    def input_grad(t, hf):
        d = jnp.concatenate([dzr[lax.rem(t + i + ring, ring), hf].reshape(rows, 2 * hidden) for i in range(WIN)], axis=0)
        du = lax.dot_general(d, wi[hf], (((1,), (1,)), ((), ())), preferred_element_type=f32)
        if hf == 0:
            duacc[...] = du
        else:
            du = (du + duacc[...]).astype(bf16)
            for i in range(WIN):
                dust[0, i] = du[i * rows:(i + 1) * rows].reshape(n_groups, GROUP, quarter)

    def flat(x):
        return x.reshape(rows, x.shape[-1])

    def fold(x):
        return x.reshape(rows // 8, 8, x.shape[-1]).sum(axis=0)

    def recur(t, hf):
        cur, nxt = lax.rem(t, 2), lax.rem(t + 1, 2)
        slot = cur
        live = lens[...] > t
        sc = scale[0:1, :bw]
        total = None
        for j in range(hf * half, (hf + 1) * half):
            cols = slice(j * bw, (j + 1) * bw)
            q, off = j * bw // quarter, j * bw % quarter
            gi, gf = gin[j, :, :bw], gin[j, :, bw:2 * bw]
            gg, go = gin[j, :, 2 * bw:3 * bw], gin[j, :, 3 * bw:]
            err = jnp.where(live, flat(dbuf[slot, q, :, :, off:off + bw]).astype(f32) - flat(ybuf[slot, :, :, cols]).astype(f32), 0.0)
            lossacc[:, cols] += fold(err * err)
            d_total = dh[cur, :, cols] + err * sc
            c_prev = cring[lax.rem(t, 3), :, cols]
            tanh_c = jnp.tanh(cring[lax.rem(t + 1, 3), :, cols])
            dc_old = dc[:, cols]
            d_c = dc_old + d_total * go * (1.0 - tanh_c * tanh_c)
            parts = (d_c * gg * gi * (1.0 - gi),
                     d_c * c_prev * gf * (1.0 - gf),
                     d_c * gi * (1.0 - gg * gg),
                     d_total * tanh_c * go * (1.0 - go))
            low = []
            for g in range(4):
                dz = jnp.where(live, parts[g], 0.0)
                dbacc[j, :, g * bw:(g + 1) * bw] += fold(dz)
                dz = dz.astype(bf16)
                at = g * hw + (j - hf * half) * bw
                dzr[lax.rem(t, ring), hf, :, :, at:at + bw] = dz.reshape(n_groups, GROUP, bw)
                low.append(dz)
            dc[:, cols] = jnp.where(live, d_c * gf, dc_old)
            keep = jnp.where(live, 0.0, d_total)
            if hf == 0:
                dh[nxt, :, cols] = keep
            else:
                dh[nxt, :, cols] += keep
            low = jnp.concatenate(low, axis=1)
            low = jnp.concatenate([low, low[:rows // 2]], axis=0)
            r = jnp.dot(low, wt[j], preferred_element_type=f32)
            total = r if total is None else total + r
        total = jnp.concatenate([jnp.maximum(total[:rows // 2], total[rows:]), total[rows // 2:rows]], axis=0)
        if hf == 0:
            dh[nxt, :, :hw] += total[:, :hw]
            dh[nxt, :, hw:] = total[:, hw:]
        else:
            dh[nxt] += total

    last = steps - 1
    for c in wi_copies(last, 0):
        c.start()
    wt_copy(0, 0).start()
    g_copy(last, 0).start()
    c_copy(last + 1).start()
    c_copy(last).start()
    dh[...] = jnp.zeros_like(dh)
    dc[...] = jnp.zeros_like(dc)
    dbacc[...] = jnp.zeros_like(dbacc)
    lossacc[...] = jnp.zeros_like(lossacc)
    ybuf[...] = jnp.zeros_like(ybuf)
    for i in range(ring):
        dzr[i] = jnp.zeros_like(dzr[i])

    def load_wt(p, _):
        slot = lax.rem(p, 2)

        @pl.when(p + 1 < 4 * NB)
        def _():
            wt_copy(p + 1, 1 - slot).start()

        wt_copy(p, slot).wait()
        j, g = p // 4, lax.rem(p, 4)
        wt[j, pl.ds(pl.multiple_of(g * bw, 8), bw), :] = wtmp[slot].T
        return 0

    lax.fori_loop(0, 4 * NB, load_wt, 0)

    @pl.when(jnp.logical_not(top))
    def _():
        for i in range(pad):
            send(last - i).wait_recv()

    fetch_d(last)
    c_copy(last + 1).wait()

    def step(v, _):
        t = last - v
        await_d(t)
        g_copy(t, 0).wait()
        c_copy(t).wait()
        for c in wi_copies(t, 0):
            c.wait()

        @pl.when(v >= ring)
        def _():
            for c in dz_copies(t + ring):
                c.wait()

        g_copy(t, 1).start()
        for c in wi_copies(t, 1):
            c.start()

        @pl.when(t >= 1)
        def _():
            c_copy(t - 1).start()

        recur(t, 0)
        input_grad(t, 0)

        g_copy(t, 1).wait()
        for c in wi_copies(t, 1):
            c.wait()

        @pl.when(jnp.logical_and(v >= 1, sends))
        def _():
            send(t + 1).wait_send()

        for c in wi_copies(t - 1, 0):
            c.start()

        @pl.when(t >= 1)
        def _():
            g_copy(t - 1, 0).start()
            fetch_d(t - 1)

        recur(t, 1)
        input_grad(t, 1)
        for c in dz_copies(t):
            c.start()

        @pl.when(sends)
        def _():
            send(t).start()

        return 0

    lax.fori_loop(0, steps, step, 0)

    for i in range(ring):
        for c in dz_copies(i):
            c.wait()
    outs = [copy_of(dh.at[1], dh_out, out_sem.at[0]), copy_of(dc, dc_out, out_sem.at[1]),
            copy_of(dbacc, db_out, out_sem.at[2])]
    for c in outs:
        c.start()

    def tell(other):
        return pltpu.make_async_remote_copy(
            src_ref=lsend, dst_ref=lrecv, send_sem=lsend_sem.at[other], recv_sem=lrecv_sem.at[0],
            device_id={"stage": other}, device_id_type=MESH)

    @pl.when(top)
    def _():
        lsend[...] = sum(lossacc[:, i * 128:(i + 1) * 128] for i in range(hidden // 128))

    for c in wi_copies(-1, 0):
        c.wait()

    @pl.when(top)
    def _():
        for other in range(n_stages - 1):
            tell(other).start()
        lrecv[...] = lsend[...]

    @pl.when(sends)
    def _():
        for c in wi_copies(-1, 0):
            c.start()

        def drain(v, _):
            t = -1 - v
            for c in wi_copies(t, 0):
                c.wait()
            for c in wi_copies(t, 1):
                c.start()
            input_grad(t, 0)
            for c in wi_copies(t, 1):
                c.wait()

            @pl.when(v < pad - 1)
            def _():
                for c in wi_copies(t - 1, 0):
                    c.start()

            send(t + 1).wait_send()
            input_grad(t, 1)
            send(t).start()
            return 0

        lax.fori_loop(0, pad, drain, 0)
        send(-pad).wait_send()

    @pl.when(top)
    def _():
        for other in range(n_stages - 1):
            tell(other).wait_send()

    @pl.when(jnp.logical_not(top))
    def _():
        tell(0).wait_recv()

    loss_copy = copy_of(lrecv, loss_out, out_sem.at[3])
    loss_copy.start()
    loss_copy.wait()
    for c in outs:
        c.wait()


def run_backward(n_stages, hseq, tseq, gates, cseq, w_in, w_rec, lens, scale):
    n_groups, steps, _, hidden = tseq.shape
    rows = n_groups * GROUP
    bw = hidden // NB
    quarter = hidden // WIN
    any_spec = pl.BlockSpec(memory_space=pl.ANY)
    vmem_spec = pl.BlockSpec(memory_space=pltpu.VMEM)
    dma = pltpu.SemaphoreType.DMA
    return pl.pallas_call(
        functools.partial(backward_kernel, n_stages, steps, rows, hidden),
        out_shape=(jax.ShapeDtypeStruct((WIN, steps + 2 * (WIN - 1), n_groups, GROUP, quarter), bf16),
                   jax.ShapeDtypeStruct((n_groups, steps, GROUP, 4 * hidden), bf16),
                   jax.ShapeDtypeStruct((rows, hidden), f32),
                   jax.ShapeDtypeStruct((rows, hidden), f32),
                   jax.ShapeDtypeStruct((NB, 8, 4 * bw), f32),
                   jax.ShapeDtypeStruct((8, 128), f32)),
        in_specs=[any_spec] * 6 + [vmem_spec] * 2,
        out_specs=(any_spec,) * 6,
        scratch_shapes=[
            pltpu.VMEM((NB, 4 * bw, hidden), bf16),
            pltpu.VMEM((2, quarter, 2 * hidden), bf16),
            pltpu.VMEM((2, hidden, bw), bf16),
            pltpu.VMEM((NB, rows, 4 * bw), f32),
            pltpu.VMEM((3, rows, hidden), f32),
            pltpu.VMEM((2, WIN, n_groups, GROUP, quarter), bf16),
            pltpu.VMEM((2, n_groups, GROUP, hidden), bf16),
            pltpu.VMEM((WIN + 1, 2, n_groups, GROUP, 2 * hidden), bf16),
            pltpu.VMEM((2, rows, hidden), f32),
            pltpu.VMEM((rows, hidden), f32),
            pltpu.VMEM((NB, 8, 4 * bw), f32),
            pltpu.VMEM((8, hidden), f32),
            pltpu.VMEM((WIN * rows, quarter), f32),
            pltpu.VMEM((1, WIN, n_groups, GROUP, quarter), bf16),
            pltpu.VMEM((8, 128), f32),
            pltpu.VMEM((8, 128), f32),
            dma((2,)), dma((2, 4)), dma((2,)), dma((3,)), dma((WIN,)), dma((1,)), dma((WIN + 1, 8)), dma((4,)), dma((1,)),
            dma((steps + WIN - 1,)), dma((n_stages - 1,)), dma((1,)),
        ],
        compiler_params=pltpu.CompilerParams(collective_id=1, has_side_effects=True, vmem_limit_bytes=VMEM_LIMIT),
        name="lstm_backward",
    )(hseq, tseq, gates, cseq, w_in, w_rec, lens, scale)


def grads_kernel(steps, hidden, spans, useq, hseq, dz, g_in, g_rec, xt, xs, dzb, acc, x_sem, z_sem, o_sem):
    n_groups = useq.shape[0]
    chunk = xs.shape[-1]
    tile = dzb.shape[-1]
    n_tiles = dz.shape[-1] // tile
    n_chunks = hidden // chunk
    seen = [spans[i] for i in range(n_groups)]
    first = [0]
    for i in range(n_groups):
        first.append(first[-1] + seen[i])
    total = first[-1]
    sizes = []
    size = 1
    while size <= steps:
        sizes.insert(0, size)
        size *= 2

    def pieces(make, act):
        for i in range(n_groups):
            for size in sizes:
                done = seen[i] // (2 * size) * (2 * size)

                @pl.when(seen[i] // size % 2 == 1)
                def _(i=i, size=size, done=done):
                    act(make(i, pl.ds(done, size), pl.ds(first[i] + done, size)))

    def load_x(src, c, slot, act):
        cols = pl.ds(pl.multiple_of(c * chunk, chunk), chunk)
        pieces(lambda i, at, to: copy_of(src.at[i, at, :, cols], xs.at[slot, to], x_sem.at[slot]), act)

    def load_z(n, slot, act):
        cols = pl.ds(pl.multiple_of(n * tile, tile), tile)
        pieces(lambda i, at, to: copy_of(dz.at[i, at, :, cols], dzb.at[slot, to], z_sem.at[slot]), act)

    def start(c):
        c.start()

    def wait(c):
        c.wait()

    def store(w, n):
        dst = g_in if w == 0 else g_rec
        return copy_of(acc.at[w], dst.at[0, :, pl.ds(pl.multiple_of(n * tile, tile), tile)], o_sem.at[w])

    for slot in range(2):
        xs[slot, pl.ds(total, 64)] = jnp.zeros((64, GROUP, chunk), bf16)
        dzb[slot, pl.ds(total, 64)] = jnp.zeros((64, GROUP, tile), bf16)
    load_z(0, 0, start)
    for w, src in enumerate((useq, hseq)):
        load_x(src, 0, 0, start)

        def turn(c, _, w=w, src=src):
            slot = lax.rem(c, 2)

            @pl.when(c + 1 < n_chunks)
            def _():
                load_x(src, c + 1, 1 - slot, start)

            load_x(src, c, slot, wait)

            def block(b, _):
                x = xs[slot, pl.ds(b * 32, 32)].reshape(32 * GROUP, chunk)
                xt[w, pl.ds(pl.multiple_of(c * chunk, chunk), chunk), pl.ds(pl.multiple_of(b * 512, 512), 512)] = x.T
                return 0

            lax.fori_loop(0, (total + 31) // 32, block, 0)
            return 0

        lax.fori_loop(0, n_chunks, turn, 0)

    def product(w, slot, at, depth, begin):
        rhs = dzb[slot, pl.ds(at, depth)].reshape(depth * GROUP, tile)
        mc = min(512, hidden)
        for m in range(hidden // mc):
            lhs = xt[w, m * mc:(m + 1) * mc, pl.ds(pl.multiple_of(at * GROUP, 256), depth * GROUP)]
            r = jnp.dot(lhs, rhs, preferred_element_type=f32)
            acc[w, m * mc:(m + 1) * mc] = r if begin else acc[w, m * mc:(m + 1) * mc] + r

    def one_tile(n, _):
        slot = lax.rem(n, 2)

        @pl.when(n + 1 < n_tiles)
        def _():
            load_z(n + 1, 1 - slot, start)

        load_z(n, slot, wait)
        units = (total + 15) // 16
        for w in range(2):
            @pl.when(n >= 1)
            def _():
                store(w, n).wait()

            product(w, slot, 0, 64, True)

            def more(b, _):
                product(w, slot, b * 64, 64, False)
                return 0

            lax.fori_loop(1, units // 4, more, 0)

            @pl.when(units // 2 % 2 == 1)
            def _():
                product(w, slot, units // 4 * 64, 32, False)

            @pl.when(units % 2 == 1)
            def _():
                product(w, slot, units // 2 * 32, 16, False)

            store(w, n).start()
        return 0

    lax.fori_loop(0, n_tiles, one_tile, 0)
    for w in range(2):
        store(w, 0).wait()


def run_grads(useq, hseq, dz, spans):
    n_groups, steps, _, hidden = useq.shape
    any_spec = pl.BlockSpec(memory_space=pl.ANY)
    blocks = n_groups * steps + 64
    chunk, tile = 256, 512
    dma = pltpu.SemaphoreType.DMA
    out = jax.ShapeDtypeStruct((1, hidden, 4 * hidden), f32)
    return pl.pallas_call(
        functools.partial(grads_kernel, steps, hidden),
        out_shape=(out, out),
        in_specs=[pl.BlockSpec(memory_space=pltpu.SMEM)] + [any_spec] * 3,
        out_specs=(any_spec, any_spec),
        scratch_shapes=[
            pltpu.VMEM((2, hidden, n_groups * steps * GROUP), bf16),
            pltpu.VMEM((2, blocks, GROUP, chunk), bf16),
            pltpu.VMEM((2, blocks, GROUP, tile), bf16),
            pltpu.VMEM((2, hidden, tile), f32),
            dma((2,)), dma((2,)), dma((2,)),
        ],
        compiler_params=pltpu.CompilerParams(vmem_limit_bytes=VMEM_LIMIT),
        name="lstm_weight_grads",
    )(spans, useq, hseq, dz)


def solution(mesh):
    n_stages = mesh.shape["stage"]

    def local_program(inputs, targets, lengths, w_in, w_rec, gate_bias, h_init, c_init):
        rows, steps, hidden = inputs.shape
        bw = hidden // NB
        is_last = lax.axis_index("stage") == n_stages - 1
        n_active = jnp.sum(lengths).astype(f32)
        lens = jnp.broadcast_to(lengths[:, None], (rows, bw))
        bias = gate_bias.reshape(4, 2, hidden // 2).transpose(1, 0, 2).reshape(8, hidden // 2)
        useq, tseq = run_prepare(n_stages, inputs, targets)
        useq, hseq, gates, cseq = run_forward(n_stages, useq, w_in, w_rec, bias, h_init[0], c_init[0], lens)
        scale = jnp.broadcast_to(jnp.where(is_last, 1.0 / n_active, 1.0), (8, 2 * bw))
        _, dz, dh0, dc0, db, sq = run_backward(n_stages, hseq, tseq, gates, cseq, w_in, w_rec, lens, scale)
        loss = jnp.sum(sq) / (2.0 * n_active)
        grad_in, grad_rec = run_grads(useq, hseq, dz, lengths[::GROUP])
        grad_bias = db.sum(axis=1).reshape(NB, 4, bw).transpose(1, 0, 2).reshape(1, 4 * hidden)
        return loss.reshape(1), grad_in, grad_rec, grad_bias, dh0[None], dc0[None]

    row_spec = P("data", None, None)
    layer_spec = P("stage", None, None)
    state_spec = P("stage", "data", None)
    grad_spec = P(("data", "stage"), None, None)
    return jax.shard_map(local_program, mesh=mesh,
                         in_specs=(row_spec, row_spec, P("data"), layer_spec, layer_spec, P("stage", None), state_spec, state_spec),
                         out_specs=(P("data"), grad_spec, grad_spec, P(("data", "stage"), None), state_spec, state_spec),
                         check_vma=False)
```

```python
import functools

import jax
import jax.numpy as jnp
from jax import lax
from jax.experimental import pallas as pl
from jax.experimental.pallas import tpu as pltpu
from jax.sharding import PartitionSpec as P

MESH = pl.DeviceIdType.MESH
NB = 8
WIN = 2
GROUP = 16
VMEM_LIMIT = 67043328
f32 = jnp.float32
bf16 = jnp.bfloat16


def sigmoid(x):
    return 0.5 * jnp.tanh(0.5 * x) + 0.5


def copy_of(src, dst, sem):
    return pltpu.make_async_copy(src, dst, sem)


def entry_barrier(stage, n_stages):
    barrier = pltpu.get_barrier_semaphore()
    for step in range(1, n_stages):
        pl.semaphore_signal(barrier, inc=1, device_id={"stage": lax.rem(stage + step, n_stages)}, device_id_type=MESH)
    pl.semaphore_wait(barrier, n_stages - 1)


def fill_lens(spans, lens):
    for r in range(lens.shape[0]):
        lens[r:r + 1, :] = jnp.full((1, lens.shape[1]), spans[r], jnp.int32)


def turn_weights(w_in, w_rec, win_t, wrec_t, src, dst, in_sem, out_sem):
    hidden = w_rec.shape[1]
    bw = hidden // NB
    per_half = NB // 2
    n_parts = win_t.shape[1]
    part = hidden // n_parts
    n_slots = src.shape[0]

    def load(i):
        slot = lax.rem(i, n_slots)
        j, g = lax.rem(i, 4 * NB) // 4, lax.rem(i, 4)
        cols = pl.ds(pl.multiple_of(g * hidden + j * bw, 128), bw)
        return (copy_of(w_rec.at[0, :, cols], src.at[slot], in_sem.at[slot]),
                copy_of(w_in.at[0, :, cols], src.at[slot], in_sem.at[slot]))

    def save(i):
        slot = lax.rem(i, n_slots)
        j, g = lax.rem(i, 4 * NB) // 4, lax.rem(i, 4)
        rec = copy_of(dst.at[slot], wrec_t.at[j, pl.ds(pl.multiple_of(g * bw, 8), bw)], out_sem.at[slot, 0])
        at = pl.multiple_of(g * per_half * bw + lax.rem(j, per_half) * bw, 8)
        ins = [copy_of(dst.at[slot, :, pl.ds(q * part, part)], win_t.at[j // per_half, q, pl.ds(at, bw)], out_sem.at[slot, q])
               for q in range(n_parts)]
        return [rec], ins

    units = 8 * NB

    def both(i, rec_do, in_do):
        @pl.when(i < 4 * NB)
        def _():
            rec_do()

        @pl.when(i >= 4 * NB)
        def _():
            in_do()

    def start_load(i):
        both(i, lambda: load(i)[0].start(), lambda: load(i)[1].start())

    def each_save(i, act):
        both(i, lambda: [act(c) for c in save(i)[0]], lambda: [act(c) for c in save(i)[1]])

    for i in range(n_slots):
        start_load(i)

    def unit(i, _):
        slot = lax.rem(i, n_slots)
        load(i)[0].wait()

        @pl.when(i >= n_slots)
        def _():
            each_save(i - n_slots, lambda c: c.wait())

        dst[slot] = src[slot].T
        each_save(i, lambda c: c.start())

        @pl.when(i + n_slots < units)
        def _():
            start_load(i + n_slots)

        return 0

    lax.fori_loop(0, units, unit, 0)
    for i in range(units - n_slots, units):
        each_save(i, lambda c: c.wait())


def early_turn(n_stages, stage):
    return stage >= n_stages // 2


def prepare_kernel(n_stages, inputs, targets, w_in, w_rec, useq, tseq, win_t, wrec_t,
                   src, dst, wsrc, wdst, in_sem, out_sem, win_sem, wout_sem):
    rows, steps, _ = inputs.shape
    stage = lax.axis_index("stage")
    n_slots = src.shape[0]
    n_cols = steps // GROUP
    units = rows // GROUP * n_cols

    def turn(x, y):
        def load(i):
            slot = lax.rem(i, n_slots)
            return copy_of(x.at[pl.ds(pl.multiple_of(i // n_cols * GROUP, GROUP), GROUP),
                                pl.ds(pl.multiple_of(lax.rem(i, n_cols) * GROUP, GROUP), GROUP)], src.at[slot], in_sem.at[slot])

        def save(i):
            slot = lax.rem(i, n_slots)
            return copy_of(dst.at[slot], y.at[i // n_cols, pl.ds(lax.rem(i, n_cols) * GROUP, GROUP)], out_sem.at[slot])

        for i in range(min(n_slots, units)):
            load(i).start()

        def unit(i, _):
            slot = lax.rem(i, n_slots)
            load(i).wait()

            @pl.when(i >= n_slots)
            def _():
                save(i).wait()

            dst[slot] = jnp.swapaxes(src[slot], 0, 1)
            save(i).start()

            @pl.when(i + n_slots < units)
            def _():
                load(i + n_slots).start()

            return 0

        lax.fori_loop(0, units, unit, 0)
        for i in range(max(0, units - n_slots), units):
            save(i).wait()

    @pl.when(stage == 0)
    def _():
        turn(inputs, useq)

    @pl.when(stage == n_stages - 1)
    def _():
        turn(targets, tseq)

    @pl.when(early_turn(n_stages, stage))
    def _():
        turn_weights(w_in, w_rec, win_t, wrec_t, wsrc, wdst, win_sem, wout_sem)


def weight_scratch(hidden):
    dma = pltpu.SemaphoreType.DMA
    slots = 4
    return ([pltpu.VMEM((slots, hidden, hidden // NB), bf16), pltpu.VMEM((slots, hidden // NB, hidden), bf16)],
            [dma((slots,)), dma((slots, WIN))])


def run_prepare(n_stages, inputs, targets, w_in, w_rec):
    rows, steps, hidden = inputs.shape
    any_spec = pl.BlockSpec(memory_space=pl.ANY)
    dma = pltpu.SemaphoreType.DMA
    seq = jax.ShapeDtypeStruct((rows // GROUP, steps, GROUP, hidden), bf16)
    buffers, sems = weight_scratch(hidden)
    return pl.pallas_call(
        functools.partial(prepare_kernel, n_stages),
        out_shape=(seq, seq, jax.ShapeDtypeStruct((2, WIN, 2 * hidden, hidden // WIN), bf16),
                   jax.ShapeDtypeStruct((NB, hidden // 2, hidden), bf16)),
        in_specs=[any_spec] * 4, out_specs=(any_spec,) * 4,
        scratch_shapes=[pltpu.VMEM((4, GROUP, GROUP, hidden), bf16), pltpu.VMEM((4, GROUP, GROUP, hidden), bf16), *buffers,
                        dma((4,)), dma((4,)), *sems],
        compiler_params=pltpu.CompilerParams(vmem_limit_bytes=VMEM_LIMIT),
        name="lstm_prepare",
    )(inputs, targets, w_in, w_rec)


def late_turn_kernel(n_stages, w_in, w_rec, after, win_old, wrec_old, win_t, wrec_t, wsrc, wdst, win_sem, wout_sem):
    del after, win_old, wrec_old

    @pl.when(jnp.logical_not(early_turn(n_stages, lax.axis_index("stage"))))
    def _():
        turn_weights(w_in, w_rec, win_t, wrec_t, wsrc, wdst, win_sem, wout_sem)


def run_late_turn(n_stages, w_in, w_rec, after, win_t, wrec_t):
    any_spec = pl.BlockSpec(memory_space=pl.ANY)
    buffers, sems = weight_scratch(w_rec.shape[1])
    return pl.pallas_call(
        functools.partial(late_turn_kernel, n_stages),
        out_shape=(jax.ShapeDtypeStruct(win_t.shape, bf16), jax.ShapeDtypeStruct(wrec_t.shape, bf16)),
        in_specs=[any_spec] * 5, out_specs=(any_spec,) * 2, input_output_aliases={3: 0, 4: 1},
        scratch_shapes=[*buffers, *sems],
        compiler_params=pltpu.CompilerParams(vmem_limit_bytes=VMEM_LIMIT),
        name="lstm_late_turn",
    )(w_in, w_rec, after, win_t, wrec_t)


def forward_kernel(n_stages, steps, rows, hidden,
                   seq_ref, w_in, w_rec, bias, h_start, c_start, spans,
                   useq, hseq, gates, cseq,
                   wr, wi, uring, zin, gst, cst, hst, lens,
                   wr_sem, wi_sem, u_sem, g_sem, c_sem, h_sem, send_sem, recv_sem):
    bw = hidden // NB
    half = NB // 2
    hw = half * bw
    per = 4 // WIN
    stage = lax.axis_index("stage")
    first = stage == 0
    sends = stage < n_stages - 1
    entry_barrier(stage, n_stages)

    def wr_copies():
        return [copy_of(w_rec.at[0, :, pl.ds(g * hidden + j * bw, bw)], wr.at[j, :, pl.ds(g * bw, bw)], wr_sem.at[j, g])
                for j in range(NB) for g in range(4)]

    def gate_of(t, i):
        return lax.rem(t + WIN, WIN) * per + i

    def wi_copies(t, slot):
        return [copy_of(w_in.at[0, :, pl.ds(pl.multiple_of(gate_of(t, i) * hidden + (1 - slot) * hw, 128), hw)],
                        wi.at[slot, i], wi_sem.at[slot]) for i in range(per)]

    def await_wi(slot):
        copy_of(wi.at[slot], wi.at[slot], wi_sem.at[slot]).wait()

    def u_copy(t):
        slot = lax.rem(t, WIN + 1)
        return copy_of(useq.at[:, t], uring.at[slot], u_sem.at[0])

    def g_copy(t, hf):
        return copy_of(gst.at[pl.ds(hf * half, half)], gates.at[t, pl.ds(hf * half, half)], g_sem.at[hf])

    def c_copy(slot, t):
        return copy_of(cst.at[slot], cseq.at[t], c_sem.at[slot])

    def h_copy(slot, t):
        return copy_of(hst.at[slot], hseq.at[:, t], h_sem.at[slot])

    def send(slot, t):
        return pltpu.make_async_remote_copy(
            src_ref=hst.at[slot], dst_ref=useq.at[:, t], send_sem=send_sem.at[slot], recv_sem=recv_sem.at[t],
            device_id={"stage": lax.rem(stage + 1, n_stages)}, device_id_type=MESH)

    def fetch_u(t):
        @pl.when(t < steps)
        def _():
            @pl.when(jnp.logical_not(first))
            def _():
                send(0, t).wait_recv()
            u_copy(t).start()

    def await_u(t):
        @pl.when(t < steps)
        def _():
            u_copy(t).wait()

    def project(t, t0, slot):
        u = jnp.concatenate([uring[lax.rem(t0 + i + 2 * (WIN + 1), WIN + 1)].reshape(rows, hidden) for i in range(WIN)], axis=0)
        for i in range(per):
            g = gate_of(t, i)
            z = jnp.dot(u, wi[slot, i], preferred_element_type=f32)
            z += bias[0:1, pl.ds(pl.multiple_of(g * hidden + (1 - slot) * hw, 128), hw)]
            for k in range(WIN):
                zin[4 * (1 - slot) + g, lax.rem(t0 + k + 2 * WIN, WIN)] = z[k * rows:(k + 1) * rows]

    def recur(t, hf, then):
        cur, nxt = lax.rem(t, 2), lax.rem(t + 1, 2)
        live = lens[...] > t
        h = hst[cur].reshape(rows, hidden)
        h_twice = jnp.concatenate([h, h], axis=0)
        for j in range(hf * half, (hf + 1) * half):
            cols = slice(j * bw, (j + 1) * bw)
            if j == hf * half + half - 1:
                then()
            z = jnp.dot(h_twice, wr[j], preferred_element_type=f32)
            z = jnp.maximum(z[:rows], z[rows:])
            at = (j - hf * half) * bw
            zi, zf, zg, zo = (z[:, g * bw:(g + 1) * bw] + zin[4 * hf + g, lax.rem(t, WIN), :, at:at + bw] for g in range(4))
            gi = sigmoid(zi)
            gf = sigmoid(zf)
            gg = jnp.tanh(zg)
            go = sigmoid(zo)
            c_prev = cst[cur, :, cols]
            c_new = gf * c_prev + gi * gg
            h_new = go * jnp.tanh(c_new)
            cst[nxt, :, cols] = jnp.where(live, c_new, c_prev)
            hst[nxt, :, :, cols] = jnp.where(live, h_new, h[:, cols].astype(f32)).astype(bf16).reshape(rows // GROUP, GROUP, bw)
            gst[j, :, :bw] = gi
            gst[j, :, bw:2 * bw] = gf
            gst[j, :, 2 * bw:3 * bw] = gg
            gst[j, :, 3 * bw:] = go

    for c in wi_copies(-WIN, 1):
        c.start()
    for c in wr_copies():
        c.start()
    fill_lens(spans, lens)
    hst[0] = h_start[0].astype(bf16).reshape(rows // GROUP, GROUP, hidden)
    cst[0] = c_start[0]
    c_copy(0, 0).start()
    h_copy(0, 0).start()

    def warm(v, _):
        t = v - WIN
        fetch_u(t + WIN)

        @pl.when(v > 0)
        def _():
            await_wi(0)
            for c in wi_copies(t, 1):
                c.start()
            project(t, t, 0)

        await_wi(1)
        await_u(t + WIN)
        for c in wi_copies(t + 1, 0):
            c.start()
        project(t, t + 1, 1)
        return 0

    lax.fori_loop(0, WIN, warm, 0)
    for c in wr_copies():
        c.wait()

    def step(t, _):
        nxt = lax.rem(t + 1, 2)
        fetch_u(t + WIN)
        for c in wi_copies(t, 1):
            c.start()

        @pl.when(t >= 1)
        def _():
            c_copy(nxt, t).wait()
            h_copy(nxt, t).wait()
            g_copy(t, 0).wait()

        @pl.when(jnp.logical_and(t >= 2, sends))
        def _():
            send(nxt, t).wait_send()

        recur(t, 0, lambda: await_wi(0))
        project(t, t, 0)

        g_copy(t, 0).start()

        @pl.when(t + 1 < steps)
        def _():
            for c in wi_copies(t + 1, 0):
                c.start()

        await_u(t + WIN)

        @pl.when(t >= 1)
        def _():
            g_copy(t, 1).wait()

        recur(t, 1, lambda: await_wi(1))
        project(t, t + 1, 1)

        g_copy(t, 1).start()
        c_copy(nxt, t + 1).start()
        h_copy(nxt, t + 1).start()

        @pl.when(sends)
        def _():
            send(nxt, t).start()

        return 0

    lax.fori_loop(0, steps, step, 0)
    for hf in range(2):
        g_copy(0, hf).wait()
        c_copy(hf, 0).wait()
        h_copy(hf, 0).wait()

        @pl.when(sends)
        def _():
            send(hf, 0).wait_send()


def run_forward(n_stages, seq, w_in, w_rec, bias, h_start, c_start, spans):
    n_groups, steps, _, hidden = seq.shape
    rows = n_groups * GROUP
    bw = hidden // NB
    any_spec = pl.BlockSpec(memory_space=pl.ANY)
    vmem_spec = pl.BlockSpec(memory_space=pltpu.VMEM)
    dma = pltpu.SemaphoreType.DMA
    return pl.pallas_call(
        functools.partial(forward_kernel, n_stages, steps, rows, hidden),
        out_shape=(jax.ShapeDtypeStruct((n_groups, steps, GROUP, hidden), bf16),
                   jax.ShapeDtypeStruct((n_groups, steps + 1, GROUP, hidden), bf16),
                   jax.ShapeDtypeStruct((steps, NB, rows, 4 * bw), f32),
                   jax.ShapeDtypeStruct((steps + 1, rows, hidden), f32)),
        in_specs=[any_spec, any_spec, any_spec, vmem_spec, vmem_spec, vmem_spec, pl.BlockSpec(memory_space=pltpu.SMEM)],
        out_specs=(any_spec,) * 4,
        input_output_aliases={0: 0},
        scratch_shapes=[
            pltpu.VMEM((NB, hidden, 4 * bw), bf16),
            pltpu.VMEM((2, 4 // WIN, hidden, hidden // 2), bf16),
            pltpu.VMEM((WIN + 1, n_groups, GROUP, hidden), bf16),
            pltpu.VMEM((8, WIN, rows, hidden // 2), f32),
            pltpu.VMEM((NB, rows, 4 * bw), f32),
            pltpu.VMEM((2, rows, hidden), f32),
            pltpu.VMEM((2, n_groups, GROUP, hidden), bf16),
            pltpu.VMEM((rows, bw), jnp.int32),
            dma((NB, 4)), dma((2,)), dma((1,)), dma((2,)), dma((2,)), dma((2,)), dma((2,)), dma((steps,)),
        ],
        compiler_params=pltpu.CompilerParams(collective_id=0, has_side_effects=True, vmem_limit_bytes=VMEM_LIMIT),
        name="lstm_forward",
    )(seq, w_in, w_rec, bias, h_start, c_start, spans)


def backward_kernel(n_stages, steps, rows, hidden,
                    hseq, tseq, gates, cseq, win_t, wrec_t, spans,
                    drecv, dz_out, dh_out, dc_out, db_out, loss_out,
                    wt, wi, gin, cring, dbuf, ybuf, dzr, dh, dc, dbacc, lossacc, duacc, dust, lsend, lrecv, lens, scale,
                    wt_sem, wi_sem, g_sem, c_sem, d_sem, y_sem, dz_sem, out_sem, send_sem, recv_sem, lsend_sem, lrecv_sem):
    bw = hidden // NB
    n_groups = rows // GROUP
    half = NB // 2
    hw = half * bw
    part = hidden // WIN
    ring = WIN + 1
    pad = WIN - 1
    stage = lax.axis_index("stage")
    top = stage == n_stages - 1
    sends = stage > 0
    entry_barrier(stage, n_stages)

    def wt_copies():
        return [copy_of(wrec_t.at[j], wt.at[j], wt_sem.at[j]) for j in range(NB)]

    def part_of(t):
        return lax.rem(t + WIN, WIN)

    def wi_copy(t, hf):
        return copy_of(win_t.at[hf, part_of(t)], wi.at[hf], wi_sem.at[hf])

    def g_copy(t, hf):
        return copy_of(gates.at[t, pl.ds(hf * half, half)], gin.at[pl.ds(hf * half, half)], g_sem.at[hf])

    def c_copy(i):
        slot = lax.rem(i, 3)
        return copy_of(cseq.at[i], cring.at[slot], c_sem.at[slot])

    def own_copies(t):
        return [copy_of(hseq.at[:, t + 1, :, pl.ds(q * part, part)], dbuf.at[lax.rem(t, 2), q], d_sem.at[q])
                for q in range(WIN)]

    def y_copy(t):
        return copy_of(tseq.at[:, t], ybuf.at[lax.rem(t, 2)], y_sem.at[0])

    def recv_copies(t):
        return [copy_of(drecv.at[q, t + pad], dbuf.at[lax.rem(t, 2), q], d_sem.at[q]) for q in range(WIN)]

    def dz_copies(t):
        slot = lax.rem(t, ring)
        return [copy_of(dzr.at[slot, hf, :, :, pl.ds(g * hw, hw)], dz_out.at[:, t, :, pl.ds(g * hidden + hf * hw, hw)],
                        dz_sem.at[slot, 4 * hf + g]) for hf in range(2) for g in range(4)]

    def send(t):
        return pltpu.make_async_remote_copy(
            src_ref=dust.at[0], dst_ref=drecv.at[part_of(t), pl.ds(t + pad, WIN)],
            send_sem=send_sem.at[0], recv_sem=recv_sem.at[t + pad],
            device_id={"stage": lax.rem(stage + n_stages - 1, n_stages)}, device_id_type=MESH)

    def fetch_d(t):
        @pl.when(top)
        def _():
            for c in own_copies(t):
                c.start()
            y_copy(t).start()

        @pl.when(jnp.logical_not(top))
        def _():
            send(t - pad).wait_recv()
            for c in recv_copies(t):
                c.start()

    def await_d(t):
        for c in recv_copies(t):
            c.wait()

        @pl.when(top)
        def _():
            y_copy(t).wait()

    def input_grad(t, hf):
        d = jnp.concatenate([dzr[lax.rem(t + i + ring, ring), hf].reshape(rows, 2 * hidden) for i in range(WIN)], axis=0)
        du = jnp.dot(d, wi[hf], preferred_element_type=f32)
        if hf == 0:
            duacc[...] = du
        else:
            du = (du + duacc[...]).astype(bf16)
            for i in range(WIN):
                dust[0, i] = du[i * rows:(i + 1) * rows].reshape(n_groups, GROUP, part)

    def flat(x):
        return x.reshape(rows, x.shape[-1])

    def fold(x):
        return x.reshape(rows // 8, 8, x.shape[-1]).sum(axis=0)

    def recur(t, hf, then):
        cur, nxt = lax.rem(t, 2), lax.rem(t + 1, 2)
        slot = cur
        live = lens[...] > t
        sc = scale[0:1, :]
        total = None
        for j in range(hf * half, (hf + 1) * half):
            cols = slice(j * bw, (j + 1) * bw)
            q, off = j * bw // part, j * bw % part
            if j == hf * half + half - 1:
                then()
            gi, gf = gin[j, :, :bw], gin[j, :, bw:2 * bw]
            gg, go = gin[j, :, 2 * bw:3 * bw], gin[j, :, 3 * bw:]
            err = jnp.where(live, flat(dbuf[slot, q, :, :, off:off + bw]).astype(f32) - flat(ybuf[slot, :, :, cols]).astype(f32), 0.0)
            lossacc[:, cols] += fold(err * err)
            d_total = dh[cur, :, cols] + err * sc
            c_prev = cring[lax.rem(t, 3), :, cols]
            tanh_c = jnp.tanh(cring[lax.rem(t + 1, 3), :, cols])
            dc_old = dc[:, cols]
            d_c = dc_old + d_total * go * (1.0 - tanh_c * tanh_c)
            gates_d = (d_c * gg * gi * (1.0 - gi),
                     d_c * c_prev * gf * (1.0 - gf),
                     d_c * gi * (1.0 - gg * gg),
                     d_total * tanh_c * go * (1.0 - go))
            low = []
            for g in range(4):
                dz = jnp.where(live, gates_d[g], 0.0)
                dbacc[j, :, g * bw:(g + 1) * bw] += fold(dz)
                dz = dz.astype(bf16)
                at = g * hw + (j - hf * half) * bw
                dzr[lax.rem(t, ring), hf, :, :, at:at + bw] = dz.reshape(n_groups, GROUP, bw)
                low.append(dz)
            dc[:, cols] = jnp.where(live, d_c * gf, dc_old)
            keep = jnp.where(live, 0.0, d_total)
            if hf == 0:
                dh[nxt, :, cols] = keep
            else:
                dh[nxt, :, cols] += keep
            low = jnp.concatenate(low, axis=1)
            low = jnp.concatenate([low, low], axis=0)
            r = jnp.dot(low, wt[j], preferred_element_type=f32)
            total = r if total is None else total + r
        total = jnp.maximum(total[:rows], total[rows:])
        if hf == 0:
            dh[nxt, :, :hw] += total[:, :hw]
            dh[nxt, :, hw:] = total[:, hw:]
        else:
            dh[nxt] += total

    last = steps - 1
    for c in wt_copies():
        c.start()
    wi_copy(last, 0).start()
    g_copy(last, 0).start()
    c_copy(last + 1).start()
    c_copy(last).start()
    fill_lens(spans, lens)
    n_active = spans[0]
    for r in range(1, rows):
        n_active += spans[r]
    share = 1.0 / jnp.full(scale.shape, n_active.astype(f32))
    scale[...] = jnp.where(top, share, 1.0)
    dh[...] = jnp.zeros_like(dh)
    dc[...] = jnp.zeros_like(dc)
    dbacc[...] = jnp.zeros_like(dbacc)
    lossacc[...] = jnp.zeros_like(lossacc)
    ybuf[...] = jnp.zeros_like(ybuf)
    for i in range(ring):
        dzr[i] = jnp.zeros_like(dzr[i])

    @pl.when(jnp.logical_not(top))
    def _():
        for i in range(pad):
            send(last - i).wait_recv()

    fetch_d(last)
    c_copy(last + 1).wait()
    for c in wt_copies():
        c.wait()

    def step(v, _):
        t = last - v
        await_d(t)
        g_copy(t, 0).wait()
        c_copy(t).wait()

        @pl.when(v >= ring)
        def _():
            for c in dz_copies(t + ring):
                c.wait()

        g_copy(t, 1).start()
        wi_copy(t, 1).start()

        @pl.when(t >= 1)
        def _():
            c_copy(t - 1).start()

        recur(t, 0, wi_copy(t, 0).wait)
        input_grad(t, 0)

        g_copy(t, 1).wait()

        @pl.when(jnp.logical_and(v >= 1, sends))
        def _():
            send(t + 1).wait_send()

        wi_copy(t - 1, 0).start()

        @pl.when(t >= 1)
        def _():
            g_copy(t - 1, 0).start()
            fetch_d(t - 1)

        recur(t, 1, wi_copy(t, 1).wait)
        input_grad(t, 1)
        for c in dz_copies(t):
            c.start()

        @pl.when(sends)
        def _():
            send(t).start()

        return 0

    lax.fori_loop(0, steps, step, 0)

    for i in range(ring):
        for c in dz_copies(i):
            c.wait()
    outs = [copy_of(dh.at[1], dh_out, out_sem.at[0]), copy_of(dc, dc_out, out_sem.at[1]),
            copy_of(dbacc, db_out, out_sem.at[2])]
    for c in outs:
        c.start()

    def tell(other):
        return pltpu.make_async_remote_copy(
            src_ref=lsend, dst_ref=lrecv, send_sem=lsend_sem.at[other], recv_sem=lrecv_sem.at[0],
            device_id={"stage": other}, device_id_type=MESH)

    @pl.when(top)
    def _():
        lsend[...] = sum(lossacc[:, i * 128:(i + 1) * 128] for i in range(hidden // 128))

    wi_copy(-1, 0).wait()

    @pl.when(top)
    def _():
        for other in range(n_stages - 1):
            tell(other).start()
        lrecv[...] = lsend[...]

    @pl.when(sends)
    def _():
        wi_copy(-1, 0).start()

        def drain(v, _):
            t = -1 - v
            wi_copy(t, 0).wait()
            wi_copy(t, 1).start()
            input_grad(t, 0)
            wi_copy(t, 1).wait()

            @pl.when(v < pad - 1)
            def _():
                wi_copy(t - 1, 0).start()

            send(t + 1).wait_send()
            input_grad(t, 1)
            send(t).start()
            return 0

        lax.fori_loop(0, pad, drain, 0)
        send(-pad).wait_send()

    @pl.when(top)
    def _():
        for other in range(n_stages - 1):
            tell(other).wait_send()

    @pl.when(jnp.logical_not(top))
    def _():
        tell(0).wait_recv()

    loss_copy = copy_of(lrecv, loss_out, out_sem.at[3])
    loss_copy.start()
    loss_copy.wait()
    for c in outs:
        c.wait()


def run_backward(n_stages, hseq, tseq, gates, cseq, win_t, wrec_t, spans):
    n_groups, steps, _, hidden = tseq.shape
    rows = n_groups * GROUP
    bw = hidden // NB
    part = hidden // WIN
    any_spec = pl.BlockSpec(memory_space=pl.ANY)
    dma = pltpu.SemaphoreType.DMA
    return pl.pallas_call(
        functools.partial(backward_kernel, n_stages, steps, rows, hidden),
        out_shape=(jax.ShapeDtypeStruct((WIN, steps + 2 * (WIN - 1), n_groups, GROUP, part), bf16),
                   jax.ShapeDtypeStruct((n_groups, steps, GROUP, 4 * hidden), bf16),
                   jax.ShapeDtypeStruct((rows, hidden), f32),
                   jax.ShapeDtypeStruct((rows, hidden), f32),
                   jax.ShapeDtypeStruct((NB, 8, 4 * bw), f32),
                   jax.ShapeDtypeStruct((8, 128), f32)),
        in_specs=[any_spec] * 6 + [pl.BlockSpec(memory_space=pltpu.SMEM)],
        out_specs=(any_spec,) * 6,
        scratch_shapes=[
            pltpu.VMEM((NB, 4 * bw, hidden), bf16),
            pltpu.VMEM((2, 2 * hidden, part), bf16),
            pltpu.VMEM((NB, rows, 4 * bw), f32),
            pltpu.VMEM((3, rows, hidden), f32),
            pltpu.VMEM((2, WIN, n_groups, GROUP, part), bf16),
            pltpu.VMEM((2, n_groups, GROUP, hidden), bf16),
            pltpu.VMEM((WIN + 1, 2, n_groups, GROUP, 2 * hidden), bf16),
            pltpu.VMEM((2, rows, hidden), f32),
            pltpu.VMEM((rows, hidden), f32),
            pltpu.VMEM((NB, 8, 4 * bw), f32),
            pltpu.VMEM((8, hidden), f32),
            pltpu.VMEM((WIN * rows, part), f32),
            pltpu.VMEM((1, WIN, n_groups, GROUP, part), bf16),
            pltpu.VMEM((8, 128), f32),
            pltpu.VMEM((8, 128), f32),
            pltpu.VMEM((rows, bw), jnp.int32),
            pltpu.VMEM((8, bw), f32),
            dma((NB,)), dma((2,)), dma((2,)), dma((3,)), dma((WIN,)), dma((1,)), dma((WIN + 1, 8)), dma((4,)), dma((1,)),
            dma((steps + WIN - 1,)), dma((n_stages - 1,)), dma((1,)),
        ],
        compiler_params=pltpu.CompilerParams(collective_id=1, has_side_effects=True, vmem_limit_bytes=VMEM_LIMIT),
        name="lstm_backward",
    )(hseq, tseq, gates, cseq, win_t, wrec_t, spans)


def grads_kernel(steps, hidden, spans, useq, hseq, dz, dh, dc, db, sq,
                 g_in, g_rec, g_bias, dh_out, dc_out, loss_out,
                 xs, dzb, acc, state, x_sem, z_sem, o_sem, s_sem):
    n_groups = useq.shape[0]
    tile = dzb.shape[-1]
    n_tiles = dz.shape[-1] // tile
    bw = hidden // NB
    seen = [spans[i * GROUP] for i in range(n_groups)]
    first = [0]
    for i in range(n_groups):
        first.append(first[-1] + seen[i])
    total = first[-1]
    sizes = []
    size = 1
    while size <= steps:
        sizes.insert(0, size)
        size *= 2

    def pieces(make, act):
        for i in range(n_groups):
            for size in sizes:
                done = seen[i] // (2 * size) * (2 * size)

                @pl.when(seen[i] // size % 2 == 1)
                def _(i=i, size=size, done=done):
                    act(make(i, pl.ds(done, size), pl.ds(first[i] + done, size)))

    def load_x(w, act):
        src = useq if w == 0 else hseq
        pieces(lambda i, at, to: copy_of(src.at[i, at], xs.at[w, to], x_sem.at[w]), act)

    def load_z(n, slot, act):
        cols = pl.ds(pl.multiple_of(n * tile, tile), tile)
        pieces(lambda i, at, to: copy_of(dz.at[i, at, :, cols], dzb.at[slot, to], z_sem.at[slot]), act)

    def start(c):
        c.start()

    def wait(c):
        c.wait()

    def store(w, n, act):
        cols = pl.ds(pl.multiple_of(n * tile, tile), tile)

        @pl.when(w == 0)
        def _():
            act(copy_of(acc.at[0], g_in.at[0, :, cols], o_sem.at[0]))

        @pl.when(w == 1)
        def _():
            act(copy_of(acc.at[1], g_rec.at[0, :, cols], o_sem.at[1]))

    for slot in range(2):
        xs[slot, pl.ds(total, GROUP)] = jnp.zeros((GROUP, GROUP, hidden), bf16)
        dzb[slot, pl.ds(total, GROUP)] = jnp.zeros((GROUP, GROUP, tile), bf16)
    load_z(0, 0, start)
    load_x(0, start)
    load_x(1, start)
    states = [(copy_of(x, state.at[i], s_sem.at[i]), copy_of(state.at[i], y.at[0], s_sem.at[i]))
              for i, (x, y) in enumerate(((dh, dh_out), (dc, dc_out)))]
    for c, _ in states:
        c.start()
    for j in range(NB):
        for g in range(4):
            g_bias[0:1, g * hidden + j * bw:g * hidden + (j + 1) * bw] = jnp.sum(
                db[j, :, g * bw:(g + 1) * bw], axis=0, keepdims=True)
    n_active = spans[0]
    for r in range(1, n_groups * GROUP):
        n_active += spans[r]
    loss_out[...] = jnp.full((1, 1), jnp.sum(sq[...]) / (2.0 * n_active.astype(f32)))

    def product(w, slot, at, depth, begin):
        rhs = dzb[slot, pl.ds(at, depth)].reshape(depth * GROUP, tile)
        mc = min(512, hidden)
        for m in range(hidden // mc):
            lhs = xs[w, pl.ds(at, depth), :, m * mc:(m + 1) * mc].reshape(depth * GROUP, mc)
            r = lax.dot_general(lhs, rhs, (((0,), (0,)), ((), ())), preferred_element_type=f32)
            acc[w, m * mc:(m + 1) * mc] = r if begin else acc[w, m * mc:(m + 1) * mc] + r

    units = (total + 15) // 16

    def one_tile(v, _):
        n, w = v // 2, lax.rem(v, 2)
        slot = lax.rem(n, 2)

        @pl.when(w == 0)
        def _():
            @pl.when(n + 1 < n_tiles)
            def _():
                load_z(n + 1, 1 - slot, start)

            load_z(n, slot, wait)

        @pl.when(v == 0)
        def _():
            load_x(0, wait)

        @pl.when(v == 1)
        def _():
            load_x(1, wait)

        @pl.when(n >= 1)
        def _():
            store(w, n, wait)

        product(w, slot, 0, 128, True)

        def more(b, _):
            product(w, slot, 128 + b * 64, 64, False)
            return 0

        rest = jnp.maximum(units - 8, 0)
        lax.fori_loop(0, rest // 4, more, 0)

        @pl.when(rest // 2 % 2 == 1)
        def _():
            product(w, slot, 128 + rest // 4 * 64, 32, False)

        @pl.when(rest % 2 == 1)
        def _():
            product(w, slot, 128 + rest // 2 * 32, 16, False)

        store(w, n, start)
        return 0

    lax.fori_loop(0, 2 * n_tiles, one_tile, 0)
    for c, d in states:
        c.wait()
        d.start()
    store(0, 0, wait)
    store(1, 0, wait)
    for _, d in states:
        d.wait()


def run_grads(useq, hseq, dz, dh, dc, db, sq, spans):
    n_groups, steps, _, hidden = useq.shape
    rows = n_groups * GROUP
    any_spec = pl.BlockSpec(memory_space=pl.ANY)
    vmem_spec = pl.BlockSpec(memory_space=pltpu.VMEM)
    blocks = n_groups * steps + GROUP
    tile = 512
    dma = pltpu.SemaphoreType.DMA
    out = jax.ShapeDtypeStruct((1, hidden, 4 * hidden), f32)
    state = jax.ShapeDtypeStruct((1, rows, hidden), f32)
    return pl.pallas_call(
        functools.partial(grads_kernel, steps, hidden),
        out_shape=(out, out, jax.ShapeDtypeStruct((1, 4 * hidden), f32), state, state, jax.ShapeDtypeStruct((1, 1), f32)),
        in_specs=[pl.BlockSpec(memory_space=pltpu.SMEM)] + [any_spec] * 5 + [vmem_spec] * 2,
        out_specs=(any_spec, any_spec, vmem_spec, any_spec, any_spec, vmem_spec),
        scratch_shapes=[
            pltpu.VMEM((2, blocks, GROUP, hidden), bf16),
            pltpu.VMEM((2, blocks, GROUP, tile), bf16),
            pltpu.VMEM((2, hidden, tile), f32),
            pltpu.VMEM((2, rows, hidden), f32),
            dma((2,)), dma((2,)), dma((2,)), dma((2,)),
        ],
        compiler_params=pltpu.CompilerParams(vmem_limit_bytes=VMEM_LIMIT),
        name="lstm_weight_grads",
    )(spans, useq, hseq, dz, dh, dc, db, sq)


def solution(mesh):
    n_stages = mesh.shape["stage"]

    def local_program(inputs, targets, lengths, w_in, w_rec, gate_bias, h_init, c_init):
        useq, tseq, win_t, wrec_t = run_prepare(n_stages, inputs, targets, w_in, w_rec)
        useq, hseq, gates, cseq = run_forward(n_stages, useq, w_in, w_rec, gate_bias, h_init, c_init, lengths)
        win_t, wrec_t = run_late_turn(n_stages, w_in, w_rec, cseq, win_t, wrec_t)
        _, dz, dh0, dc0, db, sq = run_backward(n_stages, hseq, tseq, gates, cseq, win_t, wrec_t, lengths)
        grad_in, grad_rec, grad_bias, dh0, dc0, loss = run_grads(useq, hseq, dz, dh0, dc0, db, sq, lengths)
        return loss.reshape(1), grad_in, grad_rec, grad_bias, dh0, dc0

    row_spec = P("data", None, None)
    layer_spec = P("stage", None, None)
    state_spec = P("stage", "data", None)
    grad_spec = P(("data", "stage"), None, None)
    return jax.shard_map(local_program, mesh=mesh,
                         in_specs=(row_spec, row_spec, P("data"), layer_spec, layer_spec, P("stage", None), state_spec, state_spec),
                         out_specs=(P("data"), grad_spec, grad_spec, P(("data", "stage"), None), state_spec, state_spec),
                         check_vma=False)
```

```python
import functools

import jax
import jax.numpy as jnp
from jax import lax
from jax.experimental import pallas as pl
from jax.experimental.pallas import tpu as pltpu
from jax.sharding import PartitionSpec as P

MESH = pl.DeviceIdType.MESH
NB = 8
WIN = 2
UNITS = 5
GROUP = 16
VMEM_LIMIT = 67043328
f32 = jnp.float32
bf16 = jnp.bfloat16


def sigmoid(x):
    return 0.5 * jnp.tanh(0.5 * x) + 0.5


def copy_of(src, dst, sem):
    return pltpu.make_async_copy(src, dst, sem)


def entry_barrier(stage, n_stages):
    barrier = pltpu.get_barrier_semaphore()
    for step in range(1, n_stages):
        pl.semaphore_signal(barrier, inc=1, device_id={"stage": lax.rem(stage + step, n_stages)}, device_id_type=MESH)
    pl.semaphore_wait(barrier, n_stages - 1)


def fill_lens(spans, lens):
    for r in range(lens.shape[0]):
        lens[r:r + 1, :] = jnp.full((1, lens.shape[1]), spans[r], jnp.int32)


def turn_weights(w_in, w_rec, win_t, wrec_t, src, dst, in_sem, out_sem):
    hidden = w_rec.shape[1]
    bw = hidden // NB
    per_half = NB // 2
    n_parts = win_t.shape[1]
    part = hidden // n_parts
    n_slots = src.shape[0]

    def load(i):
        slot = lax.rem(i, n_slots)
        j, g = lax.rem(i, 4 * NB) // 4, lax.rem(i, 4)
        cols = pl.ds(pl.multiple_of(g * hidden + j * bw, 128), bw)
        return (copy_of(w_rec.at[0, :, cols], src.at[slot], in_sem.at[slot]),
                copy_of(w_in.at[0, :, cols], src.at[slot], in_sem.at[slot]))

    def save(i):
        slot = lax.rem(i, n_slots)
        j, g = lax.rem(i, 4 * NB) // 4, lax.rem(i, 4)
        rec = copy_of(dst.at[slot], wrec_t.at[j, pl.ds(pl.multiple_of(g * bw, 8), bw)], out_sem.at[slot, 0])
        at = pl.multiple_of(g * per_half * bw + lax.rem(j, per_half) * bw, 8)
        ins = [copy_of(dst.at[slot, :, pl.ds(q * part, part)], win_t.at[j // per_half, q, pl.ds(at, bw)], out_sem.at[slot, q])
               for q in range(n_parts)]
        return [rec], ins

    units = 8 * NB

    def both(i, rec_do, in_do):
        @pl.when(i < 4 * NB)
        def _():
            rec_do()

        @pl.when(i >= 4 * NB)
        def _():
            in_do()

    def start_load(i):
        both(i, lambda: load(i)[0].start(), lambda: load(i)[1].start())

    def each_save(i, act):
        both(i, lambda: [act(c) for c in save(i)[0]], lambda: [act(c) for c in save(i)[1]])

    for i in range(n_slots):
        start_load(i)

    def unit(i, _):
        slot = lax.rem(i, n_slots)
        load(i)[0].wait()

        @pl.when(i >= n_slots)
        def _():
            each_save(i - n_slots, lambda c: c.wait())

        dst[slot] = src[slot].T
        each_save(i, lambda c: c.start())

        @pl.when(i + n_slots < units)
        def _():
            start_load(i + n_slots)

        return 0

    lax.fori_loop(0, units, unit, 0)
    for i in range(units - n_slots, units):
        each_save(i, lambda c: c.wait())


def early_turn(n_stages, stage):
    return stage >= n_stages // 2


def prepare_kernel(n_stages, inputs, targets, w_in, w_rec, useq, tseq, win_t, wrec_t,
                   src, dst, wsrc, wdst, in_sem, out_sem, win_sem, wout_sem):
    rows, steps, _ = inputs.shape
    stage = lax.axis_index("stage")
    n_slots = src.shape[0]
    n_cols = steps // GROUP
    units = rows // GROUP * n_cols

    def turn(x, y):
        def load(i):
            slot = lax.rem(i, n_slots)
            return copy_of(x.at[pl.ds(pl.multiple_of(i // n_cols * GROUP, GROUP), GROUP),
                                pl.ds(pl.multiple_of(lax.rem(i, n_cols) * GROUP, GROUP), GROUP)], src.at[slot], in_sem.at[slot])

        def save(i):
            slot = lax.rem(i, n_slots)
            return copy_of(dst.at[slot], y.at[i // n_cols, pl.ds(lax.rem(i, n_cols) * GROUP, GROUP)], out_sem.at[slot])

        for i in range(min(n_slots, units)):
            load(i).start()

        def unit(i, _):
            slot = lax.rem(i, n_slots)
            load(i).wait()

            @pl.when(i >= n_slots)
            def _():
                save(i).wait()

            dst[slot] = jnp.swapaxes(src[slot], 0, 1)
            save(i).start()

            @pl.when(i + n_slots < units)
            def _():
                load(i + n_slots).start()

            return 0

        lax.fori_loop(0, units, unit, 0)
        for i in range(max(0, units - n_slots), units):
            save(i).wait()

    @pl.when(stage == 0)
    def _():
        turn(inputs, useq)

    @pl.when(stage == n_stages - 1)
    def _():
        turn(targets, tseq)

    @pl.when(early_turn(n_stages, stage))
    def _():
        turn_weights(w_in, w_rec, win_t, wrec_t, wsrc, wdst, win_sem, wout_sem)


def weight_scratch(hidden):
    dma = pltpu.SemaphoreType.DMA
    slots = 4
    return ([pltpu.VMEM((slots, hidden, hidden // NB), bf16), pltpu.VMEM((slots, hidden // NB, hidden), bf16)],
            [dma((slots,)), dma((slots, WIN))])


def run_prepare(n_stages, inputs, targets, w_in, w_rec):
    rows, steps, hidden = inputs.shape
    any_spec = pl.BlockSpec(memory_space=pl.ANY)
    dma = pltpu.SemaphoreType.DMA
    seq = jax.ShapeDtypeStruct((rows // GROUP, steps, GROUP, hidden), bf16)
    buffers, sems = weight_scratch(hidden)
    return pl.pallas_call(
        functools.partial(prepare_kernel, n_stages),
        out_shape=(seq, seq, jax.ShapeDtypeStruct((2, WIN, 2 * hidden, hidden // WIN), bf16),
                   jax.ShapeDtypeStruct((NB, hidden // 2, hidden), bf16)),
        in_specs=[any_spec] * 4, out_specs=(any_spec,) * 4,
        scratch_shapes=[pltpu.VMEM((4, GROUP, GROUP, hidden), bf16), pltpu.VMEM((4, GROUP, GROUP, hidden), bf16), *buffers,
                        dma((4,)), dma((4,)), *sems],
        compiler_params=pltpu.CompilerParams(vmem_limit_bytes=VMEM_LIMIT),
        name="lstm_prepare",
    )(inputs, targets, w_in, w_rec)


def late_turn_kernel(n_stages, w_in, w_rec, after, win_old, wrec_old, win_t, wrec_t, wsrc, wdst, win_sem, wout_sem):
    del after, win_old, wrec_old

    @pl.when(jnp.logical_not(early_turn(n_stages, lax.axis_index("stage"))))
    def _():
        turn_weights(w_in, w_rec, win_t, wrec_t, wsrc, wdst, win_sem, wout_sem)


def run_late_turn(n_stages, w_in, w_rec, after, win_t, wrec_t):
    any_spec = pl.BlockSpec(memory_space=pl.ANY)
    buffers, sems = weight_scratch(w_rec.shape[1])
    return pl.pallas_call(
        functools.partial(late_turn_kernel, n_stages),
        out_shape=(jax.ShapeDtypeStruct(win_t.shape, bf16), jax.ShapeDtypeStruct(wrec_t.shape, bf16)),
        in_specs=[any_spec] * 5, out_specs=(any_spec,) * 2, input_output_aliases={3: 0, 4: 1},
        scratch_shapes=[*buffers, *sems],
        compiler_params=pltpu.CompilerParams(vmem_limit_bytes=VMEM_LIMIT),
        name="lstm_late_turn",
    )(w_in, w_rec, after, win_t, wrec_t)


def forward_kernel(n_stages, steps, rows, hidden,
                   seq_ref, w_in, w_rec, bias, h_start, c_start, spans,
                   useq, hseq, gates, cseq, w_blocks,
                   wr, wi, uring, zin, gst, cst, hst, lens,
                   wr_sem, wi_sem, wb_sem, u_sem, g_sem, c_sem, h_sem, send_sem, recv_sem):
    bw = hidden // NB
    half = NB // 2
    hw = half * bw
    per = 4 // WIN
    stage = lax.axis_index("stage")
    first = stage == 0
    sends = stage < n_stages - 1
    entry_barrier(stage, n_stages)

    def wr_copies(j):
        return [copy_of(w_rec.at[0, :, pl.ds(g * hidden + j * bw, bw)], wr.at[j, :, pl.ds(g * bw, bw)], wr_sem.at[j, g])
                for g in range(4)]

    def gate_of(t, i):
        return lax.rem(t + WIN, WIN) * per + i

    def unit_of(m, i):
        n = per * m + i
        t, hf = (m + 2 * WIN) // 2 - WIN, lax.rem(m + 2 * WIN, 2)
        return lax.rem(n + 4 * UNITS, UNITS), gate_of(t, i), 1 - hf

    def wi_natural(m, i):
        slot, g, hh = unit_of(m, i)
        return copy_of(w_in.at[0, :, pl.ds(pl.multiple_of(g * hidden + hh * hw, 128), hw)], wi.at[slot], wi_sem.at[slot])

    def wi_block(m, i):
        slot, g, hh = unit_of(m, i)
        return copy_of(w_blocks.at[hh, g], wi.at[slot], wi_sem.at[slot])

    def wi_keep(m, i):
        slot, g, hh = unit_of(m, i)
        return copy_of(wi.at[slot], w_blocks.at[hh, g], wb_sem.at[i])

    def u_copy(t):
        slot = lax.rem(t, WIN + 1)
        return copy_of(useq.at[:, t], uring.at[slot], u_sem.at[0])

    def g_copy(t, hf):
        return copy_of(gst.at[pl.ds(hf * half, half)], gates.at[t, pl.ds(hf * half, half)], g_sem.at[hf])

    def c_copy(slot, t):
        return copy_of(cst.at[slot], cseq.at[t], c_sem.at[slot])

    def h_copy(slot, t):
        return copy_of(hst.at[slot], hseq.at[:, t], h_sem.at[slot])

    def send(slot, t):
        return pltpu.make_async_remote_copy(
            src_ref=hst.at[slot], dst_ref=useq.at[:, t], send_sem=send_sem.at[slot], recv_sem=recv_sem.at[t],
            device_id={"stage": lax.rem(stage + 1, n_stages)}, device_id_type=MESH)

    def fetch_u(t):
        @pl.when(t < steps)
        def _():
            @pl.when(jnp.logical_not(first))
            def _():
                send(0, t).wait_recv()
            u_copy(t).start()

    def await_u(t):
        @pl.when(t < steps)
        def _():
            u_copy(t).wait()

    def project(t, hf):
        t0 = t + hf
        u = jnp.concatenate([uring[lax.rem(t0 + i + 2 * (WIN + 1), WIN + 1)].reshape(rows, hidden) for i in range(WIN)], axis=0)
        for i in range(per):
            slot, g, hh = unit_of(2 * t + hf, i)
            z = jnp.dot(u, wi[slot], preferred_element_type=f32)
            z += bias[0:1, pl.ds(pl.multiple_of(g * hidden + hh * hw, 128), hw)]
            for k in range(WIN):
                zin[4 * (1 - hf) + g, lax.rem(t0 + k + 2 * WIN, WIN)] = z[k * rows:(k + 1) * rows]

    def recur(t, hf):
        cur, nxt = lax.rem(t, 2), lax.rem(t + 1, 2)
        live = lens[...] > t
        h = hst[cur].reshape(rows, hidden)
        h_twice = jnp.concatenate([h, h], axis=0)
        for j in range(hf * half, (hf + 1) * half):
            cols = slice(j * bw, (j + 1) * bw)
            z = jnp.dot(h_twice, wr[j], preferred_element_type=f32)
            z = jnp.maximum(z[:rows], z[rows:])
            at = (j - hf * half) * bw
            zi, zf, zg, zo = (z[:, g * bw:(g + 1) * bw] + zin[4 * hf + g, lax.rem(t, WIN), :, at:at + bw] for g in range(4))
            gi = sigmoid(zi)
            gf = sigmoid(zf)
            gg = jnp.tanh(zg)
            go = sigmoid(zo)
            c_prev = cst[cur, :, cols]
            c_new = gf * c_prev + gi * gg
            h_new = go * jnp.tanh(c_new)
            cst[nxt, :, cols] = jnp.where(live, c_new, c_prev)
            hst[nxt, :, :, cols] = jnp.where(live, h_new, h[:, cols].astype(f32)).astype(bf16).reshape(rows // GROUP, GROUP, bw)
            gst[j, :, :bw] = gi
            gst[j, :, bw:2 * bw] = gf
            gst[j, :, 2 * bw:3 * bw] = gg
            gst[j, :, 3 * bw:] = go

    first_m = 1 - 2 * WIN
    wi_natural(first_m, 0).start()
    wi_natural(first_m, 1).start()
    wi_natural(first_m + 1, 0).start()
    fill_lens(spans, lens)
    begin = [copy_of(h_start.at[0, :, pl.ds(i * hw, hw)], gst.at[i], g_sem.at[i]) for i in range(2)]
    begin.append(copy_of(c_start.at[0], cst.at[0], c_sem.at[0]))
    for c in begin:
        c.start()
    for c in begin:
        c.wait()
    for i in range(2):
        hst[0, :, :, i * hw:(i + 1) * hw] = gst[i].astype(bf16).reshape(rows // GROUP, GROUP, hw)
    c_copy(0, 0).start()
    h_copy(0, 0).start()
    for m in range(first_m, 0):
        t, hf = m // 2, m % 2
        at = m - first_m
        if hf == 0:
            fetch_u(jnp.int32(t + WIN))
        elif m == first_m:
            fetch_u(jnp.int32(0))
        for i in range(per):
            if m > first_m:
                wi_keep(m - 1, i).wait()
            wi_natural(m, i).wait()
            wi_keep(m, i).start()
        wi_natural(m + 1, 1).start()
        (wi_natural if m + 2 <= 0 else wi_block)(m + 2, 0).start()
        for j in range(NB * at // (-first_m), NB * (at + 1) // (-first_m)):
            for c in wr_copies(j):
                c.start()
        if hf == 1:
            await_u(jnp.int32(t + WIN))
        project(t, hf)
    for j in range(NB):
        for c in wr_copies(j):
            c.wait()

    last_m = 2 * steps - 1

    def turn_units(m):
        @pl.when(m <= 1)
        def _():
            for i in range(per):
                wi_keep(m - 1, i).wait()

        for i in range(per):
            wi_block(m, i).wait()

        @pl.when(m == 0)
        def _():
            for i in range(per):
                wi_keep(m, i).start()

        @pl.when(m + 1 <= last_m)
        def _():
            wi_block(m + 1, 1).start()

        @pl.when(m + 2 <= last_m)
        def _():
            wi_block(m + 2, 0).start()

    def step(t, _):
        nxt = lax.rem(t + 1, 2)
        fetch_u(t + WIN)
        turn_units(2 * t)

        @pl.when(t >= 1)
        def _():
            c_copy(nxt, t).wait()
            h_copy(nxt, t).wait()
            g_copy(t, 0).wait()

        @pl.when(jnp.logical_and(t >= 2, sends))
        def _():
            send(nxt, t).wait_send()

        recur(t, 0)
        project(t, 0)

        g_copy(t, 0).start()
        turn_units(2 * t + 1)
        await_u(t + WIN)

        @pl.when(t >= 1)
        def _():
            g_copy(t, 1).wait()

        recur(t, 1)
        project(t, 1)

        g_copy(t, 1).start()
        c_copy(nxt, t + 1).start()
        h_copy(nxt, t + 1).start()

        @pl.when(sends)
        def _():
            send(nxt, t).start()

        return 0

    lax.fori_loop(0, steps, step, 0)
    for hf in range(2):
        g_copy(0, hf).wait()
        c_copy(hf, 0).wait()
        h_copy(hf, 0).wait()

        @pl.when(sends)
        def _():
            send(hf, 0).wait_send()


def run_forward(n_stages, seq, w_in, w_rec, bias, h_start, c_start, spans):
    n_groups, steps, _, hidden = seq.shape
    rows = n_groups * GROUP
    bw = hidden // NB
    any_spec = pl.BlockSpec(memory_space=pl.ANY)
    vmem_spec = pl.BlockSpec(memory_space=pltpu.VMEM)
    dma = pltpu.SemaphoreType.DMA
    return pl.pallas_call(
        functools.partial(forward_kernel, n_stages, steps, rows, hidden),
        out_shape=(jax.ShapeDtypeStruct((n_groups, steps, GROUP, hidden), bf16),
                   jax.ShapeDtypeStruct((n_groups, steps + 1, GROUP, hidden), bf16),
                   jax.ShapeDtypeStruct((steps, NB, rows, 4 * bw), f32),
                   jax.ShapeDtypeStruct((steps + 1, rows, hidden), f32),
                   jax.ShapeDtypeStruct((2, 4, hidden, hidden // 2), bf16)),
        in_specs=[any_spec, any_spec, any_spec, vmem_spec, any_spec, any_spec, pl.BlockSpec(memory_space=pltpu.SMEM)],
        out_specs=(any_spec,) * 5,
        input_output_aliases={0: 0},
        scratch_shapes=[
            pltpu.VMEM((NB, hidden, 4 * bw), bf16),
            pltpu.VMEM((UNITS, hidden, hidden // 2), bf16),
            pltpu.VMEM((WIN + 1, n_groups, GROUP, hidden), bf16),
            pltpu.VMEM((8, WIN, rows, hidden // 2), f32),
            pltpu.VMEM((NB, rows, 4 * bw), f32),
            pltpu.VMEM((2, rows, hidden), f32),
            pltpu.VMEM((2, n_groups, GROUP, hidden), bf16),
            pltpu.VMEM((rows, bw), jnp.int32),
            dma((NB, 4)), dma((UNITS,)), dma((2,)), dma((1,)), dma((2,)), dma((2,)), dma((2,)), dma((2,)), dma((steps,)),
        ],
        compiler_params=pltpu.CompilerParams(collective_id=0, has_side_effects=True, vmem_limit_bytes=VMEM_LIMIT),
        name="lstm_forward",
    )(seq, w_in, w_rec, bias, h_start, c_start, spans)


def backward_kernel(n_stages, steps, rows, hidden,
                    hseq, tseq, gates, cseq, win_t, wrec_t, spans,
                    drecv, dz_out, dh_out, dc_out, db_out, loss_out,
                    wt, wi, gin, cring, dbuf, ybuf, dzr, dh, dc, dbacc, lossacc, duacc, dust, lsend, lrecv, lens, scale,
                    wt_sem, wi_sem, g_sem, c_sem, d_sem, y_sem, dz_sem, out_sem, send_sem, recv_sem, lsend_sem, lrecv_sem):
    bw = hidden // NB
    n_groups = rows // GROUP
    half = NB // 2
    hw = half * bw
    part = hidden // WIN
    ring = WIN
    pad = WIN - 1
    stage = lax.axis_index("stage")
    top = stage == n_stages - 1
    sends = stage > 0
    last = steps - 1
    halves = jnp.where(sends, 2 * (steps + pad), 2 * steps)
    entry_barrier(stage, n_stages)

    def wt_copies():
        return [copy_of(wrec_t.at[j], wt.at[j], wt_sem.at[j]) for j in range(NB)]

    def part_of(t):
        return lax.rem(t + WIN, WIN)

    def wi_copy(m, i):
        n = 2 * m + i
        t, hf = last - m // 2, lax.rem(m, 2)
        return copy_of(win_t.at[hf, part_of(t), pl.ds(i * hidden, hidden)], wi.at[lax.rem(n, UNITS)], wi_sem.at[lax.rem(n, UNITS)])

    def turn_units(m):
        for i in range(2):
            wi_copy(m, i).wait()

        @pl.when(m + 1 < halves)
        def _():
            wi_copy(m + 1, 1).start()

        @pl.when(m + 2 < halves)
        def _():
            wi_copy(m + 2, 0).start()

    def g_copy(t, hf):
        return copy_of(gates.at[t, pl.ds(hf * half, half)], gin.at[pl.ds(hf * half, half)], g_sem.at[hf])

    def c_copy(i):
        slot = lax.rem(i, 3)
        return copy_of(cseq.at[i], cring.at[slot], c_sem.at[slot])

    def own_copies(t):
        return [copy_of(hseq.at[:, t + 1, :, pl.ds(q * part, part)], dbuf.at[lax.rem(t, 2), q], d_sem.at[q])
                for q in range(WIN)]

    def y_copy(t):
        return copy_of(tseq.at[:, t], ybuf.at[lax.rem(t, 2)], y_sem.at[0])

    def recv_copies(t):
        return [copy_of(drecv.at[q, t + pad], dbuf.at[lax.rem(t, 2), q], d_sem.at[q]) for q in range(WIN)]

    def dz_copies(t):
        slot = lax.rem(t, ring)
        return [copy_of(dzr.at[slot, hf, :, :, pl.ds(g * hw, hw)], dz_out.at[:, t, :, pl.ds(g * hidden + hf * hw, hw)],
                        dz_sem.at[slot, 4 * hf + g]) for hf in range(2) for g in range(4)]

    def send(t):
        return pltpu.make_async_remote_copy(
            src_ref=dust.at[0], dst_ref=drecv.at[part_of(t), pl.ds(t + pad, WIN)],
            send_sem=send_sem.at[0], recv_sem=recv_sem.at[t + pad],
            device_id={"stage": lax.rem(stage + n_stages - 1, n_stages)}, device_id_type=MESH)

    def fetch_d(t):
        @pl.when(top)
        def _():
            for c in own_copies(t):
                c.start()
            y_copy(t).start()

        @pl.when(jnp.logical_not(top))
        def _():
            send(t - pad).wait_recv()
            for c in recv_copies(t):
                c.start()

    def await_d(t):
        for c in recv_copies(t):
            c.wait()

        @pl.when(top)
        def _():
            y_copy(t).wait()

    def input_grad(t, hf):
        d = jnp.concatenate([dzr[lax.rem(t + i + ring, ring), hf].reshape(rows, 2 * hidden) for i in range(WIN)], axis=0)
        n = 2 * (2 * (last - t) + hf)
        du = jnp.dot(d[:, :hidden], wi[lax.rem(n, UNITS)], preferred_element_type=f32)
        du += jnp.dot(d[:, hidden:], wi[lax.rem(n + 1, UNITS)], preferred_element_type=f32)
        if hf == 0:
            duacc[...] = du
        else:
            du = (du + duacc[...]).astype(bf16)
            for i in range(WIN):
                dust[0, i] = du[i * rows:(i + 1) * rows].reshape(n_groups, GROUP, part)

    def flat(x):
        return x.reshape(rows, x.shape[-1])

    def fold(x):
        return x.reshape(rows // 8, 8, x.shape[-1]).sum(axis=0)

    def recur(t, hf):
        cur, nxt = lax.rem(t, 2), lax.rem(t + 1, 2)
        slot = cur
        live = lens[...] > t
        sc = scale[0:1, :]
        total = None
        for j in range(hf * half, (hf + 1) * half):
            cols = slice(j * bw, (j + 1) * bw)
            q, off = j * bw // part, j * bw % part
            gi, gf = gin[j, :, :bw], gin[j, :, bw:2 * bw]
            gg, go = gin[j, :, 2 * bw:3 * bw], gin[j, :, 3 * bw:]
            err = jnp.where(live, flat(dbuf[slot, q, :, :, off:off + bw]).astype(f32) - flat(ybuf[slot, :, :, cols]).astype(f32), 0.0)
            lossacc[:, cols] += fold(err * err)
            d_total = dh[cur, :, cols] + err * sc
            c_prev = cring[lax.rem(t, 3), :, cols]
            tanh_c = jnp.tanh(cring[lax.rem(t + 1, 3), :, cols])
            dc_old = dc[:, cols]
            d_c = dc_old + d_total * go * (1.0 - tanh_c * tanh_c)
            gates_d = (d_c * gg * gi * (1.0 - gi),
                     d_c * c_prev * gf * (1.0 - gf),
                     d_c * gi * (1.0 - gg * gg),
                     d_total * tanh_c * go * (1.0 - go))
            low = []
            for g in range(4):
                dz = jnp.where(live, gates_d[g], 0.0)
                dbacc[j, :, g * bw:(g + 1) * bw] += fold(dz)
                dz = dz.astype(bf16)
                at = g * hw + (j - hf * half) * bw
                dzr[lax.rem(t, ring), hf, :, :, at:at + bw] = dz.reshape(n_groups, GROUP, bw)
                low.append(dz)
            dc[:, cols] = jnp.where(live, d_c * gf, dc_old)
            keep = jnp.where(live, 0.0, d_total)
            if hf == 0:
                dh[nxt, :, cols] = keep
            else:
                dh[nxt, :, cols] += keep
            low = jnp.concatenate(low, axis=1)
            low = jnp.concatenate([low, low], axis=0)
            r = jnp.dot(low, wt[j], preferred_element_type=f32)
            total = r if total is None else total + r
        total = jnp.maximum(total[:rows], total[rows:])
        if hf == 0:
            dh[nxt, :, :hw] += total[:, :hw]
            dh[nxt, :, hw:] = total[:, hw:]
        else:
            dh[nxt] += total

    for c in wt_copies():
        c.start()
    wi_copy(0, 0).start()
    wi_copy(0, 1).start()
    wi_copy(1, 0).start()
    g_copy(last, 0).start()
    c_copy(last + 1).start()
    c_copy(last).start()
    fill_lens(spans, lens)
    n_active = spans[0]
    for r in range(1, rows):
        n_active += spans[r]
    share = 1.0 / jnp.full(scale.shape, n_active.astype(f32))
    scale[...] = jnp.where(top, share, 1.0)
    dh[...] = jnp.zeros_like(dh)
    dc[...] = jnp.zeros_like(dc)
    dbacc[...] = jnp.zeros_like(dbacc)
    lossacc[...] = jnp.zeros_like(lossacc)
    ybuf[...] = jnp.zeros_like(ybuf)
    for i in range(ring):
        dzr[i] = jnp.zeros_like(dzr[i])

    @pl.when(jnp.logical_not(top))
    def _():
        for i in range(pad):
            send(last - i).wait_recv()

    fetch_d(last)
    c_copy(last + 1).wait()
    for c in wt_copies():
        c.wait()

    def step(v, _):
        t = last - v
        await_d(t)
        g_copy(t, 0).wait()
        c_copy(t).wait()

        @pl.when(v >= ring)
        def _():
            for c in dz_copies(t + ring):
                c.wait()

        g_copy(t, 1).start()
        turn_units(2 * v)

        @pl.when(t >= 1)
        def _():
            c_copy(t - 1).start()

        recur(t, 0)
        input_grad(t, 0)

        g_copy(t, 1).wait()

        @pl.when(jnp.logical_and(v >= 1, sends))
        def _():
            send(t + 1).wait_send()

        turn_units(2 * v + 1)

        @pl.when(t >= 1)
        def _():
            g_copy(t - 1, 0).start()
            fetch_d(t - 1)

        recur(t, 1)
        input_grad(t, 1)
        for c in dz_copies(t):
            c.start()

        @pl.when(sends)
        def _():
            send(t).start()

        return 0

    lax.fori_loop(0, steps, step, 0)

    for i in range(ring):
        for c in dz_copies(i):
            c.wait()
    outs = [copy_of(dh.at[1], dh_out, out_sem.at[0]), copy_of(dc, dc_out, out_sem.at[1]),
            copy_of(dbacc, db_out, out_sem.at[2])]
    for c in outs:
        c.start()

    def tell(other):
        return pltpu.make_async_remote_copy(
            src_ref=lsend, dst_ref=lrecv, send_sem=lsend_sem.at[other], recv_sem=lrecv_sem.at[0],
            device_id={"stage": other}, device_id_type=MESH)

    @pl.when(top)
    def _():
        lsend[...] = sum(lossacc[:, i * 128:(i + 1) * 128] for i in range(hidden // 128))

    @pl.when(top)
    def _():
        for other in range(n_stages - 1):
            tell(other).start()
        lrecv[...] = lsend[...]

    @pl.when(sends)
    def _():
        def drain(v, _):
            t = -1 - v
            turn_units(2 * (last - t))
            input_grad(t, 0)
            turn_units(2 * (last - t) + 1)
            send(t + 1).wait_send()
            input_grad(t, 1)
            send(t).start()
            return 0

        lax.fori_loop(0, pad, drain, 0)
        send(-pad).wait_send()

    @pl.when(top)
    def _():
        for other in range(n_stages - 1):
            tell(other).wait_send()

    @pl.when(jnp.logical_not(top))
    def _():
        tell(0).wait_recv()

    loss_copy = copy_of(lrecv, loss_out, out_sem.at[3])
    loss_copy.start()
    loss_copy.wait()
    for c in outs:
        c.wait()


def run_backward(n_stages, hseq, tseq, gates, cseq, win_t, wrec_t, spans):
    n_groups, steps, _, hidden = tseq.shape
    rows = n_groups * GROUP
    bw = hidden // NB
    part = hidden // WIN
    any_spec = pl.BlockSpec(memory_space=pl.ANY)
    dma = pltpu.SemaphoreType.DMA
    return pl.pallas_call(
        functools.partial(backward_kernel, n_stages, steps, rows, hidden),
        out_shape=(jax.ShapeDtypeStruct((WIN, steps + 2 * (WIN - 1), n_groups, GROUP, part), bf16),
                   jax.ShapeDtypeStruct((n_groups, steps, GROUP, 4 * hidden), bf16),
                   jax.ShapeDtypeStruct((rows, hidden), f32),
                   jax.ShapeDtypeStruct((rows, hidden), f32),
                   jax.ShapeDtypeStruct((NB, 8, 4 * bw), f32),
                   jax.ShapeDtypeStruct((8, 128), f32)),
        in_specs=[any_spec] * 6 + [pl.BlockSpec(memory_space=pltpu.SMEM)],
        out_specs=(any_spec,) * 6,
        scratch_shapes=[
            pltpu.VMEM((NB, 4 * bw, hidden), bf16),
            pltpu.VMEM((UNITS, hidden, part), bf16),
            pltpu.VMEM((NB, rows, 4 * bw), f32),
            pltpu.VMEM((3, rows, hidden), f32),
            pltpu.VMEM((2, WIN, n_groups, GROUP, part), bf16),
            pltpu.VMEM((2, n_groups, GROUP, hidden), bf16),
            pltpu.VMEM((WIN, 2, n_groups, GROUP, 2 * hidden), bf16),
            pltpu.VMEM((2, rows, hidden), f32),
            pltpu.VMEM((rows, hidden), f32),
            pltpu.VMEM((NB, 8, 4 * bw), f32),
            pltpu.VMEM((8, hidden), f32),
            pltpu.VMEM((WIN * rows, part), f32),
            pltpu.VMEM((1, WIN, n_groups, GROUP, part), bf16),
            pltpu.VMEM((8, 128), f32),
            pltpu.VMEM((8, 128), f32),
            pltpu.VMEM((rows, bw), jnp.int32),
            pltpu.VMEM((8, bw), f32),
            dma((NB,)), dma((UNITS,)), dma((2,)), dma((3,)), dma((WIN,)), dma((1,)), dma((WIN, 8)), dma((4,)), dma((1,)),
            dma((steps + WIN - 1,)), dma((n_stages - 1,)), dma((1,)),
        ],
        compiler_params=pltpu.CompilerParams(collective_id=1, has_side_effects=True, vmem_limit_bytes=VMEM_LIMIT),
        name="lstm_backward",
    )(hseq, tseq, gates, cseq, win_t, wrec_t, spans)


def grads_kernel(steps, hidden, spans, useq, hseq, dz, dh, dc, db, sq,
                 g_in, g_rec, g_bias, dh_out, dc_out, loss_out,
                 xs, dzb, acc, state, x_sem, z_sem, o_sem, s_sem):
    n_groups = useq.shape[0]
    tile = dzb.shape[-1]
    n_tiles = dz.shape[-1] // tile
    bw = hidden // NB
    seen = [spans[i * GROUP] for i in range(n_groups)]
    first = [0]
    for i in range(n_groups):
        first.append(first[-1] + seen[i])
    total = first[-1]
    sizes = []
    size = 1
    while size <= steps:
        sizes.insert(0, size)
        size *= 2

    def pieces(make, act):
        for i in range(n_groups):
            for size in sizes:
                done = seen[i] // (2 * size) * (2 * size)

                @pl.when(seen[i] // size % 2 == 1)
                def _(i=i, size=size, done=done):
                    act(make(i, pl.ds(done, size), pl.ds(first[i] + done, size)))

    def load_x(w, act):
        src = useq if w == 0 else hseq
        pieces(lambda i, at, to: copy_of(src.at[i, at], xs.at[w, to], x_sem.at[w]), act)

    def load_z(n, slot, act):
        cols = pl.ds(pl.multiple_of(n * tile, tile), tile)
        pieces(lambda i, at, to: copy_of(dz.at[i, at, :, cols], dzb.at[slot, to], z_sem.at[slot]), act)

    def start(c):
        c.start()

    def wait(c):
        c.wait()

    def store(w, n, act):
        cols = pl.ds(pl.multiple_of(n * tile, tile), tile)

        @pl.when(w == 0)
        def _():
            act(copy_of(acc.at[0], g_in.at[0, :, cols], o_sem.at[0]))

        @pl.when(w == 1)
        def _():
            act(copy_of(acc.at[1], g_rec.at[0, :, cols], o_sem.at[1]))

    for slot in range(2):
        xs[slot, pl.ds(total, GROUP)] = jnp.zeros((GROUP, GROUP, hidden), bf16)
        dzb[slot, pl.ds(total, GROUP)] = jnp.zeros((GROUP, GROUP, tile), bf16)
    load_z(0, 0, start)
    load_x(0, start)
    load_x(1, start)
    states = [(copy_of(x, state.at[i], s_sem.at[i]), copy_of(state.at[i], y.at[0], s_sem.at[i]))
              for i, (x, y) in enumerate(((dh, dh_out), (dc, dc_out)))]
    for c, _ in states:
        c.start()
    for j in range(NB):
        for g in range(4):
            g_bias[0:1, g * hidden + j * bw:g * hidden + (j + 1) * bw] = jnp.sum(
                db[j, :, g * bw:(g + 1) * bw], axis=0, keepdims=True)
    n_active = spans[0]
    for r in range(1, n_groups * GROUP):
        n_active += spans[r]
    loss_out[...] = jnp.full((1, 1), jnp.sum(sq[...]) / (2.0 * n_active.astype(f32)))

    def product(w, slot, at, depth, begin):
        rhs = dzb[slot, pl.ds(at, depth)].reshape(depth * GROUP, tile)
        mc = min(512, hidden)
        for m in range(hidden // mc):
            lhs = xs[w, pl.ds(at, depth), :, m * mc:(m + 1) * mc].reshape(depth * GROUP, mc)
            r = lax.dot_general(lhs, rhs, (((0,), (0,)), ((), ())), preferred_element_type=f32)
            acc[w, m * mc:(m + 1) * mc] = r if begin else acc[w, m * mc:(m + 1) * mc] + r

    units = (total + 15) // 16

    def one_tile(v, _):
        n, w = v // 2, lax.rem(v, 2)
        slot = lax.rem(n, 2)

        @pl.when(w == 0)
        def _():
            @pl.when(n + 1 < n_tiles)
            def _():
                load_z(n + 1, 1 - slot, start)

            load_z(n, slot, wait)

        @pl.when(v == 0)
        def _():
            load_x(0, wait)

        @pl.when(v == 1)
        def _():
            load_x(1, wait)

        @pl.when(n >= 1)
        def _():
            store(w, n, wait)

        product(w, slot, 0, 128, True)

        def more(b, _):
            product(w, slot, 128 + b * 64, 64, False)
            return 0

        rest = jnp.maximum(units - 8, 0)
        lax.fori_loop(0, rest // 4, more, 0)

        @pl.when(rest // 2 % 2 == 1)
        def _():
            product(w, slot, 128 + rest // 4 * 64, 32, False)

        @pl.when(rest % 2 == 1)
        def _():
            product(w, slot, 128 + rest // 2 * 32, 16, False)

        store(w, n, start)
        return 0

    lax.fori_loop(0, 2 * n_tiles, one_tile, 0)
    for c, d in states:
        c.wait()
        d.start()
    store(0, 0, wait)
    store(1, 0, wait)
    for _, d in states:
        d.wait()


def run_grads(useq, hseq, dz, dh, dc, db, sq, spans):
    n_groups, steps, _, hidden = useq.shape
    rows = n_groups * GROUP
    any_spec = pl.BlockSpec(memory_space=pl.ANY)
    vmem_spec = pl.BlockSpec(memory_space=pltpu.VMEM)
    blocks = n_groups * steps + GROUP
    tile = 512
    dma = pltpu.SemaphoreType.DMA
    out = jax.ShapeDtypeStruct((1, hidden, 4 * hidden), f32)
    state = jax.ShapeDtypeStruct((1, rows, hidden), f32)
    return pl.pallas_call(
        functools.partial(grads_kernel, steps, hidden),
        out_shape=(out, out, jax.ShapeDtypeStruct((1, 4 * hidden), f32), state, state, jax.ShapeDtypeStruct((1, 1), f32)),
        in_specs=[pl.BlockSpec(memory_space=pltpu.SMEM)] + [any_spec] * 5 + [vmem_spec] * 2,
        out_specs=(any_spec, any_spec, vmem_spec, any_spec, any_spec, vmem_spec),
        scratch_shapes=[
            pltpu.VMEM((2, blocks, GROUP, hidden), bf16),
            pltpu.VMEM((2, blocks, GROUP, tile), bf16),
            pltpu.VMEM((2, hidden, tile), f32),
            pltpu.VMEM((2, rows, hidden), f32),
            dma((2,)), dma((2,)), dma((2,)), dma((2,)),
        ],
        compiler_params=pltpu.CompilerParams(vmem_limit_bytes=VMEM_LIMIT),
        name="lstm_weight_grads",
    )(spans, useq, hseq, dz, dh, dc, db, sq)


def solution(mesh):
    n_stages = mesh.shape["stage"]

    def local_program(inputs, targets, lengths, w_in, w_rec, gate_bias, h_init, c_init):
        useq, tseq, win_t, wrec_t = run_prepare(n_stages, inputs, targets, w_in, w_rec)
        useq, hseq, gates, cseq, _ = run_forward(n_stages, useq, w_in, w_rec, gate_bias, h_init, c_init, lengths)
        win_t, wrec_t = run_late_turn(n_stages, w_in, w_rec, cseq, win_t, wrec_t)
        _, dz, dh0, dc0, db, sq = run_backward(n_stages, hseq, tseq, gates, cseq, win_t, wrec_t, lengths)
        grad_in, grad_rec, grad_bias, dh0, dc0, loss = run_grads(useq, hseq, dz, dh0, dc0, db, sq, lengths)
        return loss.reshape(1), grad_in, grad_rec, grad_bias, dh0, dc0

    row_spec = P("data", None, None)
    layer_spec = P("stage", None, None)
    state_spec = P("stage", "data", None)
    grad_spec = P(("data", "stage"), None, None)
    return jax.shard_map(local_program, mesh=mesh,
                         in_specs=(row_spec, row_spec, P("data"), layer_spec, layer_spec, P("stage", None), state_spec, state_spec),
                         out_specs=(P("data"), grad_spec, grad_spec, P(("data", "stage"), None), state_spec, state_spec),
                         check_vma=False)
```

```python
import functools

import jax
import jax.numpy as jnp
from jax import lax
from jax.experimental import pallas as pl
from jax.experimental.pallas import tpu as pltpu
from jax.sharding import PartitionSpec as P

MESH = pl.DeviceIdType.MESH
NB = 8
FWIN = 4
WIN = 2
FUNITS = 3
UNITS = 5
GROUP = 16
VMEM_LIMIT = 67043328
f32 = jnp.float32
bf16 = jnp.bfloat16


def sigmoid(x):
    return 0.5 * jnp.tanh(0.5 * x) + 0.5


def copy_of(src, dst, sem):
    return pltpu.make_async_copy(src, dst, sem)


def entry_barrier(stage, n_stages):
    barrier = pltpu.get_barrier_semaphore()
    for step in range(1, n_stages):
        pl.semaphore_signal(barrier, inc=1, device_id={"stage": lax.rem(stage + step, n_stages)}, device_id_type=MESH)
    pl.semaphore_wait(barrier, n_stages - 1)


def fill_lens(spans, lens):
    for r in range(lens.shape[0]):
        lens[r:r + 1, :] = jnp.full((1, lens.shape[1]), spans[r], jnp.int32)


def turn_weights(w_in, w_rec, win_t, wrec_t, src, dst, in_sem, out_sem):
    hidden = w_rec.shape[1]
    bw = hidden // NB
    per_half = NB // 2
    n_parts = win_t.shape[1]
    part = hidden // n_parts
    n_slots = src.shape[0]

    def load(i):
        slot = lax.rem(i, n_slots)
        j, g = lax.rem(i, 4 * NB) // 4, lax.rem(i, 4)
        cols = pl.ds(pl.multiple_of(g * hidden + j * bw, 128), bw)
        return (copy_of(w_rec.at[0, :, cols], src.at[slot], in_sem.at[slot]),
                copy_of(w_in.at[0, :, cols], src.at[slot], in_sem.at[slot]))

    def save(i):
        slot = lax.rem(i, n_slots)
        j, g = lax.rem(i, 4 * NB) // 4, lax.rem(i, 4)
        rec = copy_of(dst.at[slot], wrec_t.at[j, pl.ds(pl.multiple_of(g * bw, 8), bw)], out_sem.at[slot, 0])
        at = pl.multiple_of(g * per_half * bw + lax.rem(j, per_half) * bw, 8)
        ins = [copy_of(dst.at[slot, :, pl.ds(q * part, part)], win_t.at[j // per_half, q, pl.ds(at, bw)], out_sem.at[slot, q])
               for q in range(n_parts)]
        return [rec], ins

    units = 8 * NB

    def both(i, rec_do, in_do):
        @pl.when(i < 4 * NB)
        def _():
            rec_do()

        @pl.when(i >= 4 * NB)
        def _():
            in_do()

    def start_load(i):
        both(i, lambda: load(i)[0].start(), lambda: load(i)[1].start())

    def each_save(i, act):
        both(i, lambda: [act(c) for c in save(i)[0]], lambda: [act(c) for c in save(i)[1]])

    for i in range(n_slots):
        start_load(i)

    def unit(i, _):
        slot = lax.rem(i, n_slots)
        load(i)[0].wait()

        @pl.when(i >= n_slots)
        def _():
            each_save(i - n_slots, lambda c: c.wait())

        dst[slot] = src[slot].T
        each_save(i, lambda c: c.start())

        @pl.when(i + n_slots < units)
        def _():
            start_load(i + n_slots)

        return 0

    lax.fori_loop(0, units, unit, 0)
    for i in range(units - n_slots, units):
        each_save(i, lambda c: c.wait())


def early_turn(n_stages, stage):
    return stage >= n_stages // 2


def prepare_kernel(n_stages, inputs, targets, w_in, w_rec, useq, tseq, win_t, wrec_t,
                   src, dst, wsrc, wdst, in_sem, out_sem, win_sem, wout_sem):
    rows, steps, _ = inputs.shape
    stage = lax.axis_index("stage")
    n_slots = src.shape[0]
    n_cols = steps // GROUP
    units = rows // GROUP * n_cols

    def turn(x, y):
        def load(i):
            slot = lax.rem(i, n_slots)
            return copy_of(x.at[pl.ds(pl.multiple_of(i // n_cols * GROUP, GROUP), GROUP),
                                pl.ds(pl.multiple_of(lax.rem(i, n_cols) * GROUP, GROUP), GROUP)], src.at[slot], in_sem.at[slot])

        def save(i):
            slot = lax.rem(i, n_slots)
            return copy_of(dst.at[slot], y.at[i // n_cols, pl.ds(lax.rem(i, n_cols) * GROUP, GROUP)], out_sem.at[slot])

        for i in range(min(n_slots, units)):
            load(i).start()

        def unit(i, _):
            slot = lax.rem(i, n_slots)
            load(i).wait()

            @pl.when(i >= n_slots)
            def _():
                save(i).wait()

            dst[slot] = jnp.swapaxes(src[slot], 0, 1)
            save(i).start()

            @pl.when(i + n_slots < units)
            def _():
                load(i + n_slots).start()

            return 0

        lax.fori_loop(0, units, unit, 0)
        for i in range(max(0, units - n_slots), units):
            save(i).wait()

    @pl.when(stage == 0)
    def _():
        turn(inputs, useq)

    @pl.when(stage == n_stages - 1)
    def _():
        turn(targets, tseq)

    @pl.when(early_turn(n_stages, stage))
    def _():
        turn_weights(w_in, w_rec, win_t, wrec_t, wsrc, wdst, win_sem, wout_sem)


def weight_scratch(hidden):
    dma = pltpu.SemaphoreType.DMA
    slots = 4
    return ([pltpu.VMEM((slots, hidden, hidden // NB), bf16), pltpu.VMEM((slots, hidden // NB, hidden), bf16)],
            [dma((slots,)), dma((slots, WIN))])


def run_prepare(n_stages, inputs, targets, w_in, w_rec):
    rows, steps, hidden = inputs.shape
    any_spec = pl.BlockSpec(memory_space=pl.ANY)
    dma = pltpu.SemaphoreType.DMA
    seq = jax.ShapeDtypeStruct((rows // GROUP, steps, GROUP, hidden), bf16)
    buffers, sems = weight_scratch(hidden)
    return pl.pallas_call(
        functools.partial(prepare_kernel, n_stages),
        out_shape=(seq, seq, jax.ShapeDtypeStruct((2, WIN, 2 * hidden, hidden // WIN), bf16),
                   jax.ShapeDtypeStruct((NB, hidden // 2, hidden), bf16)),
        in_specs=[any_spec] * 4, out_specs=(any_spec,) * 4,
        scratch_shapes=[pltpu.VMEM((4, GROUP, GROUP, hidden), bf16), pltpu.VMEM((4, GROUP, GROUP, hidden), bf16), *buffers,
                        dma((4,)), dma((4,)), *sems],
        compiler_params=pltpu.CompilerParams(vmem_limit_bytes=VMEM_LIMIT),
        name="lstm_prepare",
    )(inputs, targets, w_in, w_rec)


def late_turn_kernel(n_stages, w_in, w_rec, after, win_old, wrec_old, win_t, wrec_t, wsrc, wdst, win_sem, wout_sem):
    del after, win_old, wrec_old

    @pl.when(jnp.logical_not(early_turn(n_stages, lax.axis_index("stage"))))
    def _():
        turn_weights(w_in, w_rec, win_t, wrec_t, wsrc, wdst, win_sem, wout_sem)


def run_late_turn(n_stages, w_in, w_rec, after, win_t, wrec_t):
    any_spec = pl.BlockSpec(memory_space=pl.ANY)
    buffers, sems = weight_scratch(w_rec.shape[1])
    return pl.pallas_call(
        functools.partial(late_turn_kernel, n_stages),
        out_shape=(jax.ShapeDtypeStruct(win_t.shape, bf16), jax.ShapeDtypeStruct(wrec_t.shape, bf16)),
        in_specs=[any_spec] * 5, out_specs=(any_spec,) * 2, input_output_aliases={3: 0, 4: 1},
        scratch_shapes=[*buffers, *sems],
        compiler_params=pltpu.CompilerParams(vmem_limit_bytes=VMEM_LIMIT),
        name="lstm_late_turn",
    )(w_in, w_rec, after, win_t, wrec_t)


def forward_kernel(n_stages, steps, rows, hidden,
                   seq_ref, w_in, w_rec, bias, h_start, c_start, spans,
                   useq, hseq, gates, cseq,
                   wr, wi, uring, zin, gst, cst, hst, lens,
                   wr_sem, wi_sem, u_sem, g_sem, c_sem, h_sem, send_sem, recv_sem):
    bw = hidden // NB
    half = NB // 2
    hw = half * bw
    per = 4 // FWIN
    stage = lax.axis_index("stage")
    first = stage == 0
    sends = stage < n_stages - 1
    entry_barrier(stage, n_stages)

    def wr_copies():
        return [copy_of(w_rec.at[0, :, pl.ds(g * hidden + j * bw, bw)], wr.at[j, :, pl.ds(g * bw, bw)], wr_sem.at[j, g])
                for j in range(NB) for g in range(4)]

    first_m = 2 - 2 * FWIN
    last_m = 2 * steps - 1

    def gate_of(t, i):
        return lax.rem(t + FWIN, FWIN) * per + i

    def slot_of(n):
        return lax.rem(n + 4 * FUNITS, FUNITS)

    def wi_copy(n):
        m = (n + 2 * FWIN * per) // per - 2 * FWIN
        t, hf = (m + 2 * FWIN) // 2 - FWIN, lax.rem(m + 2 * FWIN, 2)
        first_col = gate_of(t, n - per * m) * hidden + hf * hw
        return copy_of(w_in.at[0, :, pl.ds(pl.multiple_of(first_col, 128), hw)], wi.at[slot_of(n)], wi_sem.at[slot_of(n)])

    def turn_units(m):
        for i in range(per):
            wi_copy(per * m + i).wait()
        for k in range(per):
            n = per * (m - 1) + FUNITS + k

            @pl.when(n < per * (last_m + 1))
            def _(n=n):
                wi_copy(n).start()

    def u_copy(t):
        slot = lax.rem(t, FWIN + 1)
        return copy_of(useq.at[:, t], uring.at[slot], u_sem.at[0])

    def g_copy(t, hf):
        return copy_of(gst.at[pl.ds(hf * half, half)], gates.at[t, pl.ds(hf * half, half)], g_sem.at[hf])

    def c_copy(slot, t):
        return copy_of(cst.at[slot], cseq.at[t], c_sem.at[slot])

    def h_copy(slot, t):
        return copy_of(hst.at[slot], hseq.at[:, t], h_sem.at[slot])

    def send(slot, t):
        return pltpu.make_async_remote_copy(
            src_ref=hst.at[slot], dst_ref=useq.at[:, t], send_sem=send_sem.at[slot], recv_sem=recv_sem.at[t],
            device_id={"stage": lax.rem(stage + 1, n_stages)}, device_id_type=MESH)

    def fetch_u(t):
        @pl.when(t < steps)
        def _():
            @pl.when(jnp.logical_not(first))
            def _():
                send(0, t).wait_recv()
            u_copy(t).start()

    def await_u(t):
        @pl.when(t < steps)
        def _():
            u_copy(t).wait()

    def project(t, hf):
        u = jnp.concatenate([uring[lax.rem(t + i + 2 * (FWIN + 1), FWIN + 1)].reshape(rows, hidden) for i in range(FWIN)], axis=0)
        for i in range(per):
            g = gate_of(t, i)
            z = jnp.dot(u, wi[slot_of(per * (2 * t + hf) + i)], preferred_element_type=f32)
            z += bias[0:1, pl.ds(pl.multiple_of(g * hidden + hf * hw, 128), hw)]
            for k in range(FWIN):
                zin[4 * hf + g, lax.rem(t + k + 2 * FWIN, FWIN)] = z[k * rows:(k + 1) * rows]

    def recur(t, hf):
        cur, nxt = lax.rem(t, 2), lax.rem(t + 1, 2)
        live = lens[...] > t
        h = hst[cur].reshape(rows, hidden)
        h_twice = jnp.concatenate([h, h], axis=0)
        for j in range(hf * half, (hf + 1) * half):
            cols = slice(j * bw, (j + 1) * bw)
            z = jnp.dot(h_twice, wr[j], preferred_element_type=f32)
            z = jnp.maximum(z[:rows], z[rows:])
            at = (j - hf * half) * bw
            zi, zf, zg, zo = (z[:, g * bw:(g + 1) * bw] + zin[4 * hf + g, lax.rem(t, FWIN), :, at:at + bw] for g in range(4))
            gi = sigmoid(zi)
            gf = sigmoid(zf)
            gg = jnp.tanh(zg)
            go = sigmoid(zo)
            c_prev = cst[cur, :, cols]
            c_new = gf * c_prev + gi * gg
            h_new = go * jnp.tanh(c_new)
            cst[nxt, :, cols] = jnp.where(live, c_new, c_prev)
            hst[nxt, :, :, cols] = jnp.where(live, h_new, h[:, cols].astype(f32)).astype(bf16).reshape(rows // GROUP, GROUP, bw)
            gst[j, :, :bw] = gi
            gst[j, :, bw:2 * bw] = gf
            gst[j, :, 2 * bw:3 * bw] = gg
            gst[j, :, 3 * bw:] = go

    for n in range(per * first_m, per * (first_m - 1) + FUNITS):
        wi_copy(n).start()
    for c in wr_copies():
        c.start()
    fill_lens(spans, lens)
    begin = [copy_of(h_start.at[0, :, pl.ds(i * hw, hw)], gst.at[i], g_sem.at[i]) for i in range(2)]
    begin.append(copy_of(c_start.at[0], cst.at[0], c_sem.at[0]))
    for c in begin:
        c.start()
    for c in begin:
        c.wait()
    for i in range(2):
        hst[0, :, :, i * hw:(i + 1) * hw] = gst[i].astype(bf16).reshape(rows // GROUP, GROUP, hw)
    c_copy(0, 0).start()
    h_copy(0, 0).start()

    def warm(v, _):
        m = v + first_m
        t, hf = (m + 2 * FWIN) // 2 - FWIN, lax.rem(m + 2 * FWIN, 2)
        turn_units(m)

        @pl.when(hf == 0)
        def _():
            fetch_u(t + FWIN - 1)
            await_u(t + FWIN - 1)

        project(t, hf)
        return 0

    lax.fori_loop(0, -first_m, warm, 0)
    for c in wr_copies():
        c.wait()
    fetch_u(jnp.int32(FWIN - 1))

    def step(t, _):
        nxt = lax.rem(t + 1, 2)
        await_u(t + FWIN - 1)
        turn_units(2 * t)

        @pl.when(t >= 1)
        def _():
            c_copy(nxt, t).wait()
            h_copy(nxt, t).wait()
            g_copy(t, 0).wait()

        @pl.when(jnp.logical_and(t >= 2, sends))
        def _():
            send(nxt, t).wait_send()

        project(t, 0)
        recur(t, 0)

        g_copy(t, 0).start()
        turn_units(2 * t + 1)
        fetch_u(t + FWIN)

        @pl.when(t >= 1)
        def _():
            g_copy(t, 1).wait()

        project(t, 1)
        recur(t, 1)

        g_copy(t, 1).start()
        c_copy(nxt, t + 1).start()
        h_copy(nxt, t + 1).start()

        @pl.when(sends)
        def _():
            send(nxt, t).start()

        return 0

    lax.fori_loop(0, steps, step, 0)
    for hf in range(2):
        g_copy(0, hf).wait()
        c_copy(hf, 0).wait()
        h_copy(hf, 0).wait()

        @pl.when(sends)
        def _():
            send(hf, 0).wait_send()


def run_forward(n_stages, seq, w_in, w_rec, bias, h_start, c_start, spans):
    n_groups, steps, _, hidden = seq.shape
    rows = n_groups * GROUP
    bw = hidden // NB
    any_spec = pl.BlockSpec(memory_space=pl.ANY)
    vmem_spec = pl.BlockSpec(memory_space=pltpu.VMEM)
    dma = pltpu.SemaphoreType.DMA
    return pl.pallas_call(
        functools.partial(forward_kernel, n_stages, steps, rows, hidden),
        out_shape=(jax.ShapeDtypeStruct((n_groups, steps, GROUP, hidden), bf16),
                   jax.ShapeDtypeStruct((n_groups, steps + 1, GROUP, hidden), bf16),
                   jax.ShapeDtypeStruct((steps, NB, rows, 4 * bw), f32),
                   jax.ShapeDtypeStruct((steps + 1, rows, hidden), f32)),
        in_specs=[any_spec, any_spec, any_spec, vmem_spec, any_spec, any_spec, pl.BlockSpec(memory_space=pltpu.SMEM)],
        out_specs=(any_spec,) * 4,
        input_output_aliases={0: 0},
        scratch_shapes=[
            pltpu.VMEM((NB, hidden, 4 * bw), bf16),
            pltpu.VMEM((FUNITS, hidden, hidden // 2), bf16),
            pltpu.VMEM((FWIN + 1, n_groups, GROUP, hidden), bf16),
            pltpu.VMEM((8, FWIN, rows, hidden // 2), f32),
            pltpu.VMEM((NB, rows, 4 * bw), f32),
            pltpu.VMEM((2, rows, hidden), f32),
            pltpu.VMEM((2, n_groups, GROUP, hidden), bf16),
            pltpu.VMEM((rows, bw), jnp.int32),
            dma((NB, 4)), dma((FUNITS,)), dma((1,)), dma((2,)), dma((2,)), dma((2,)), dma((2,)), dma((steps,)),
        ],
        compiler_params=pltpu.CompilerParams(collective_id=0, has_side_effects=True, vmem_limit_bytes=VMEM_LIMIT),
        name="lstm_forward",
    )(seq, w_in, w_rec, bias, h_start, c_start, spans)


def backward_kernel(n_stages, steps, rows, hidden,
                    hseq, tseq, gates, cseq, win_t, wrec_t, spans,
                    drecv, dz_out, dh_out, dc_out, db_out, loss_out,
                    wt, wi, gin, cring, dbuf, ybuf, dzr, dh, dc, dbacc, lossacc, duacc, dust, lsend, lrecv, lens, scale,
                    wt_sem, wi_sem, g_sem, c_sem, d_sem, y_sem, dz_sem, out_sem, send_sem, recv_sem, lsend_sem, lrecv_sem):
    bw = hidden // NB
    n_groups = rows // GROUP
    half = NB // 2
    hw = half * bw
    part = hidden // WIN
    ring = WIN
    pad = WIN - 1
    stage = lax.axis_index("stage")
    top = stage == n_stages - 1
    sends = stage > 0
    last = steps - 1
    halves = jnp.where(sends, 2 * (steps + pad), 2 * steps)
    entry_barrier(stage, n_stages)

    def wt_copies():
        return [copy_of(wrec_t.at[j], wt.at[j], wt_sem.at[j]) for j in range(NB)]

    def part_of(t):
        return lax.rem(t + WIN, WIN)

    def wi_copy(m, i):
        n = 2 * m + i
        t, hf = last - m // 2, lax.rem(m, 2)
        return copy_of(win_t.at[hf, part_of(t), pl.ds(i * hidden, hidden)], wi.at[lax.rem(n, UNITS)], wi_sem.at[lax.rem(n, UNITS)])

    def turn_units(m):
        for i in range(2):
            wi_copy(m, i).wait()

        @pl.when(m + 1 < halves)
        def _():
            wi_copy(m + 1, 1).start()

        @pl.when(m + 2 < halves)
        def _():
            wi_copy(m + 2, 0).start()

    def g_copy(t, hf):
        return copy_of(gates.at[t, pl.ds(hf * half, half)], gin.at[pl.ds(hf * half, half)], g_sem.at[hf])

    def c_copy(i):
        slot = lax.rem(i, 3)
        return copy_of(cseq.at[i], cring.at[slot], c_sem.at[slot])

    def own_copies(t):
        return [copy_of(hseq.at[:, t + 1, :, pl.ds(q * part, part)], dbuf.at[lax.rem(t, 2), q], d_sem.at[q])
                for q in range(WIN)]

    def y_copy(t):
        return copy_of(tseq.at[:, t], ybuf.at[lax.rem(t, 2)], y_sem.at[0])

    def recv_copies(t):
        return [copy_of(drecv.at[q, t + pad], dbuf.at[lax.rem(t, 2), q], d_sem.at[q]) for q in range(WIN)]

    def dz_copies(t):
        slot = lax.rem(t, ring)
        return [copy_of(dzr.at[slot, hf, :, :, pl.ds(g * hw, hw)], dz_out.at[:, t, :, pl.ds(g * hidden + hf * hw, hw)],
                        dz_sem.at[slot, 4 * hf + g]) for hf in range(2) for g in range(4)]

    def send(t):
        return pltpu.make_async_remote_copy(
            src_ref=dust.at[0], dst_ref=drecv.at[part_of(t), pl.ds(t + pad, WIN)],
            send_sem=send_sem.at[0], recv_sem=recv_sem.at[t + pad],
            device_id={"stage": lax.rem(stage + n_stages - 1, n_stages)}, device_id_type=MESH)

    def fetch_d(t):
        @pl.when(top)
        def _():
            for c in own_copies(t):
                c.start()
            y_copy(t).start()

        @pl.when(jnp.logical_not(top))
        def _():
            send(t - pad).wait_recv()
            for c in recv_copies(t):
                c.start()

    def await_d(t):
        for c in recv_copies(t):
            c.wait()

        @pl.when(top)
        def _():
            y_copy(t).wait()

    def input_grad(t, hf):
        d = jnp.concatenate([dzr[lax.rem(t + i + ring, ring), hf].reshape(rows, 2 * hidden) for i in range(WIN)], axis=0)
        n = 2 * (2 * (last - t) + hf)
        du = jnp.dot(d[:, :hidden], wi[lax.rem(n, UNITS)], preferred_element_type=f32)
        du += jnp.dot(d[:, hidden:], wi[lax.rem(n + 1, UNITS)], preferred_element_type=f32)
        if hf == 0:
            duacc[...] = du
        else:
            du = (du + duacc[...]).astype(bf16)
            for i in range(WIN):
                dust[0, i] = du[i * rows:(i + 1) * rows].reshape(n_groups, GROUP, part)

    def flat(x):
        return x.reshape(rows, x.shape[-1])

    def fold(x):
        return x.reshape(rows // 8, 8, x.shape[-1]).sum(axis=0)

    def recur(t, hf):
        cur, nxt = lax.rem(t, 2), lax.rem(t + 1, 2)
        slot = cur
        live = lens[...] > t
        sc = scale[0:1, :]
        total = None
        for j in range(hf * half, (hf + 1) * half):
            cols = slice(j * bw, (j + 1) * bw)
            q, off = j * bw // part, j * bw % part
            gi, gf = gin[j, :, :bw], gin[j, :, bw:2 * bw]
            gg, go = gin[j, :, 2 * bw:3 * bw], gin[j, :, 3 * bw:]
            err = jnp.where(live, flat(dbuf[slot, q, :, :, off:off + bw]).astype(f32) - flat(ybuf[slot, :, :, cols]).astype(f32), 0.0)
            lossacc[:, cols] += fold(err * err)
            d_total = dh[cur, :, cols] + err * sc
            c_prev = cring[lax.rem(t, 3), :, cols]
            tanh_c = jnp.tanh(cring[lax.rem(t + 1, 3), :, cols])
            dc_old = dc[:, cols]
            d_c = dc_old + d_total * go * (1.0 - tanh_c * tanh_c)
            gates_d = (d_c * gg * gi * (1.0 - gi),
                     d_c * c_prev * gf * (1.0 - gf),
                     d_c * gi * (1.0 - gg * gg),
                     d_total * tanh_c * go * (1.0 - go))
            low = []
            for g in range(4):
                dz = jnp.where(live, gates_d[g], 0.0)
                dbacc[j, :, g * bw:(g + 1) * bw] += fold(dz)
                dz = dz.astype(bf16)
                at = g * hw + (j - hf * half) * bw
                dzr[lax.rem(t, ring), hf, :, :, at:at + bw] = dz.reshape(n_groups, GROUP, bw)
                low.append(dz)
            dc[:, cols] = jnp.where(live, d_c * gf, dc_old)
            keep = jnp.where(live, 0.0, d_total)
            if hf == 0:
                dh[nxt, :, cols] = keep
            else:
                dh[nxt, :, cols] += keep
            low = jnp.concatenate(low, axis=1)
            low = jnp.concatenate([low, low], axis=0)
            r = jnp.dot(low, wt[j], preferred_element_type=f32)
            total = r if total is None else total + r
        total = jnp.maximum(total[:rows], total[rows:])
        if hf == 0:
            dh[nxt, :, :hw] += total[:, :hw]
            dh[nxt, :, hw:] = total[:, hw:]
        else:
            dh[nxt] += total

    for c in wt_copies():
        c.start()
    wi_copy(0, 0).start()
    wi_copy(0, 1).start()
    wi_copy(1, 0).start()
    g_copy(last, 0).start()
    c_copy(last + 1).start()
    c_copy(last).start()
    fill_lens(spans, lens)
    n_active = spans[0]
    for r in range(1, rows):
        n_active += spans[r]
    share = 1.0 / jnp.full(scale.shape, n_active.astype(f32))
    scale[...] = jnp.where(top, share, 1.0)
    dh[...] = jnp.zeros_like(dh)
    dc[...] = jnp.zeros_like(dc)
    dbacc[...] = jnp.zeros_like(dbacc)
    lossacc[...] = jnp.zeros_like(lossacc)
    ybuf[...] = jnp.zeros_like(ybuf)
    for i in range(ring):
        dzr[i] = jnp.zeros_like(dzr[i])

    @pl.when(jnp.logical_not(top))
    def _():
        for i in range(pad):
            send(last - i).wait_recv()

    fetch_d(last)
    c_copy(last + 1).wait()
    for c in wt_copies():
        c.wait()

    def step(v, _):
        t = last - v
        await_d(t)
        g_copy(t, 0).wait()
        c_copy(t).wait()

        @pl.when(v >= ring)
        def _():
            for c in dz_copies(t + ring):
                c.wait()

        g_copy(t, 1).start()
        turn_units(2 * v)

        @pl.when(t >= 1)
        def _():
            c_copy(t - 1).start()

        recur(t, 0)
        input_grad(t, 0)

        g_copy(t, 1).wait()

        @pl.when(jnp.logical_and(v >= 1, sends))
        def _():
            send(t + 1).wait_send()

        turn_units(2 * v + 1)

        @pl.when(t >= 1)
        def _():
            g_copy(t - 1, 0).start()
            fetch_d(t - 1)

        recur(t, 1)
        input_grad(t, 1)
        for c in dz_copies(t):
            c.start()

        @pl.when(sends)
        def _():
            send(t).start()

        return 0

    lax.fori_loop(0, steps, step, 0)

    for i in range(ring):
        for c in dz_copies(i):
            c.wait()
    outs = [copy_of(dh.at[1], dh_out, out_sem.at[0]), copy_of(dc, dc_out, out_sem.at[1]),
            copy_of(dbacc, db_out, out_sem.at[2])]
    for c in outs:
        c.start()

    def tell(other):
        return pltpu.make_async_remote_copy(
            src_ref=lsend, dst_ref=lrecv, send_sem=lsend_sem.at[other], recv_sem=lrecv_sem.at[0],
            device_id={"stage": other}, device_id_type=MESH)

    @pl.when(top)
    def _():
        lsend[...] = sum(lossacc[:, i * 128:(i + 1) * 128] for i in range(hidden // 128))

    @pl.when(top)
    def _():
        for other in range(n_stages - 1):
            tell(other).start()
        lrecv[...] = lsend[...]

    @pl.when(sends)
    def _():
        def drain(v, _):
            t = -1 - v
            turn_units(2 * (last - t))
            input_grad(t, 0)
            turn_units(2 * (last - t) + 1)
            send(t + 1).wait_send()
            input_grad(t, 1)
            send(t).start()
            return 0

        lax.fori_loop(0, pad, drain, 0)
        send(-pad).wait_send()

    @pl.when(top)
    def _():
        for other in range(n_stages - 1):
            tell(other).wait_send()

    @pl.when(jnp.logical_not(top))
    def _():
        tell(0).wait_recv()

    loss_copy = copy_of(lrecv, loss_out, out_sem.at[3])
    loss_copy.start()
    loss_copy.wait()
    for c in outs:
        c.wait()


def run_backward(n_stages, hseq, tseq, gates, cseq, win_t, wrec_t, spans):
    n_groups, steps, _, hidden = tseq.shape
    rows = n_groups * GROUP
    bw = hidden // NB
    part = hidden // WIN
    any_spec = pl.BlockSpec(memory_space=pl.ANY)
    dma = pltpu.SemaphoreType.DMA
    return pl.pallas_call(
        functools.partial(backward_kernel, n_stages, steps, rows, hidden),
        out_shape=(jax.ShapeDtypeStruct((WIN, steps + 2 * (WIN - 1), n_groups, GROUP, part), bf16),
                   jax.ShapeDtypeStruct((n_groups, steps, GROUP, 4 * hidden), bf16),
                   jax.ShapeDtypeStruct((rows, hidden), f32),
                   jax.ShapeDtypeStruct((rows, hidden), f32),
                   jax.ShapeDtypeStruct((NB, 8, 4 * bw), f32),
                   jax.ShapeDtypeStruct((8, 128), f32)),
        in_specs=[any_spec] * 6 + [pl.BlockSpec(memory_space=pltpu.SMEM)],
        out_specs=(any_spec,) * 6,
        scratch_shapes=[
            pltpu.VMEM((NB, 4 * bw, hidden), bf16),
            pltpu.VMEM((UNITS, hidden, part), bf16),
            pltpu.VMEM((NB, rows, 4 * bw), f32),
            pltpu.VMEM((3, rows, hidden), f32),
            pltpu.VMEM((2, WIN, n_groups, GROUP, part), bf16),
            pltpu.VMEM((2, n_groups, GROUP, hidden), bf16),
            pltpu.VMEM((WIN, 2, n_groups, GROUP, 2 * hidden), bf16),
            pltpu.VMEM((2, rows, hidden), f32),
            pltpu.VMEM((rows, hidden), f32),
            pltpu.VMEM((NB, 8, 4 * bw), f32),
            pltpu.VMEM((8, hidden), f32),
            pltpu.VMEM((WIN * rows, part), f32),
            pltpu.VMEM((1, WIN, n_groups, GROUP, part), bf16),
            pltpu.VMEM((8, 128), f32),
            pltpu.VMEM((8, 128), f32),
            pltpu.VMEM((rows, bw), jnp.int32),
            pltpu.VMEM((8, bw), f32),
            dma((NB,)), dma((UNITS,)), dma((2,)), dma((3,)), dma((WIN,)), dma((1,)), dma((WIN, 8)), dma((4,)), dma((1,)),
            dma((steps + WIN - 1,)), dma((n_stages - 1,)), dma((1,)),
        ],
        compiler_params=pltpu.CompilerParams(collective_id=1, has_side_effects=True, vmem_limit_bytes=VMEM_LIMIT),
        name="lstm_backward",
    )(hseq, tseq, gates, cseq, win_t, wrec_t, spans)


def grads_kernel(steps, hidden, spans, useq, hseq, dz, dh, dc, db, sq,
                 g_in, g_rec, g_bias, dh_out, dc_out, loss_out,
                 xs, dzb, acc, state, x_sem, z_sem, o_sem, s_sem):
    n_groups = useq.shape[0]
    tile = dzb.shape[-1]
    n_tiles = dz.shape[-1] // tile
    bw = hidden // NB
    seen = [spans[i * GROUP] for i in range(n_groups)]
    first = [0]
    for i in range(n_groups):
        first.append(first[-1] + seen[i])
    total = first[-1]
    sizes = []
    size = 1
    while size <= steps:
        sizes.insert(0, size)
        size *= 2

    def pieces(make, act):
        for i in range(n_groups):
            for size in sizes:
                done = seen[i] // (2 * size) * (2 * size)

                @pl.when(seen[i] // size % 2 == 1)
                def _(i=i, size=size, done=done):
                    act(make(i, pl.ds(done, size), pl.ds(first[i] + done, size)))

    def load_x(w, act):
        src = useq if w == 0 else hseq
        pieces(lambda i, at, to: copy_of(src.at[i, at], xs.at[w, to], x_sem.at[w]), act)

    def load_z(n, slot, act):
        cols = pl.ds(pl.multiple_of(n * tile, tile), tile)
        pieces(lambda i, at, to: copy_of(dz.at[i, at, :, cols], dzb.at[slot, to], z_sem.at[slot]), act)

    def start(c):
        c.start()

    def wait(c):
        c.wait()

    def store(w, n, act):
        cols = pl.ds(pl.multiple_of(n * tile, tile), tile)

        @pl.when(w == 0)
        def _():
            act(copy_of(acc.at[0], g_in.at[0, :, cols], o_sem.at[0]))

        @pl.when(w == 1)
        def _():
            act(copy_of(acc.at[1], g_rec.at[0, :, cols], o_sem.at[1]))

    for slot in range(2):
        xs[slot, pl.ds(total, GROUP)] = jnp.zeros((GROUP, GROUP, hidden), bf16)
        dzb[slot, pl.ds(total, GROUP)] = jnp.zeros((GROUP, GROUP, tile), bf16)
    load_z(0, 0, start)
    load_x(0, start)
    load_x(1, start)
    states = [(copy_of(x, state.at[i], s_sem.at[i]), copy_of(state.at[i], y.at[0], s_sem.at[i]))
              for i, (x, y) in enumerate(((dh, dh_out), (dc, dc_out)))]
    for c, _ in states:
        c.start()
    for j in range(NB):
        for g in range(4):
            g_bias[0:1, g * hidden + j * bw:g * hidden + (j + 1) * bw] = jnp.sum(
                db[j, :, g * bw:(g + 1) * bw], axis=0, keepdims=True)
    n_active = spans[0]
    for r in range(1, n_groups * GROUP):
        n_active += spans[r]
    loss_out[...] = jnp.full((1, 1), jnp.sum(sq[...]) / (2.0 * n_active.astype(f32)))

    def product(w, slot, at, depth, begin):
        rhs = dzb[slot, pl.ds(at, depth)].reshape(depth * GROUP, tile)
        mc = min(512, hidden)
        for m in range(hidden // mc):
            lhs = xs[w, pl.ds(at, depth), :, m * mc:(m + 1) * mc].reshape(depth * GROUP, mc)
            r = lax.dot_general(lhs, rhs, (((0,), (0,)), ((), ())), preferred_element_type=f32)
            acc[w, m * mc:(m + 1) * mc] = r if begin else acc[w, m * mc:(m + 1) * mc] + r

    units = (total + 15) // 16

    def one_tile(v, _):
        n, w = v // 2, lax.rem(v, 2)
        slot = lax.rem(n, 2)

        @pl.when(w == 0)
        def _():
            @pl.when(n + 1 < n_tiles)
            def _():
                load_z(n + 1, 1 - slot, start)

            load_z(n, slot, wait)

        @pl.when(v == 0)
        def _():
            load_x(0, wait)

        @pl.when(v == 1)
        def _():
            load_x(1, wait)

        @pl.when(n >= 1)
        def _():
            store(w, n, wait)

        product(w, slot, 0, 128, True)

        def more(b, _):
            product(w, slot, 128 + b * 64, 64, False)
            return 0

        rest = jnp.maximum(units - 8, 0)
        lax.fori_loop(0, rest // 4, more, 0)

        @pl.when(rest // 2 % 2 == 1)
        def _():
            product(w, slot, 128 + rest // 4 * 64, 32, False)

        @pl.when(rest % 2 == 1)
        def _():
            product(w, slot, 128 + rest // 2 * 32, 16, False)

        store(w, n, start)
        return 0

    lax.fori_loop(0, 2 * n_tiles, one_tile, 0)
    for c, d in states:
        c.wait()
        d.start()
    store(0, 0, wait)
    store(1, 0, wait)
    for _, d in states:
        d.wait()


def run_grads(useq, hseq, dz, dh, dc, db, sq, spans):
    n_groups, steps, _, hidden = useq.shape
    rows = n_groups * GROUP
    any_spec = pl.BlockSpec(memory_space=pl.ANY)
    vmem_spec = pl.BlockSpec(memory_space=pltpu.VMEM)
    blocks = n_groups * steps + GROUP
    tile = 512
    dma = pltpu.SemaphoreType.DMA
    out = jax.ShapeDtypeStruct((1, hidden, 4 * hidden), f32)
    state = jax.ShapeDtypeStruct((1, rows, hidden), f32)
    return pl.pallas_call(
        functools.partial(grads_kernel, steps, hidden),
        out_shape=(out, out, jax.ShapeDtypeStruct((1, 4 * hidden), f32), state, state, jax.ShapeDtypeStruct((1, 1), f32)),
        in_specs=[pl.BlockSpec(memory_space=pltpu.SMEM)] + [any_spec] * 5 + [vmem_spec] * 2,
        out_specs=(any_spec, any_spec, vmem_spec, any_spec, any_spec, vmem_spec),
        scratch_shapes=[
            pltpu.VMEM((2, blocks, GROUP, hidden), bf16),
            pltpu.VMEM((2, blocks, GROUP, tile), bf16),
            pltpu.VMEM((2, hidden, tile), f32),
            pltpu.VMEM((2, rows, hidden), f32),
            dma((2,)), dma((2,)), dma((2,)), dma((2,)),
        ],
        compiler_params=pltpu.CompilerParams(vmem_limit_bytes=VMEM_LIMIT),
        name="lstm_weight_grads",
    )(spans, useq, hseq, dz, dh, dc, db, sq)


def solution(mesh):
    n_stages = mesh.shape["stage"]

    def local_program(inputs, targets, lengths, w_in, w_rec, gate_bias, h_init, c_init):
        useq, tseq, win_t, wrec_t = run_prepare(n_stages, inputs, targets, w_in, w_rec)
        useq, hseq, gates, cseq = run_forward(n_stages, useq, w_in, w_rec, gate_bias, h_init, c_init, lengths)
        win_t, wrec_t = run_late_turn(n_stages, w_in, w_rec, cseq, win_t, wrec_t)
        _, dz, dh0, dc0, db, sq = run_backward(n_stages, hseq, tseq, gates, cseq, win_t, wrec_t, lengths)
        grad_in, grad_rec, grad_bias, dh0, dc0, loss = run_grads(useq, hseq, dz, dh0, dc0, db, sq, lengths)
        return loss.reshape(1), grad_in, grad_rec, grad_bias, dh0, dc0

    row_spec = P("data", None, None)
    layer_spec = P("stage", None, None)
    state_spec = P("stage", "data", None)
    grad_spec = P(("data", "stage"), None, None)
    return jax.shard_map(local_program, mesh=mesh,
                         in_specs=(row_spec, row_spec, P("data"), layer_spec, layer_spec, P("stage", None), state_spec, state_spec),
                         out_specs=(P("data"), grad_spec, grad_spec, P(("data", "stage"), None), state_spec, state_spec),
                         check_vma=False)
```

```python
import functools

import jax
import jax.numpy as jnp
from jax import lax
from jax.experimental import pallas as pl
from jax.experimental.pallas import tpu as pltpu
from jax.sharding import PartitionSpec as P

MESH = pl.DeviceIdType.MESH
NB = 8
FWIN = 2
WIN = 2
FUNITS = 5
UNITS = 5
GROUP = 16
VMEM_LIMIT = 67043328
f32 = jnp.float32
bf16 = jnp.bfloat16


def sigmoid(x):
    return 0.5 * jnp.tanh(0.5 * x) + 0.5


def copy_of(src, dst, sem):
    return pltpu.make_async_copy(src, dst, sem)


def entry_signal(stage, n_stages):
    barrier = pltpu.get_barrier_semaphore()

    @pl.when(stage > 0)
    def _():
        pl.semaphore_signal(barrier, inc=1, device_id={"stage": lax.rem(stage + n_stages - 1, n_stages)}, device_id_type=MESH)

    @pl.when(stage < n_stages - 1)
    def _():
        pl.semaphore_signal(barrier, inc=1, device_id={"stage": lax.rem(stage + 1, n_stages)}, device_id_type=MESH)


def entry_wait(stage, n_stages):
    peers = jnp.minimum(stage, 1) + jnp.minimum(n_stages - 1 - stage, 1)
    pl.semaphore_wait(pltpu.get_barrier_semaphore(), peers)


def fill_lens(spans, lens):
    for r in range(lens.shape[0]):
        lens[r:r + 1, :] = jnp.full((1, lens.shape[1]), spans[r], jnp.int32)


def turn_weights(w_in, w_rec, win_t, wrec_t, src, dst, in_sem, out_sem):
    hidden = w_rec.shape[1]
    bw = hidden // NB
    per_half = NB // 2
    n_parts = win_t.shape[1]
    part = hidden // n_parts
    n_slots = src.shape[0]

    def load(i):
        slot = lax.rem(i, n_slots)
        j, g = lax.rem(i, 4 * NB) // 4, lax.rem(i, 4)
        cols = pl.ds(pl.multiple_of(g * hidden + j * bw, 128), bw)
        return (copy_of(w_rec.at[0, :, cols], src.at[slot], in_sem.at[slot]),
                copy_of(w_in.at[0, :, cols], src.at[slot], in_sem.at[slot]))

    def save(i):
        slot = lax.rem(i, n_slots)
        j, g = lax.rem(i, 4 * NB) // 4, lax.rem(i, 4)
        rec = copy_of(dst.at[slot], wrec_t.at[j, pl.ds(pl.multiple_of(g * bw, 8), bw)], out_sem.at[slot, 0])
        at = pl.multiple_of(g * per_half * bw + lax.rem(j, per_half) * bw, 8)
        ins = [copy_of(dst.at[slot, :, pl.ds(q * part, part)], win_t.at[j // per_half, q, pl.ds(at, bw)], out_sem.at[slot, q])
               for q in range(n_parts)]
        return [rec], ins

    units = 8 * NB

    def both(i, rec_do, in_do):
        @pl.when(i < 4 * NB)
        def _():
            rec_do()

        @pl.when(i >= 4 * NB)
        def _():
            in_do()

    def start_load(i):
        both(i, lambda: load(i)[0].start(), lambda: load(i)[1].start())

    def each_save(i, act):
        both(i, lambda: [act(c) for c in save(i)[0]], lambda: [act(c) for c in save(i)[1]])

    for i in range(n_slots):
        start_load(i)

    def unit(i, _):
        slot = lax.rem(i, n_slots)
        load(i)[0].wait()

        @pl.when(i >= n_slots)
        def _():
            each_save(i - n_slots, lambda c: c.wait())

        dst[slot] = src[slot].T
        each_save(i, lambda c: c.start())

        @pl.when(i + n_slots < units)
        def _():
            start_load(i + n_slots)

        return 0

    lax.fori_loop(0, units, unit, 0)
    for i in range(units - n_slots, units):
        each_save(i, lambda c: c.wait())


def early_turn(n_stages, stage):
    return stage >= n_stages // 2


def prepare_kernel(n_stages, inputs, targets, w_in, w_rec, useq, tseq, win_t, wrec_t,
                   src, dst, wsrc, wdst, in_sem, out_sem, win_sem, wout_sem):
    rows, steps, _ = inputs.shape
    stage = lax.axis_index("stage")
    n_slots = src.shape[0]
    n_cols = steps // GROUP
    units = rows // GROUP * n_cols

    def turn(x, y):
        def load(i):
            slot = lax.rem(i, n_slots)
            return copy_of(x.at[pl.ds(pl.multiple_of(i // n_cols * GROUP, GROUP), GROUP),
                                pl.ds(pl.multiple_of(lax.rem(i, n_cols) * GROUP, GROUP), GROUP)], src.at[slot], in_sem.at[slot])

        def save(i):
            slot = lax.rem(i, n_slots)
            return copy_of(dst.at[slot], y.at[i // n_cols, pl.ds(lax.rem(i, n_cols) * GROUP, GROUP)], out_sem.at[slot])

        for i in range(min(n_slots, units)):
            load(i).start()

        def unit(i, _):
            slot = lax.rem(i, n_slots)
            load(i).wait()

            @pl.when(i >= n_slots)
            def _():
                save(i).wait()

            dst[slot] = jnp.swapaxes(src[slot], 0, 1)
            save(i).start()

            @pl.when(i + n_slots < units)
            def _():
                load(i + n_slots).start()

            return 0

        lax.fori_loop(0, units, unit, 0)
        for i in range(max(0, units - n_slots), units):
            save(i).wait()

    @pl.when(stage == 0)
    def _():
        turn(inputs, useq)

    @pl.when(stage == n_stages - 1)
    def _():
        turn(targets, tseq)

    @pl.when(early_turn(n_stages, stage))
    def _():
        turn_weights(w_in, w_rec, win_t, wrec_t, wsrc, wdst, win_sem, wout_sem)


def weight_scratch(hidden):
    dma = pltpu.SemaphoreType.DMA
    slots = 4
    return ([pltpu.VMEM((slots, hidden, hidden // NB), bf16), pltpu.VMEM((slots, hidden // NB, hidden), bf16)],
            [dma((slots,)), dma((slots, WIN))])


def run_prepare(n_stages, inputs, targets, w_in, w_rec):
    rows, steps, hidden = inputs.shape
    any_spec = pl.BlockSpec(memory_space=pl.ANY)
    dma = pltpu.SemaphoreType.DMA
    seq = jax.ShapeDtypeStruct((rows // GROUP, steps, GROUP, hidden), bf16)
    buffers, sems = weight_scratch(hidden)
    return pl.pallas_call(
        functools.partial(prepare_kernel, n_stages),
        out_shape=(seq, seq, jax.ShapeDtypeStruct((2, WIN, 2 * hidden, hidden // WIN), bf16),
                   jax.ShapeDtypeStruct((NB, hidden // 2, hidden), bf16)),
        in_specs=[any_spec] * 4, out_specs=(any_spec,) * 4,
        scratch_shapes=[pltpu.VMEM((4, GROUP, GROUP, hidden), bf16), pltpu.VMEM((4, GROUP, GROUP, hidden), bf16), *buffers,
                        dma((4,)), dma((4,)), *sems],
        compiler_params=pltpu.CompilerParams(vmem_limit_bytes=VMEM_LIMIT),
        name="lstm_prepare",
    )(inputs, targets, w_in, w_rec)


def late_turn_kernel(n_stages, w_in, w_rec, after, win_old, wrec_old, win_t, wrec_t, wsrc, wdst, win_sem, wout_sem):
    del after, win_old, wrec_old

    @pl.when(jnp.logical_not(early_turn(n_stages, lax.axis_index("stage"))))
    def _():
        turn_weights(w_in, w_rec, win_t, wrec_t, wsrc, wdst, win_sem, wout_sem)


def run_late_turn(n_stages, w_in, w_rec, after, win_t, wrec_t):
    any_spec = pl.BlockSpec(memory_space=pl.ANY)
    buffers, sems = weight_scratch(w_rec.shape[1])
    return pl.pallas_call(
        functools.partial(late_turn_kernel, n_stages),
        out_shape=(jax.ShapeDtypeStruct(win_t.shape, bf16), jax.ShapeDtypeStruct(wrec_t.shape, bf16)),
        in_specs=[any_spec] * 5, out_specs=(any_spec,) * 2, input_output_aliases={3: 0, 4: 1},
        scratch_shapes=[*buffers, *sems],
        compiler_params=pltpu.CompilerParams(vmem_limit_bytes=VMEM_LIMIT),
        name="lstm_late_turn",
    )(w_in, w_rec, after, win_t, wrec_t)


def forward_kernel(n_stages, steps, rows, hidden,
                   seq_ref, w_in, w_rec, bias, h_start, c_start, spans,
                   useq, hseq, gates, cseq,
                   wr, wi, uring, zin, gst, cst, hst, lens,
                   wr_sem, wi_sem, u_sem, g_sem, c_sem, h_sem, send_sem, recv_sem):
    bw = hidden // NB
    half = NB // 2
    hw = half * bw
    per = 4 // FWIN
    stage = lax.axis_index("stage")
    first = stage == 0
    sends = stage < n_stages - 1
    entry_signal(stage, n_stages)

    def wr_copies():
        return [copy_of(w_rec.at[0, :, pl.ds(g * hidden + j * bw, bw)], wr.at[j, :, pl.ds(g * bw, bw)], wr_sem.at[j, g])
                for j in range(NB) for g in range(4)]

    first_m = 2 - 2 * FWIN
    last_m = 2 * steps - 1

    def gate_of(t, i):
        return lax.rem(t + FWIN, FWIN) * per + i

    def slot_of(n):
        return lax.rem(n + 4 * FUNITS, FUNITS)

    def wi_copy(n):
        m = (n + 2 * FWIN * per) // per - 2 * FWIN
        t, hf = (m + 2 * FWIN) // 2 - FWIN, lax.rem(m + 2 * FWIN, 2)
        first_col = gate_of(t, n - per * m) * hidden + hf * hw
        return copy_of(w_in.at[0, :, pl.ds(pl.multiple_of(first_col, 128), hw)], wi.at[slot_of(n)], wi_sem.at[slot_of(n)])

    def turn_units(m):
        for i in range(per):
            wi_copy(per * m + i).wait()
        for k in range(per):
            n = per * (m - 1) + FUNITS + k

            @pl.when(n < per * (last_m + 1))
            def _(n=n):
                wi_copy(n).start()

    def u_copy(t):
        slot = lax.rem(t, FWIN + 1)
        return copy_of(useq.at[:, t], uring.at[slot], u_sem.at[0])

    def g_copy(t, hf):
        return copy_of(gst.at[pl.ds(hf * half, half)], gates.at[t, pl.ds(hf * half, half)], g_sem.at[hf])

    def c_copy(slot, t):
        return copy_of(cst.at[slot], cseq.at[t], c_sem.at[slot])

    def h_copy(slot, t):
        return copy_of(hst.at[slot], hseq.at[:, t], h_sem.at[slot])

    def send(slot, t):
        return pltpu.make_async_remote_copy(
            src_ref=hst.at[slot], dst_ref=useq.at[:, t], send_sem=send_sem.at[slot], recv_sem=recv_sem.at[t],
            device_id={"stage": lax.rem(stage + 1, n_stages)}, device_id_type=MESH)

    def fetch_u(t):
        @pl.when(t < steps)
        def _():
            @pl.when(jnp.logical_not(first))
            def _():
                send(0, t).wait_recv()
            u_copy(t).start()

    def await_u(t):
        @pl.when(t < steps)
        def _():
            u_copy(t).wait()

    def project(t, hf):
        u = jnp.concatenate([uring[lax.rem(t + i + 2 * (FWIN + 1), FWIN + 1)].reshape(rows, hidden) for i in range(FWIN)], axis=0)
        for i in range(per):
            g = gate_of(t, i)
            z = jnp.dot(u, wi[slot_of(per * (2 * t + hf) + i)], preferred_element_type=f32)
            z += bias[0:1, pl.ds(pl.multiple_of(g * hidden + hf * hw, 128), hw)]
            for k in range(FWIN):
                zin[4 * hf + g, lax.rem(t + k + 2 * FWIN, FWIN)] = z[k * rows:(k + 1) * rows]

    def recur(t, hf):
        cur, nxt = lax.rem(t, 2), lax.rem(t + 1, 2)
        live = lens[...] > t
        h = hst[cur].reshape(rows, hidden)
        h_twice = jnp.concatenate([h, h], axis=0)
        for j in range(hf * half, (hf + 1) * half):
            cols = slice(j * bw, (j + 1) * bw)
            z = jnp.dot(h_twice, wr[j], preferred_element_type=f32)
            z = jnp.maximum(z[:rows], z[rows:])
            at = (j - hf * half) * bw
            zi, zf, zg, zo = (z[:, g * bw:(g + 1) * bw] + zin[4 * hf + g, lax.rem(t, FWIN), :, at:at + bw] for g in range(4))
            gi = sigmoid(zi)
            gf = sigmoid(zf)
            gg = jnp.tanh(zg)
            go = sigmoid(zo)
            c_prev = cst[cur, :, cols]
            c_new = gf * c_prev + gi * gg
            h_new = go * jnp.tanh(c_new)
            cst[nxt, :, cols] = jnp.where(live, c_new, c_prev)
            hst[nxt, :, :, cols] = jnp.where(live, h_new, h[:, cols].astype(f32)).astype(bf16).reshape(rows // GROUP, GROUP, bw)
            gst[j, :, :bw] = gi
            gst[j, :, bw:2 * bw] = gf
            gst[j, :, 2 * bw:3 * bw] = gg
            gst[j, :, 3 * bw:] = go

    for n in range(per * first_m, per * (first_m - 1) + FUNITS):
        wi_copy(n).start()
    for c in wr_copies():
        c.start()
    fill_lens(spans, lens)
    entry_wait(stage, n_stages)
    begin = [copy_of(h_start.at[0, :, pl.ds(i * hw, hw)], gst.at[i], g_sem.at[i]) for i in range(2)]
    begin.append(copy_of(c_start.at[0], cst.at[0], c_sem.at[0]))
    for c in begin:
        c.start()
    for c in begin:
        c.wait()
    for i in range(2):
        hst[0, :, :, i * hw:(i + 1) * hw] = gst[i].astype(bf16).reshape(rows // GROUP, GROUP, hw)
    c_copy(0, 0).start()
    h_copy(0, 0).start()

    def warm(v, _):
        m = v + first_m
        t, hf = (m + 2 * FWIN) // 2 - FWIN, lax.rem(m + 2 * FWIN, 2)
        turn_units(m)

        @pl.when(hf == 0)
        def _():
            fetch_u(t + FWIN - 1)
            await_u(t + FWIN - 1)

        project(t, hf)
        return 0

    lax.fori_loop(0, -first_m, warm, 0)
    for c in wr_copies():
        c.wait()
    fetch_u(jnp.int32(FWIN - 1))

    def step(t, _):
        nxt = lax.rem(t + 1, 2)
        await_u(t + FWIN - 1)
        turn_units(2 * t)

        @pl.when(t >= 1)
        def _():
            c_copy(nxt, t).wait()
            h_copy(nxt, t).wait()
            g_copy(t, 0).wait()

        @pl.when(jnp.logical_and(t >= 2, sends))
        def _():
            send(nxt, t).wait_send()

        project(t, 0)
        recur(t, 0)

        g_copy(t, 0).start()
        turn_units(2 * t + 1)
        fetch_u(t + FWIN)

        @pl.when(t >= 1)
        def _():
            g_copy(t, 1).wait()

        project(t, 1)
        recur(t, 1)

        g_copy(t, 1).start()
        c_copy(nxt, t + 1).start()
        h_copy(nxt, t + 1).start()

        @pl.when(sends)
        def _():
            send(nxt, t).start()

        return 0

    lax.fori_loop(0, steps, step, 0)
    for hf in range(2):
        g_copy(0, hf).wait()
        c_copy(hf, 0).wait()
        h_copy(hf, 0).wait()

        @pl.when(sends)
        def _():
            send(hf, 0).wait_send()


def run_forward(n_stages, seq, w_in, w_rec, bias, h_start, c_start, spans):
    n_groups, steps, _, hidden = seq.shape
    rows = n_groups * GROUP
    bw = hidden // NB
    any_spec = pl.BlockSpec(memory_space=pl.ANY)
    vmem_spec = pl.BlockSpec(memory_space=pltpu.VMEM)
    dma = pltpu.SemaphoreType.DMA
    return pl.pallas_call(
        functools.partial(forward_kernel, n_stages, steps, rows, hidden),
        out_shape=(jax.ShapeDtypeStruct((n_groups, steps, GROUP, hidden), bf16),
                   jax.ShapeDtypeStruct((n_groups, steps + 1, GROUP, hidden), bf16),
                   jax.ShapeDtypeStruct((steps, NB, rows, 4 * bw), f32),
                   jax.ShapeDtypeStruct((steps + 1, rows, hidden), f32)),
        in_specs=[any_spec, any_spec, any_spec, vmem_spec, any_spec, any_spec, pl.BlockSpec(memory_space=pltpu.SMEM)],
        out_specs=(any_spec,) * 4,
        input_output_aliases={0: 0},
        scratch_shapes=[
            pltpu.VMEM((NB, hidden, 4 * bw), bf16),
            pltpu.VMEM((FUNITS, hidden, hidden // 2), bf16),
            pltpu.VMEM((FWIN + 1, n_groups, GROUP, hidden), bf16),
            pltpu.VMEM((8, FWIN, rows, hidden // 2), f32),
            pltpu.VMEM((NB, rows, 4 * bw), f32),
            pltpu.VMEM((2, rows, hidden), f32),
            pltpu.VMEM((2, n_groups, GROUP, hidden), bf16),
            pltpu.VMEM((rows, bw), jnp.int32),
            dma((NB, 4)), dma((FUNITS,)), dma((1,)), dma((2,)), dma((2,)), dma((2,)), dma((2,)), dma((steps,)),
        ],
        compiler_params=pltpu.CompilerParams(collective_id=0, has_side_effects=True, vmem_limit_bytes=VMEM_LIMIT),
        name="lstm_forward",
    )(seq, w_in, w_rec, bias, h_start, c_start, spans)


def backward_kernel(n_stages, steps, rows, hidden,
                    hseq, tseq, gates, cseq, win_t, wrec_t, spans,
                    drecv, dz_out, dh_out, dc_out, db_out, loss_out,
                    wt, wi, gin, cring, dbuf, ybuf, dzr, dh, dc, dbacc, lossacc, duacc, dust, lsend, lrecv, lens, scale,
                    wt_sem, wi_sem, g_sem, c_sem, d_sem, y_sem, dz_sem, out_sem, send_sem, recv_sem, lsend_sem, lrecv_sem):
    bw = hidden // NB
    n_groups = rows // GROUP
    half = NB // 2
    hw = half * bw
    part = hidden // WIN
    ring = WIN
    pad = WIN - 1
    stage = lax.axis_index("stage")
    top = stage == n_stages - 1
    sends = stage > 0
    last = steps - 1
    halves = jnp.where(sends, 2 * (steps + pad), 2 * steps)
    entry_signal(stage, n_stages)

    def wt_copies():
        return [copy_of(wrec_t.at[j], wt.at[j], wt_sem.at[j]) for j in range(NB)]

    def part_of(t):
        return lax.rem(t + WIN, WIN)

    def wi_copy(m, i):
        n = 2 * m + i
        t, hf = last - m // 2, lax.rem(m, 2)
        return copy_of(win_t.at[hf, part_of(t), pl.ds(i * hidden, hidden)], wi.at[lax.rem(n, UNITS)], wi_sem.at[lax.rem(n, UNITS)])

    def turn_units(m):
        for i in range(2):
            wi_copy(m, i).wait()

        @pl.when(m + 1 < halves)
        def _():
            wi_copy(m + 1, 1).start()

        @pl.when(m + 2 < halves)
        def _():
            wi_copy(m + 2, 0).start()

    def g_copy(t, hf):
        return copy_of(gates.at[t, pl.ds(hf * half, half)], gin.at[pl.ds(hf * half, half)], g_sem.at[hf])

    def c_copy(i):
        slot = lax.rem(i, 3)
        return copy_of(cseq.at[i], cring.at[slot], c_sem.at[slot])

    def own_copies(t):
        return [copy_of(hseq.at[:, t + 1, :, pl.ds(q * part, part)], dbuf.at[lax.rem(t, 2), q], d_sem.at[q])
                for q in range(WIN)]

    def y_copy(t):
        return copy_of(tseq.at[:, t], ybuf.at[lax.rem(t, 2)], y_sem.at[0])

    def recv_copies(t):
        return [copy_of(drecv.at[q, t + pad], dbuf.at[lax.rem(t, 2), q], d_sem.at[q]) for q in range(WIN)]

    def dz_copies(t):
        slot = lax.rem(t, ring)
        return [copy_of(dzr.at[slot, hf, :, :, pl.ds(g * hw, hw)], dz_out.at[:, t, :, pl.ds(g * hidden + hf * hw, hw)],
                        dz_sem.at[slot, 4 * hf + g]) for hf in range(2) for g in range(4)]

    def send(t):
        return pltpu.make_async_remote_copy(
            src_ref=dust.at[0], dst_ref=drecv.at[part_of(t), pl.ds(t + pad, WIN)],
            send_sem=send_sem.at[0], recv_sem=recv_sem.at[t + pad],
            device_id={"stage": lax.rem(stage + n_stages - 1, n_stages)}, device_id_type=MESH)

    def fetch_d(t):
        @pl.when(top)
        def _():
            for c in own_copies(t):
                c.start()
            y_copy(t).start()

        @pl.when(jnp.logical_not(top))
        def _():
            send(t - pad).wait_recv()
            for c in recv_copies(t):
                c.start()

    def await_d(t):
        for c in recv_copies(t):
            c.wait()

        @pl.when(top)
        def _():
            y_copy(t).wait()

    def input_grad(t, hf):
        d = jnp.concatenate([dzr[lax.rem(t + i + ring, ring), hf].reshape(rows, 2 * hidden) for i in range(WIN)], axis=0)
        n = 2 * (2 * (last - t) + hf)
        du = jnp.dot(d[:, :hidden], wi[lax.rem(n, UNITS)], preferred_element_type=f32)
        du += jnp.dot(d[:, hidden:], wi[lax.rem(n + 1, UNITS)], preferred_element_type=f32)
        if hf == 0:
            duacc[...] = du
        else:
            du = (du + duacc[...]).astype(bf16)
            for i in range(WIN):
                dust[0, i] = du[i * rows:(i + 1) * rows].reshape(n_groups, GROUP, part)

    def flat(x):
        return x.reshape(rows, x.shape[-1])

    def fold(x):
        return x.reshape(rows // 8, 8, x.shape[-1]).sum(axis=0)

    def recur(t, hf):
        cur, nxt = lax.rem(t, 2), lax.rem(t + 1, 2)
        slot = cur
        live = lens[...] > t
        sc = scale[0:1, :]
        total = None
        for j in range(hf * half, (hf + 1) * half):
            cols = slice(j * bw, (j + 1) * bw)
            q, off = j * bw // part, j * bw % part
            gi, gf = gin[j, :, :bw], gin[j, :, bw:2 * bw]
            gg, go = gin[j, :, 2 * bw:3 * bw], gin[j, :, 3 * bw:]
            err = jnp.where(live, flat(dbuf[slot, q, :, :, off:off + bw]).astype(f32) - flat(ybuf[slot, :, :, cols]).astype(f32), 0.0)
            lossacc[:, cols] += fold(err * err)
            d_total = dh[cur, :, cols] + err * sc
            c_prev = cring[lax.rem(t, 3), :, cols]
            tanh_c = jnp.tanh(cring[lax.rem(t + 1, 3), :, cols])
            dc_old = dc[:, cols]
            d_c = dc_old + d_total * go * (1.0 - tanh_c * tanh_c)
            gates_d = (d_c * gg * gi * (1.0 - gi),
                     d_c * c_prev * gf * (1.0 - gf),
                     d_c * gi * (1.0 - gg * gg),
                     d_total * tanh_c * go * (1.0 - go))
            low = []
            for g in range(4):
                dz = jnp.where(live, gates_d[g], 0.0)
                dbacc[j, :, g * bw:(g + 1) * bw] += fold(dz)
                dz = dz.astype(bf16)
                at = g * hw + (j - hf * half) * bw
                dzr[lax.rem(t, ring), hf, :, :, at:at + bw] = dz.reshape(n_groups, GROUP, bw)
                low.append(dz)
            dc[:, cols] = jnp.where(live, d_c * gf, dc_old)
            keep = jnp.where(live, 0.0, d_total)
            if hf == 0:
                dh[nxt, :, cols] = keep
            else:
                dh[nxt, :, cols] += keep
            low = jnp.concatenate(low, axis=1)
            low = jnp.concatenate([low, low], axis=0)
            r = jnp.dot(low, wt[j], preferred_element_type=f32)
            total = r if total is None else total + r
        total = jnp.maximum(total[:rows], total[rows:])
        if hf == 0:
            dh[nxt, :, :hw] += total[:, :hw]
            dh[nxt, :, hw:] = total[:, hw:]
        else:
            dh[nxt] += total

    for c in wt_copies():
        c.start()
    wi_copy(0, 0).start()
    wi_copy(0, 1).start()
    wi_copy(1, 0).start()
    g_copy(last, 0).start()
    c_copy(last + 1).start()
    c_copy(last).start()
    fill_lens(spans, lens)
    entry_wait(stage, n_stages)
    n_active = spans[0]
    for r in range(1, rows):
        n_active += spans[r]
    share = 1.0 / jnp.full(scale.shape, n_active.astype(f32))
    scale[...] = jnp.where(top, share, 1.0)
    dh[...] = jnp.zeros_like(dh)
    dc[...] = jnp.zeros_like(dc)
    dbacc[...] = jnp.zeros_like(dbacc)
    lossacc[...] = jnp.zeros_like(lossacc)
    ybuf[...] = jnp.zeros_like(ybuf)
    for i in range(ring):
        dzr[i] = jnp.zeros_like(dzr[i])

    @pl.when(jnp.logical_not(top))
    def _():
        for i in range(pad):
            send(last - i).wait_recv()

    fetch_d(last)
    c_copy(last + 1).wait()
    for c in wt_copies():
        c.wait()

    def step(v, _):
        t = last - v
        await_d(t)
        g_copy(t, 0).wait()
        c_copy(t).wait()

        @pl.when(v >= ring)
        def _():
            for c in dz_copies(t + ring):
                c.wait()

        g_copy(t, 1).start()
        turn_units(2 * v)

        @pl.when(t >= 1)
        def _():
            c_copy(t - 1).start()

        recur(t, 0)
        input_grad(t, 0)

        g_copy(t, 1).wait()

        @pl.when(jnp.logical_and(v >= 1, sends))
        def _():
            send(t + 1).wait_send()

        turn_units(2 * v + 1)

        @pl.when(t >= 1)
        def _():
            g_copy(t - 1, 0).start()
            fetch_d(t - 1)

        recur(t, 1)
        input_grad(t, 1)
        for c in dz_copies(t):
            c.start()

        @pl.when(sends)
        def _():
            send(t).start()

        return 0

    lax.fori_loop(0, steps, step, 0)

    for i in range(ring):
        for c in dz_copies(i):
            c.wait()
    outs = [copy_of(dh.at[1], dh_out, out_sem.at[0]), copy_of(dc, dc_out, out_sem.at[1]),
            copy_of(dbacc, db_out, out_sem.at[2])]
    for c in outs:
        c.start()

    def tell():
        return pltpu.make_async_remote_copy(
            src_ref=lsend, dst_ref=lrecv, send_sem=lsend_sem.at[0], recv_sem=lrecv_sem.at[0],
            device_id={"stage": lax.rem(stage + n_stages - 1, n_stages)}, device_id_type=MESH)

    @pl.when(top)
    def _():
        lsend[...] = sum(lossacc[:, i * 128:(i + 1) * 128] for i in range(hidden // 128))

    @pl.when(sends)
    def _():
        def drain(v, _):
            t = -1 - v
            turn_units(2 * (last - t))
            input_grad(t, 0)
            turn_units(2 * (last - t) + 1)
            send(t + 1).wait_send()
            input_grad(t, 1)
            send(t).start()
            return 0

        lax.fori_loop(0, pad, drain, 0)
        send(-pad).wait_send()

    @pl.when(jnp.logical_not(top))
    def _():
        tell().wait_recv()
        lsend[...] = lrecv[...]

    for c in outs:
        c.wait()
    loss_copy = copy_of(lsend, loss_out, out_sem.at[3])
    loss_copy.start()
    loss_copy.wait()

    @pl.when(sends)
    def _():
        tell().start()
        tell().wait_send()


def run_backward(n_stages, hseq, tseq, gates, cseq, win_t, wrec_t, spans):
    n_groups, steps, _, hidden = tseq.shape
    rows = n_groups * GROUP
    bw = hidden // NB
    part = hidden // WIN
    any_spec = pl.BlockSpec(memory_space=pl.ANY)
    dma = pltpu.SemaphoreType.DMA
    return pl.pallas_call(
        functools.partial(backward_kernel, n_stages, steps, rows, hidden),
        out_shape=(jax.ShapeDtypeStruct((WIN, steps + 2 * (WIN - 1), n_groups, GROUP, part), bf16),
                   jax.ShapeDtypeStruct((n_groups, steps, GROUP, 4 * hidden), bf16),
                   jax.ShapeDtypeStruct((rows, hidden), f32),
                   jax.ShapeDtypeStruct((rows, hidden), f32),
                   jax.ShapeDtypeStruct((NB, 8, 4 * bw), f32),
                   jax.ShapeDtypeStruct((8, 128), f32)),
        in_specs=[any_spec] * 6 + [pl.BlockSpec(memory_space=pltpu.SMEM)],
        out_specs=(any_spec,) * 6,
        scratch_shapes=[
            pltpu.VMEM((NB, 4 * bw, hidden), bf16),
            pltpu.VMEM((UNITS, hidden, part), bf16),
            pltpu.VMEM((NB, rows, 4 * bw), f32),
            pltpu.VMEM((3, rows, hidden), f32),
            pltpu.VMEM((2, WIN, n_groups, GROUP, part), bf16),
            pltpu.VMEM((2, n_groups, GROUP, hidden), bf16),
            pltpu.VMEM((WIN, 2, n_groups, GROUP, 2 * hidden), bf16),
            pltpu.VMEM((2, rows, hidden), f32),
            pltpu.VMEM((rows, hidden), f32),
            pltpu.VMEM((NB, 8, 4 * bw), f32),
            pltpu.VMEM((8, hidden), f32),
            pltpu.VMEM((WIN * rows, part), f32),
            pltpu.VMEM((1, WIN, n_groups, GROUP, part), bf16),
            pltpu.VMEM((8, 128), f32),
            pltpu.VMEM((8, 128), f32),
            pltpu.VMEM((rows, bw), jnp.int32),
            pltpu.VMEM((8, bw), f32),
            dma((NB,)), dma((UNITS,)), dma((2,)), dma((3,)), dma((WIN,)), dma((1,)), dma((WIN, 8)), dma((4,)), dma((1,)),
            dma((steps + WIN - 1,)), dma((1,)), dma((1,)),
        ],
        compiler_params=pltpu.CompilerParams(collective_id=1, has_side_effects=True, vmem_limit_bytes=VMEM_LIMIT),
        name="lstm_backward",
    )(hseq, tseq, gates, cseq, win_t, wrec_t, spans)


def grads_kernel(steps, hidden, spans, useq, hseq, dz, dh, dc, db, sq,
                 g_in, g_rec, g_bias, dh_out, dc_out, loss_out,
                 xs, dzb, acc, state, x_sem, z_sem, o_sem, s_sem):
    n_groups = useq.shape[0]
    tile = dzb.shape[-1]
    n_tiles = dz.shape[-1] // tile
    bw = hidden // NB
    seen = [spans[i * GROUP] for i in range(n_groups)]
    first = [0]
    for i in range(n_groups):
        first.append(first[-1] + seen[i])
    total = first[-1]
    sizes = []
    size = 1
    while size <= steps:
        sizes.insert(0, size)
        size *= 2

    def pieces(make, act):
        for i in range(n_groups):
            for size in sizes:
                done = seen[i] // (2 * size) * (2 * size)

                @pl.when(seen[i] // size % 2 == 1)
                def _(i=i, size=size, done=done):
                    act(make(i, pl.ds(done, size), pl.ds(first[i] + done, size)))

    def load_x(w, act):
        src = useq if w == 0 else hseq
        pieces(lambda i, at, to: copy_of(src.at[i, at], xs.at[w, to], x_sem.at[w]), act)

    def load_z(n, slot, act):
        cols = pl.ds(pl.multiple_of(n * tile, tile), tile)
        pieces(lambda i, at, to: copy_of(dz.at[i, at, :, cols], dzb.at[slot, to], z_sem.at[slot]), act)

    def start(c):
        c.start()

    def wait(c):
        c.wait()

    def store(w, n, act):
        cols = pl.ds(pl.multiple_of(n * tile, tile), tile)

        @pl.when(w == 0)
        def _():
            act(copy_of(acc.at[0], g_in.at[0, :, cols], o_sem.at[0]))

        @pl.when(w == 1)
        def _():
            act(copy_of(acc.at[1], g_rec.at[0, :, cols], o_sem.at[1]))

    for slot in range(2):
        xs[slot, pl.ds(total, GROUP)] = jnp.zeros((GROUP, GROUP, hidden), bf16)
        dzb[slot, pl.ds(total, GROUP)] = jnp.zeros((GROUP, GROUP, tile), bf16)
    load_z(0, 0, start)
    load_x(0, start)
    load_x(1, start)
    states = [(copy_of(x, state.at[i], s_sem.at[i]), copy_of(state.at[i], y.at[0], s_sem.at[i]))
              for i, (x, y) in enumerate(((dh, dh_out), (dc, dc_out)))]
    for c, _ in states:
        c.start()
    for j in range(NB):
        for g in range(4):
            g_bias[0:1, g * hidden + j * bw:g * hidden + (j + 1) * bw] = jnp.sum(
                db[j, :, g * bw:(g + 1) * bw], axis=0, keepdims=True)
    n_active = spans[0]
    for r in range(1, n_groups * GROUP):
        n_active += spans[r]
    loss_out[...] = jnp.full((1, 1), jnp.sum(sq[...]) / (2.0 * n_active.astype(f32)))

    def product(w, slot, at, depth, begin):
        rhs = dzb[slot, pl.ds(at, depth)].reshape(depth * GROUP, tile)
        mc = min(512, hidden)
        for m in range(hidden // mc):
            lhs = xs[w, pl.ds(at, depth), :, m * mc:(m + 1) * mc].reshape(depth * GROUP, mc)
            r = lax.dot_general(lhs, rhs, (((0,), (0,)), ((), ())), preferred_element_type=f32)
            acc[w, m * mc:(m + 1) * mc] = r if begin else acc[w, m * mc:(m + 1) * mc] + r

    units = (total + 15) // 16

    def one_tile(v, _):
        n, w = v // 2, lax.rem(v, 2)
        slot = lax.rem(n, 2)

        @pl.when(w == 0)
        def _():
            @pl.when(n + 1 < n_tiles)
            def _():
                load_z(n + 1, 1 - slot, start)

            load_z(n, slot, wait)

        @pl.when(v == 0)
        def _():
            load_x(0, wait)

        @pl.when(v == 1)
        def _():
            load_x(1, wait)

        @pl.when(n >= 1)
        def _():
            store(w, n, wait)

        product(w, slot, 0, 128, True)

        def more(b, _):
            product(w, slot, 128 + b * 64, 64, False)
            return 0

        rest = jnp.maximum(units - 8, 0)
        lax.fori_loop(0, rest // 4, more, 0)

        @pl.when(rest // 2 % 2 == 1)
        def _():
            product(w, slot, 128 + rest // 4 * 64, 32, False)

        @pl.when(rest % 2 == 1)
        def _():
            product(w, slot, 128 + rest // 2 * 32, 16, False)

        store(w, n, start)
        return 0

    lax.fori_loop(0, 2 * n_tiles, one_tile, 0)
    for c, d in states:
        c.wait()
        d.start()
    store(0, 0, wait)
    store(1, 0, wait)
    for _, d in states:
        d.wait()


def run_grads(useq, hseq, dz, dh, dc, db, sq, spans):
    n_groups, steps, _, hidden = useq.shape
    rows = n_groups * GROUP
    any_spec = pl.BlockSpec(memory_space=pl.ANY)
    vmem_spec = pl.BlockSpec(memory_space=pltpu.VMEM)
    blocks = n_groups * steps + GROUP
    tile = 512
    dma = pltpu.SemaphoreType.DMA
    out = jax.ShapeDtypeStruct((1, hidden, 4 * hidden), f32)
    state = jax.ShapeDtypeStruct((1, rows, hidden), f32)
    return pl.pallas_call(
        functools.partial(grads_kernel, steps, hidden),
        out_shape=(out, out, jax.ShapeDtypeStruct((1, 4 * hidden), f32), state, state, jax.ShapeDtypeStruct((1, 1), f32)),
        in_specs=[pl.BlockSpec(memory_space=pltpu.SMEM)] + [any_spec] * 5 + [vmem_spec] * 2,
        out_specs=(any_spec, any_spec, vmem_spec, any_spec, any_spec, vmem_spec),
        scratch_shapes=[
            pltpu.VMEM((2, blocks, GROUP, hidden), bf16),
            pltpu.VMEM((2, blocks, GROUP, tile), bf16),
            pltpu.VMEM((2, hidden, tile), f32),
            pltpu.VMEM((2, rows, hidden), f32),
            dma((2,)), dma((2,)), dma((2,)), dma((2,)),
        ],
        compiler_params=pltpu.CompilerParams(vmem_limit_bytes=VMEM_LIMIT),
        name="lstm_weight_grads",
    )(spans, useq, hseq, dz, dh, dc, db, sq)


def solution(mesh):
    n_stages = mesh.shape["stage"]

    def local_program(inputs, targets, lengths, w_in, w_rec, gate_bias, h_init, c_init):
        useq, tseq, win_t, wrec_t = run_prepare(n_stages, inputs, targets, w_in, w_rec)
        useq, hseq, gates, cseq = run_forward(n_stages, useq, w_in, w_rec, gate_bias, h_init, c_init, lengths)
        win_t, wrec_t = run_late_turn(n_stages, w_in, w_rec, cseq, win_t, wrec_t)
        _, dz, dh0, dc0, db, sq = run_backward(n_stages, hseq, tseq, gates, cseq, win_t, wrec_t, lengths)
        grad_in, grad_rec, grad_bias, dh0, dc0, loss = run_grads(useq, hseq, dz, dh0, dc0, db, sq, lengths)
        return loss.reshape(1), grad_in, grad_rec, grad_bias, dh0, dc0

    row_spec = P("data", None, None)
    layer_spec = P("stage", None, None)
    state_spec = P("stage", "data", None)
    grad_spec = P(("data", "stage"), None, None)
    return jax.shard_map(local_program, mesh=mesh,
                         in_specs=(row_spec, row_spec, P("data"), layer_spec, layer_spec, P("stage", None), state_spec, state_spec),
                         out_specs=(P("data"), grad_spec, grad_spec, P(("data", "stage"), None), state_spec, state_spec),
                         check_vma=False)
```

```python
import functools

import jax
import jax.numpy as jnp
from jax import lax
from jax.experimental import pallas as pl
from jax.experimental.pallas import tpu as pltpu
from jax.sharding import PartitionSpec as P

MESH = pl.DeviceIdType.MESH
NB = 8
FWIN = 2
WIN = 2
FUNITS = 5
UNITS = 5
RING = 4
GROUP = 16
VMEM_LIMIT = 67043328
f32 = jnp.float32
bf16 = jnp.bfloat16


def sigmoid(x):
    return 0.5 * jnp.tanh(0.5 * x) + 0.5


def copy_of(src, dst, sem):
    return pltpu.make_async_copy(src, dst, sem)


def entry_signal(stage, n_stages):
    barrier = pltpu.get_barrier_semaphore()

    @pl.when(stage > 0)
    def _():
        pl.semaphore_signal(barrier, inc=1, device_id={"stage": lax.rem(stage + n_stages - 1, n_stages)}, device_id_type=MESH)

    @pl.when(stage < n_stages - 1)
    def _():
        pl.semaphore_signal(barrier, inc=1, device_id={"stage": lax.rem(stage + 1, n_stages)}, device_id_type=MESH)


def entry_wait(stage, n_stages):
    peers = jnp.minimum(stage, 1) + jnp.minimum(n_stages - 1 - stage, 1)
    pl.semaphore_wait(pltpu.get_barrier_semaphore(), peers)


def fill_lens(spans, lens):
    for r in range(lens.shape[0]):
        lens[r:r + 1, :] = jnp.full((1, lens.shape[1]), spans[r], jnp.int32)


def turn_weights(w_in, w_rec, win_t, wrec_t, src, dst, in_sem, out_sem):
    hidden = w_rec.shape[1]
    bw = hidden // NB
    per_half = NB // 2
    n_parts = win_t.shape[1]
    part = hidden // n_parts
    n_slots = src.shape[0]

    def load(i):
        slot = lax.rem(i, n_slots)
        j, g = lax.rem(i, 4 * NB) // 4, lax.rem(i, 4)
        cols = pl.ds(pl.multiple_of(g * hidden + j * bw, 128), bw)
        return (copy_of(w_rec.at[0, :, cols], src.at[slot], in_sem.at[slot]),
                copy_of(w_in.at[0, :, cols], src.at[slot], in_sem.at[slot]))

    def save(i):
        slot = lax.rem(i, n_slots)
        j, g = lax.rem(i, 4 * NB) // 4, lax.rem(i, 4)
        rec = copy_of(dst.at[slot], wrec_t.at[j, pl.ds(pl.multiple_of(g * bw, 8), bw)], out_sem.at[slot, 0])
        at = pl.multiple_of(g * per_half * bw + lax.rem(j, per_half) * bw, 8)
        ins = [copy_of(dst.at[slot, :, pl.ds(q * part, part)], win_t.at[j // per_half, q, pl.ds(at, bw)], out_sem.at[slot, q])
               for q in range(n_parts)]
        return [rec], ins

    units = 8 * NB

    def both(i, rec_do, in_do):
        @pl.when(i < 4 * NB)
        def _():
            rec_do()

        @pl.when(i >= 4 * NB)
        def _():
            in_do()

    def start_load(i):
        both(i, lambda: load(i)[0].start(), lambda: load(i)[1].start())

    def each_save(i, act):
        both(i, lambda: [act(c) for c in save(i)[0]], lambda: [act(c) for c in save(i)[1]])

    for i in range(n_slots):
        start_load(i)

    def unit(i, _):
        slot = lax.rem(i, n_slots)
        load(i)[0].wait()

        @pl.when(i >= n_slots)
        def _():
            each_save(i - n_slots, lambda c: c.wait())

        dst[slot] = src[slot].T
        each_save(i, lambda c: c.start())

        @pl.when(i + n_slots < units)
        def _():
            start_load(i + n_slots)

        return 0

    lax.fori_loop(0, units, unit, 0)
    for i in range(units - n_slots, units):
        each_save(i, lambda c: c.wait())


def early_turn(n_stages, stage):
    return stage >= n_stages // 2


def prepare_kernel(n_stages, inputs, targets, w_in, w_rec, useq, tseq, win_t, wrec_t,
                   src, dst, wsrc, wdst, in_sem, out_sem, win_sem, wout_sem):
    rows, steps, _ = inputs.shape
    stage = lax.axis_index("stage")
    n_slots = src.shape[0]
    n_cols = steps // GROUP
    units = rows // GROUP * n_cols

    def turn(x, y):
        def load(i):
            slot = lax.rem(i, n_slots)
            return copy_of(x.at[pl.ds(pl.multiple_of(i // n_cols * GROUP, GROUP), GROUP),
                                pl.ds(pl.multiple_of(lax.rem(i, n_cols) * GROUP, GROUP), GROUP)], src.at[slot], in_sem.at[slot])

        def save(i):
            slot = lax.rem(i, n_slots)
            return copy_of(dst.at[slot], y.at[i // n_cols, pl.ds(lax.rem(i, n_cols) * GROUP, GROUP)], out_sem.at[slot])

        for i in range(min(n_slots, units)):
            load(i).start()

        def unit(i, _):
            slot = lax.rem(i, n_slots)
            load(i).wait()

            @pl.when(i >= n_slots)
            def _():
                save(i).wait()

            dst[slot] = jnp.swapaxes(src[slot], 0, 1)
            save(i).start()

            @pl.when(i + n_slots < units)
            def _():
                load(i + n_slots).start()

            return 0

        lax.fori_loop(0, units, unit, 0)
        for i in range(max(0, units - n_slots), units):
            save(i).wait()

    @pl.when(stage == 0)
    def _():
        turn(inputs, useq)

    @pl.when(stage == n_stages - 1)
    def _():
        turn(targets, tseq)

    @pl.when(early_turn(n_stages, stage))
    def _():
        turn_weights(w_in, w_rec, win_t, wrec_t, wsrc, wdst, win_sem, wout_sem)


def weight_scratch(hidden):
    dma = pltpu.SemaphoreType.DMA
    slots = 4
    return ([pltpu.VMEM((slots, hidden, hidden // NB), bf16), pltpu.VMEM((slots, hidden // NB, hidden), bf16)],
            [dma((slots,)), dma((slots, WIN))])


def run_prepare(n_stages, inputs, targets, w_in, w_rec):
    rows, steps, hidden = inputs.shape
    any_spec = pl.BlockSpec(memory_space=pl.ANY)
    dma = pltpu.SemaphoreType.DMA
    seq = jax.ShapeDtypeStruct((rows // GROUP, steps, GROUP, hidden), bf16)
    buffers, sems = weight_scratch(hidden)
    return pl.pallas_call(
        functools.partial(prepare_kernel, n_stages),
        out_shape=(seq, seq, jax.ShapeDtypeStruct((2, WIN, 2 * hidden, hidden // WIN), bf16),
                   jax.ShapeDtypeStruct((NB, hidden // 2, hidden), bf16)),
        in_specs=[any_spec] * 4, out_specs=(any_spec,) * 4,
        scratch_shapes=[pltpu.VMEM((4, GROUP, GROUP, hidden), bf16), pltpu.VMEM((4, GROUP, GROUP, hidden), bf16), *buffers,
                        dma((4,)), dma((4,)), *sems],
        compiler_params=pltpu.CompilerParams(vmem_limit_bytes=VMEM_LIMIT),
        name="lstm_prepare",
    )(inputs, targets, w_in, w_rec)


def late_turn_kernel(n_stages, w_in, w_rec, after, win_old, wrec_old, win_t, wrec_t, wsrc, wdst, win_sem, wout_sem):
    del after, win_old, wrec_old

    @pl.when(jnp.logical_not(early_turn(n_stages, lax.axis_index("stage"))))
    def _():
        turn_weights(w_in, w_rec, win_t, wrec_t, wsrc, wdst, win_sem, wout_sem)


def run_late_turn(n_stages, w_in, w_rec, after, win_t, wrec_t):
    any_spec = pl.BlockSpec(memory_space=pl.ANY)
    buffers, sems = weight_scratch(w_rec.shape[1])
    return pl.pallas_call(
        functools.partial(late_turn_kernel, n_stages),
        out_shape=(jax.ShapeDtypeStruct(win_t.shape, bf16), jax.ShapeDtypeStruct(wrec_t.shape, bf16)),
        in_specs=[any_spec] * 5, out_specs=(any_spec,) * 2, input_output_aliases={3: 0, 4: 1},
        scratch_shapes=[*buffers, *sems],
        compiler_params=pltpu.CompilerParams(vmem_limit_bytes=VMEM_LIMIT),
        name="lstm_late_turn",
    )(w_in, w_rec, after, win_t, wrec_t)


def forward_kernel(n_stages, steps, rows, hidden,
                   seq_ref, w_in, w_rec, bias, h_start, c_start, spans,
                   useq, hseq, gates, cseq,
                   wr, wi, uring, zin, gst, cst, hst, lens,
                   wr_sem, wi_sem, u_sem, g_sem, c_sem, h_sem, send_sem, recv_sem, keep_sem, credit):
    bw = hidden // NB
    half = NB // 2
    hw = half * bw
    per = 4 // FWIN
    stage = lax.axis_index("stage")
    first = stage == 0
    sends = stage < n_stages - 1
    entry_signal(stage, n_stages)

    def wr_copies(hf):
        return [copy_of(w_rec.at[0, :, pl.ds(g * hidden + j * bw, bw)], wr.at[j, :, pl.ds(g * bw, bw)], wr_sem.at[j, g])
                for j in range(hf * half, (hf + 1) * half) for g in range(4)]

    first_m = 2 - 2 * FWIN
    last_m = 2 * steps - 1

    def gate_of(t, i):
        return lax.rem(t + FWIN, FWIN) * per + i

    def slot_of(n):
        return lax.rem(n + 4 * FUNITS, FUNITS)

    def wi_copy(n):
        m = (n + 2 * FWIN * per) // per - 2 * FWIN
        t, hf = (m + 2 * FWIN) // 2 - FWIN, lax.rem(m + 2 * FWIN, 2)
        first_col = gate_of(t, n - per * m) * hidden + hf * hw
        return copy_of(w_in.at[0, :, pl.ds(pl.multiple_of(first_col, 128), hw)], wi.at[slot_of(n)], wi_sem.at[slot_of(n)])

    def turn_units(m):
        for i in range(per):
            wi_copy(per * m + i).wait()
        for k in range(per):
            n = per * (m - 1) + FUNITS + k

            @pl.when(n < per * (last_m + 1))
            def _(n=n):
                wi_copy(n).start()

    def u_slot(t):
        return lax.rem(t + 2 * RING, RING)

    def u_copy(t):
        return copy_of(useq.at[:, t], uring.at[u_slot(t)], u_sem.at[0])

    def u_keep(t):
        return copy_of(uring.at[u_slot(t)], useq.at[:, t], keep_sem.at[u_slot(t)])

    def g_copy(t, hf):
        return copy_of(gst.at[pl.ds(hf * half, half)], gates.at[t, pl.ds(hf * half, half)], g_sem.at[hf])

    def c_copy(slot, t):
        return copy_of(cst.at[slot], cseq.at[t], c_sem.at[slot])

    def h_copy(slot, t):
        return copy_of(hst.at[slot], hseq.at[:, t], h_sem.at[slot])

    def send(slot, t):
        return pltpu.make_async_remote_copy(
            src_ref=hst.at[slot], dst_ref=uring.at[u_slot(t)], send_sem=send_sem.at[slot], recv_sem=recv_sem.at[t],
            device_id={"stage": lax.rem(stage + 1, n_stages)}, device_id_type=MESH)

    def fetch_u(t):
        @pl.when(jnp.logical_and(first, t < steps))
        def _():
            u_copy(t).start()

    def await_u(t):
        @pl.when(jnp.logical_and(first, t < steps))
        def _():
            u_copy(t).wait()

        @pl.when(jnp.logical_and(jnp.logical_not(first), t < steps))
        def _():
            send(0, t).wait_recv()
            u_keep(t).start()

    def release_u(t):
        @pl.when(jnp.logical_not(first))
        def _():
            u_keep(t).wait()

            @pl.when(t < steps - RING)
            def _():
                pl.semaphore_signal(credit, inc=1, device_id={"stage": lax.rem(stage + n_stages - 1, n_stages)},
                                    device_id_type=MESH)

    def project(t, hf):
        u = jnp.concatenate([uring[u_slot(jnp.maximum(t + i, 0))].reshape(rows, hidden) for i in range(FWIN)], axis=0)
        for i in range(per):
            g = gate_of(t, i)
            z = jnp.dot(u, wi[slot_of(per * (2 * t + hf) + i)], preferred_element_type=f32)
            z += bias[0:1, pl.ds(pl.multiple_of(g * hidden + hf * hw, 128), hw)]
            for k in range(FWIN):
                zin[4 * hf + g, lax.rem(t + k + 2 * FWIN, FWIN)] = z[k * rows:(k + 1) * rows]

    def recur(t, hf):
        cur, nxt = lax.rem(t, 2), lax.rem(t + 1, 2)
        live = lens[...] > t
        h = hst[cur].reshape(rows, hidden)
        h_twice = jnp.concatenate([h, h], axis=0)
        for j in range(hf * half, (hf + 1) * half):
            cols = slice(j * bw, (j + 1) * bw)
            z = jnp.dot(h_twice, wr[j], preferred_element_type=f32)
            z = jnp.maximum(z[:rows], z[rows:])
            at = (j - hf * half) * bw
            zi, zf, zg, zo = (z[:, g * bw:(g + 1) * bw] + zin[4 * hf + g, lax.rem(t, FWIN), :, at:at + bw] for g in range(4))
            gi = sigmoid(zi)
            gf = sigmoid(zf)
            gg = jnp.tanh(zg)
            go = sigmoid(zo)
            c_prev = cst[cur, :, cols]
            c_new = gf * c_prev + gi * gg
            h_new = go * jnp.tanh(c_new)
            cst[nxt, :, cols] = jnp.where(live, c_new, c_prev)
            hst[nxt, :, :, cols] = jnp.where(live, h_new, h[:, cols].astype(f32)).astype(bf16).reshape(rows // GROUP, GROUP, bw)
            gst[j, :, :bw] = gi
            gst[j, :, bw:2 * bw] = gf
            gst[j, :, 2 * bw:3 * bw] = gg
            gst[j, :, 3 * bw:] = go

    for n in range(per * first_m, per * (first_m - 1) + FUNITS):
        wi_copy(n).start()
    for c in wr_copies(0) + wr_copies(1):
        c.start()
    fill_lens(spans, lens)
    entry_wait(stage, n_stages)
    begin = [copy_of(h_start.at[0, :, pl.ds(i * hw, hw)], gst.at[i], g_sem.at[i]) for i in range(2)]
    begin.append(copy_of(c_start.at[0], cst.at[0], c_sem.at[0]))
    for c in begin:
        c.start()
    for c in begin:
        c.wait()
    for i in range(2):
        hst[0, :, :, i * hw:(i + 1) * hw] = gst[i].astype(bf16).reshape(rows // GROUP, GROUP, hw)
    c_copy(0, 0).start()
    h_copy(0, 0).start()

    def warm(v, _):
        m = v + first_m
        t, hf = (m + 2 * FWIN) // 2 - FWIN, lax.rem(m + 2 * FWIN, 2)
        turn_units(m)

        @pl.when(hf == 0)
        def _():
            fetch_u(t + FWIN - 1)
            await_u(t + FWIN - 1)

        project(t, hf)
        return 0

    lax.fori_loop(0, -first_m, warm, 0)
    fetch_u(jnp.int32(FWIN - 1))

    def step(t, _):
        nxt = lax.rem(t + 1, 2)
        await_u(t + FWIN - 1)
        turn_units(2 * t)

        @pl.when(t == 0)
        def _():
            for c in wr_copies(0):
                c.wait()

        @pl.when(t >= 1)
        def _():
            release_u(t - 1)
            c_copy(nxt, t).wait()
            h_copy(nxt, t).wait()
            g_copy(t, 0).wait()

        @pl.when(jnp.logical_and(t >= 2, sends))
        def _():
            send(nxt, t).wait_send()

        project(t, 0)
        recur(t, 0)

        g_copy(t, 0).start()
        turn_units(2 * t + 1)
        fetch_u(t + FWIN)

        @pl.when(t == 0)
        def _():
            for c in wr_copies(1):
                c.wait()

        @pl.when(t >= 1)
        def _():
            g_copy(t, 1).wait()

        project(t, 1)
        recur(t, 1)

        g_copy(t, 1).start()
        c_copy(nxt, t + 1).start()
        h_copy(nxt, t + 1).start()

        @pl.when(sends)
        def _():
            @pl.when(t >= RING)
            def _():
                pl.semaphore_wait(credit, 1)

            send(nxt, t).start()

        return 0

    lax.fori_loop(0, steps, step, 0)
    release_u(jnp.int32(steps - 1))
    for hf in range(2):
        g_copy(0, hf).wait()
        c_copy(hf, 0).wait()
        h_copy(hf, 0).wait()

        @pl.when(sends)
        def _():
            send(hf, 0).wait_send()


def run_forward(n_stages, seq, w_in, w_rec, bias, h_start, c_start, spans):
    n_groups, steps, _, hidden = seq.shape
    rows = n_groups * GROUP
    bw = hidden // NB
    any_spec = pl.BlockSpec(memory_space=pl.ANY)
    vmem_spec = pl.BlockSpec(memory_space=pltpu.VMEM)
    dma = pltpu.SemaphoreType.DMA
    return pl.pallas_call(
        functools.partial(forward_kernel, n_stages, steps, rows, hidden),
        out_shape=(jax.ShapeDtypeStruct((n_groups, steps, GROUP, hidden), bf16),
                   jax.ShapeDtypeStruct((n_groups, steps + 1, GROUP, hidden), bf16),
                   jax.ShapeDtypeStruct((steps, NB, rows, 4 * bw), f32),
                   jax.ShapeDtypeStruct((steps + 1, rows, hidden), f32)),
        in_specs=[any_spec, any_spec, any_spec, vmem_spec, any_spec, any_spec, pl.BlockSpec(memory_space=pltpu.SMEM)],
        out_specs=(any_spec,) * 4,
        input_output_aliases={0: 0},
        scratch_shapes=[
            pltpu.VMEM((NB, hidden, 4 * bw), bf16),
            pltpu.VMEM((FUNITS, hidden, hidden // 2), bf16),
            pltpu.VMEM((RING, n_groups, GROUP, hidden), bf16),
            pltpu.VMEM((8, FWIN, rows, hidden // 2), f32),
            pltpu.VMEM((NB, rows, 4 * bw), f32),
            pltpu.VMEM((2, rows, hidden), f32),
            pltpu.VMEM((2, n_groups, GROUP, hidden), bf16),
            pltpu.VMEM((rows, bw), jnp.int32),
            dma((NB, 4)), dma((FUNITS,)), dma((1,)), dma((2,)), dma((2,)), dma((2,)), dma((2,)), dma((steps,)),
            dma((RING,)), pltpu.SemaphoreType.REGULAR,
        ],
        compiler_params=pltpu.CompilerParams(collective_id=0, has_side_effects=True, vmem_limit_bytes=VMEM_LIMIT),
        name="lstm_forward",
    )(seq, w_in, w_rec, bias, h_start, c_start, spans)


def backward_kernel(n_stages, steps, rows, hidden,
                    hseq, tseq, gates, cseq, win_t, wrec_t, spans,
                    dz_out, dh_out, dc_out, db_out, loss_out,
                    wt, wi, gin, cring, dbuf, ybuf, dzr, dh, dc, dbacc, lossacc, duacc, dust, lsend, lrecv, lens, scale,
                    wt_sem, wi_sem, g_sem, c_sem, d_sem, y_sem, dz_sem, out_sem, send_sem, recv_sem, lsend_sem, lrecv_sem, credit):
    bw = hidden // NB
    n_groups = rows // GROUP
    half = NB // 2
    hw = half * bw
    part = hidden // WIN
    ring = WIN
    pad = WIN - 1
    stage = lax.axis_index("stage")
    top = stage == n_stages - 1
    sends = stage > 0
    last = steps - 1
    halves = jnp.where(sends, 2 * (steps + pad), 2 * steps)
    entry_signal(stage, n_stages)

    def wt_copies(hf):
        return [copy_of(wrec_t.at[j], wt.at[j], wt_sem.at[j]) for j in range(hf * half, (hf + 1) * half)]

    def part_of(t):
        return lax.rem(t + WIN, WIN)

    def wi_copy(m, i):
        n = 2 * m + i
        t, hf = last - m // 2, lax.rem(m, 2)
        return copy_of(win_t.at[hf, part_of(t), pl.ds(i * hidden, hidden)], wi.at[lax.rem(n, UNITS)], wi_sem.at[lax.rem(n, UNITS)])

    def turn_units(m):
        for i in range(2):
            wi_copy(m, i).wait()

        @pl.when(m + 1 < halves)
        def _():
            wi_copy(m + 1, 1).start()

        @pl.when(m + 2 < halves)
        def _():
            wi_copy(m + 2, 0).start()

    def g_copy(t, hf):
        return copy_of(gates.at[t, pl.ds(hf * half, half)], gin.at[pl.ds(hf * half, half)], g_sem.at[hf])

    def c_copy(i):
        slot = lax.rem(i, 3)
        return copy_of(cseq.at[i], cring.at[slot], c_sem.at[slot])

    def d_slot(t):
        return lax.rem(t + RING, RING)

    def own_copies(t):
        return [copy_of(hseq.at[:, t + 1, :, pl.ds(q * part, part)], dbuf.at[d_slot(t), q], d_sem.at[q])
                for q in range(WIN)]

    def y_copy(t):
        return copy_of(tseq.at[:, t], ybuf.at[lax.rem(t, 2)], y_sem.at[0])

    def dz_copy(t):
        slot = lax.rem(t, ring)
        return copy_of(dzr.at[slot], dz_out.at[:, :, t], dz_sem.at[slot])

    def send(t, k):
        return pltpu.make_async_remote_copy(
            src_ref=dust.at[k], dst_ref=dbuf.at[d_slot(t + k), part_of(t)],
            send_sem=send_sem.at[k], recv_sem=recv_sem.at[k, t + pad],
            device_id={"stage": lax.rem(stage + n_stages - 1, n_stages)}, device_id_type=MESH)

    def each_send(t, act):
        @pl.when(t >= 0)
        def _():
            act(send(t, 0))

        @pl.when(t < last)
        def _():
            act(send(t, 1))

    def fetch_d(t):
        @pl.when(top)
        def _():
            for c in own_copies(t):
                c.start()
            y_copy(t).start()

    def await_d(t):
        @pl.when(top)
        def _():
            for c in own_copies(t):
                c.wait()
            y_copy(t).wait()

        @pl.when(jnp.logical_not(top))
        def _():
            send(t, 0).wait_recv()
            send(t - 1, 1).wait_recv()

    def release_d(t):
        @pl.when(jnp.logical_and(jnp.logical_not(top), t >= RING))
        def _():
            pl.semaphore_signal(credit, inc=1, device_id={"stage": lax.rem(stage + 1, n_stages)}, device_id_type=MESH)

    def input_grad(t, hf):
        d = jnp.concatenate([dzr[lax.rem(t + i + ring, ring), hf].reshape(rows, 2 * hidden) for i in range(WIN)], axis=0)
        n = 2 * (2 * (last - t) + hf)
        du = jnp.dot(d[:, :hidden], wi[lax.rem(n, UNITS)], preferred_element_type=f32)
        du += jnp.dot(d[:, hidden:], wi[lax.rem(n + 1, UNITS)], preferred_element_type=f32)
        if hf == 0:
            duacc[...] = du
        else:
            du = (du + duacc[...]).astype(bf16)
            for i in range(WIN):
                dust[i] = du[i * rows:(i + 1) * rows].reshape(n_groups, GROUP, part)

    def flat(x):
        return x.reshape(rows, x.shape[-1])

    def fold(x):
        return x.reshape(rows // 8, 8, x.shape[-1]).sum(axis=0)

    def recur(t, hf):
        cur, nxt = lax.rem(t, 2), lax.rem(t + 1, 2)
        slot = d_slot(t)
        live = lens[...] > t
        sc = scale[0:1, :]
        total = None
        for j in range(hf * half, (hf + 1) * half):
            cols = slice(j * bw, (j + 1) * bw)
            q, off = j * bw // part, j * bw % part
            gi, gf = gin[j, :, :bw], gin[j, :, bw:2 * bw]
            gg, go = gin[j, :, 2 * bw:3 * bw], gin[j, :, 3 * bw:]
            err = jnp.where(live, flat(dbuf[slot, q, :, :, off:off + bw]).astype(f32) - flat(ybuf[cur, :, :, cols]).astype(f32), 0.0)
            lossacc[:, cols] += fold(err * err)
            d_total = dh[cur, :, cols] + err * sc
            c_prev = cring[lax.rem(t, 3), :, cols]
            tanh_c = jnp.tanh(cring[lax.rem(t + 1, 3), :, cols])
            dc_old = dc[:, cols]
            d_c = dc_old + d_total * go * (1.0 - tanh_c * tanh_c)
            gates_d = (d_c * gg * gi * (1.0 - gi),
                     d_c * c_prev * gf * (1.0 - gf),
                     d_c * gi * (1.0 - gg * gg),
                     d_total * tanh_c * go * (1.0 - go))
            low = []
            for g in range(4):
                dz = jnp.where(live, gates_d[g], 0.0)
                dbacc[j, :, g * bw:(g + 1) * bw] += fold(dz)
                dz = dz.astype(bf16)
                at = g * hw + (j - hf * half) * bw
                dzr[lax.rem(t, ring), hf, :, :, at:at + bw] = dz.reshape(n_groups, GROUP, bw)
                low.append(dz)
            dc[:, cols] = jnp.where(live, d_c * gf, dc_old)
            keep = jnp.where(live, 0.0, d_total)
            if hf == 0:
                dh[nxt, :, cols] = keep
            else:
                dh[nxt, :, cols] += keep
            low = jnp.concatenate(low, axis=1)
            low = jnp.concatenate([low, low], axis=0)
            r = jnp.dot(low, wt[j], preferred_element_type=f32)
            total = r if total is None else total + r
        total = jnp.maximum(total[:rows], total[rows:])
        if hf == 0:
            dh[nxt, :, :hw] += total[:, :hw]
            dh[nxt, :, hw:] = total[:, hw:]
        else:
            dh[nxt] += total

    for c in wt_copies(0):
        c.start()
    g_copy(last, 0).start()
    c_copy(last + 1).start()
    c_copy(last).start()
    wi_copy(0, 0).start()
    wi_copy(0, 1).start()
    for c in wt_copies(1):
        c.start()
    wi_copy(1, 0).start()
    fill_lens(spans, lens)
    entry_wait(stage, n_stages)
    n_active = spans[0]
    for r in range(1, rows):
        n_active += spans[r]
    share = 1.0 / jnp.full(scale.shape, n_active.astype(f32))
    scale[...] = jnp.where(top, share, 1.0)
    dh[...] = jnp.zeros_like(dh)
    dc[...] = jnp.zeros_like(dc)
    dbacc[...] = jnp.zeros_like(dbacc)
    lossacc[...] = jnp.zeros_like(lossacc)
    ybuf[...] = jnp.zeros_like(ybuf)
    for i in range(ring):
        dzr[i] = jnp.zeros_like(dzr[i])

    fetch_d(last)
    c_copy(last + 1).wait()

    def step(v, _):
        t = last - v
        await_d(t)
        g_copy(t, 0).wait()
        c_copy(t).wait()

        @pl.when(v == 0)
        def _():
            for c in wt_copies(0):
                c.wait()

        @pl.when(v >= ring)
        def _():
            dz_copy(t + ring).wait()

        g_copy(t, 1).start()
        turn_units(2 * v)

        @pl.when(t >= 1)
        def _():
            c_copy(t - 1).start()

        recur(t, 0)
        input_grad(t, 0)

        g_copy(t, 1).wait()

        @pl.when(v == 0)
        def _():
            for c in wt_copies(1):
                c.wait()

        @pl.when(jnp.logical_and(v >= 1, sends))
        def _():
            each_send(t + 1, lambda c: c.wait_send())

        turn_units(2 * v + 1)

        @pl.when(t >= 1)
        def _():
            g_copy(t - 1, 0).start()
            fetch_d(t - 1)

        recur(t, 1)
        input_grad(t, 1)
        dz_copy(t).start()
        release_d(t)

        @pl.when(sends)
        def _():
            @pl.when(t <= last - RING)
            def _():
                pl.semaphore_wait(credit, 1)

            each_send(t, lambda c: c.start())

        return 0

    lax.fori_loop(0, steps, step, 0)

    for i in range(ring):
        dz_copy(i).wait()
    outs = [copy_of(dh.at[1], dh_out, out_sem.at[0]), copy_of(dc, dc_out, out_sem.at[1]),
            copy_of(dbacc, db_out, out_sem.at[2])]
    for c in outs:
        c.start()

    def tell():
        return pltpu.make_async_remote_copy(
            src_ref=lsend, dst_ref=lrecv, send_sem=lsend_sem.at[0], recv_sem=lrecv_sem.at[0],
            device_id={"stage": lax.rem(stage + n_stages - 1, n_stages)}, device_id_type=MESH)

    @pl.when(top)
    def _():
        lsend[...] = sum(lossacc[:, i * 128:(i + 1) * 128] for i in range(hidden // 128))

    @pl.when(sends)
    def _():
        def drain(v, _):
            t = -1 - v
            turn_units(2 * (last - t))
            input_grad(t, 0)
            turn_units(2 * (last - t) + 1)
            each_send(t + 1, lambda c: c.wait_send())
            input_grad(t, 1)
            each_send(t, lambda c: c.start())
            return 0

        lax.fori_loop(0, pad, drain, 0)
        each_send(jnp.int32(-pad), lambda c: c.wait_send())

    @pl.when(jnp.logical_not(top))
    def _():
        tell().wait_recv()
        lsend[...] = lrecv[...]

    for c in outs:
        c.wait()
    loss_copy = copy_of(lsend, loss_out, out_sem.at[3])
    loss_copy.start()
    loss_copy.wait()

    @pl.when(sends)
    def _():
        tell().start()
        tell().wait_send()


def run_backward(n_stages, hseq, tseq, gates, cseq, win_t, wrec_t, spans):
    n_groups, steps, _, hidden = tseq.shape
    rows = n_groups * GROUP
    bw = hidden // NB
    part = hidden // WIN
    any_spec = pl.BlockSpec(memory_space=pl.ANY)
    dma = pltpu.SemaphoreType.DMA
    return pl.pallas_call(
        functools.partial(backward_kernel, n_stages, steps, rows, hidden),
        out_shape=(jax.ShapeDtypeStruct((2, n_groups, steps, GROUP, 2 * hidden), bf16),
                   jax.ShapeDtypeStruct((rows, hidden), f32),
                   jax.ShapeDtypeStruct((rows, hidden), f32),
                   jax.ShapeDtypeStruct((NB, 8, 4 * bw), f32),
                   jax.ShapeDtypeStruct((8, 128), f32)),
        in_specs=[any_spec] * 6 + [pl.BlockSpec(memory_space=pltpu.SMEM)],
        out_specs=(any_spec,) * 5,
        scratch_shapes=[
            pltpu.VMEM((NB, 4 * bw, hidden), bf16),
            pltpu.VMEM((UNITS, hidden, part), bf16),
            pltpu.VMEM((NB, rows, 4 * bw), f32),
            pltpu.VMEM((3, rows, hidden), f32),
            pltpu.VMEM((RING, WIN, n_groups, GROUP, part), bf16),
            pltpu.VMEM((2, n_groups, GROUP, hidden), bf16),
            pltpu.VMEM((WIN, 2, n_groups, GROUP, 2 * hidden), bf16),
            pltpu.VMEM((2, rows, hidden), f32),
            pltpu.VMEM((rows, hidden), f32),
            pltpu.VMEM((NB, 8, 4 * bw), f32),
            pltpu.VMEM((8, hidden), f32),
            pltpu.VMEM((WIN * rows, part), f32),
            pltpu.VMEM((WIN, n_groups, GROUP, part), bf16),
            pltpu.VMEM((8, 128), f32),
            pltpu.VMEM((8, 128), f32),
            pltpu.VMEM((rows, bw), jnp.int32),
            pltpu.VMEM((8, bw), f32),
            dma((NB,)), dma((UNITS,)), dma((2,)), dma((3,)), dma((WIN,)), dma((1,)), dma((WIN,)), dma((4,)), dma((WIN,)),
            dma((WIN, steps + WIN - 1)), dma((1,)), dma((1,)), pltpu.SemaphoreType.REGULAR,
        ],
        compiler_params=pltpu.CompilerParams(collective_id=1, has_side_effects=True, vmem_limit_bytes=VMEM_LIMIT),
        name="lstm_backward",
    )(hseq, tseq, gates, cseq, win_t, wrec_t, spans)


def grads_kernel(steps, hidden, spans, useq, hseq, dz, dh, dc, db, sq,
                 g_in, g_rec, g_bias, dh_out, dc_out, loss_out,
                 xs, dzb, acc, state, x_sem, z_sem, o_sem, s_sem):
    n_groups = useq.shape[0]
    tile = dzb.shape[-1]
    n_tiles = 2 * dz.shape[-1] // tile
    per = hidden // 2 // tile
    bw = hidden // NB
    seen = [spans[i * GROUP] for i in range(n_groups)]
    first = [0]
    for i in range(n_groups):
        first.append(first[-1] + seen[i])
    total = first[-1]
    sizes = []
    size = 1
    while size <= steps:
        sizes.insert(0, size)
        size *= 2

    def pieces(make, act):
        for i in range(n_groups):
            for size in sizes:
                done = seen[i] // (2 * size) * (2 * size)

                @pl.when(seen[i] // size % 2 == 1)
                def _(i=i, size=size, done=done):
                    act(make(i, pl.ds(done, size), pl.ds(first[i] + done, size)))

    def load_x(w, act):
        src = useq if w == 0 else hseq
        pieces(lambda i, at, to: copy_of(src.at[i, at], xs.at[w, to], x_sem.at[w]), act)

    def load_z(n, slot, act):
        gate, hf = n // (2 * per), lax.rem(n, 2 * per) // per
        cols = pl.ds(pl.multiple_of((gate * per + lax.rem(n, per)) * tile, tile), tile)
        pieces(lambda i, at, to: copy_of(dz.at[hf, i, at, :, cols], dzb.at[slot, to], z_sem.at[slot]), act)

    def start(c):
        c.start()

    def wait(c):
        c.wait()

    def store(w, n, act):
        cols = pl.ds(pl.multiple_of(n * tile, tile), tile)

        @pl.when(w == 0)
        def _():
            act(copy_of(acc.at[0], g_in.at[0, :, cols], o_sem.at[0]))

        @pl.when(w == 1)
        def _():
            act(copy_of(acc.at[1], g_rec.at[0, :, cols], o_sem.at[1]))

    for slot in range(2):
        xs[slot, pl.ds(total, GROUP)] = jnp.zeros((GROUP, GROUP, hidden), bf16)
        dzb[slot, pl.ds(total, GROUP)] = jnp.zeros((GROUP, GROUP, tile), bf16)
    load_z(0, 0, start)
    load_x(0, start)
    load_x(1, start)
    states = [(copy_of(x, state.at[i], s_sem.at[i]), copy_of(state.at[i], y.at[0], s_sem.at[i]))
              for i, (x, y) in enumerate(((dh, dh_out), (dc, dc_out)))]
    for c, _ in states:
        c.start()
    for j in range(NB):
        for g in range(4):
            g_bias[0:1, g * hidden + j * bw:g * hidden + (j + 1) * bw] = jnp.sum(
                db[j, :, g * bw:(g + 1) * bw], axis=0, keepdims=True)
    n_active = spans[0]
    for r in range(1, n_groups * GROUP):
        n_active += spans[r]
    loss_out[...] = jnp.full((1, 1), jnp.sum(sq[...]) / (2.0 * n_active.astype(f32)))

    def product(w, slot, at, depth, begin):
        rhs = dzb[slot, pl.ds(at, depth)].reshape(depth * GROUP, tile)
        mc = min(512, hidden)
        for m in range(hidden // mc):
            lhs = xs[w, pl.ds(at, depth), :, m * mc:(m + 1) * mc].reshape(depth * GROUP, mc)
            r = lax.dot_general(lhs, rhs, (((0,), (0,)), ((), ())), preferred_element_type=f32)
            acc[w, m * mc:(m + 1) * mc] = r if begin else acc[w, m * mc:(m + 1) * mc] + r

    units = (total + 15) // 16

    def one_tile(v, _):
        n, w = v // 2, lax.rem(v, 2)
        slot = lax.rem(n, 2)

        @pl.when(w == 0)
        def _():
            @pl.when(n + 1 < n_tiles)
            def _():
                load_z(n + 1, 1 - slot, start)

            load_z(n, slot, wait)

        @pl.when(v == 0)
        def _():
            load_x(0, wait)

        @pl.when(v == 1)
        def _():
            load_x(1, wait)

        @pl.when(n >= 1)
        def _():
            store(w, n, wait)

        product(w, slot, 0, 128, True)

        def more(b, _):
            product(w, slot, 128 + b * 64, 64, False)
            return 0

        rest = jnp.maximum(units - 8, 0)
        lax.fori_loop(0, rest // 4, more, 0)

        @pl.when(rest // 2 % 2 == 1)
        def _():
            product(w, slot, 128 + rest // 4 * 64, 32, False)

        @pl.when(rest % 2 == 1)
        def _():
            product(w, slot, 128 + rest // 2 * 32, 16, False)

        store(w, n, start)
        return 0

    lax.fori_loop(0, 2 * n_tiles, one_tile, 0)
    for c, d in states:
        c.wait()
        d.start()
    store(0, 0, wait)
    store(1, 0, wait)
    for _, d in states:
        d.wait()


def run_grads(useq, hseq, dz, dh, dc, db, sq, spans):
    n_groups, steps, _, hidden = useq.shape
    rows = n_groups * GROUP
    any_spec = pl.BlockSpec(memory_space=pl.ANY)
    vmem_spec = pl.BlockSpec(memory_space=pltpu.VMEM)
    blocks = n_groups * steps + GROUP
    tile = 512
    dma = pltpu.SemaphoreType.DMA
    out = jax.ShapeDtypeStruct((1, hidden, 4 * hidden), f32)
    state = jax.ShapeDtypeStruct((1, rows, hidden), f32)
    return pl.pallas_call(
        functools.partial(grads_kernel, steps, hidden),
        out_shape=(out, out, jax.ShapeDtypeStruct((1, 4 * hidden), f32), state, state, jax.ShapeDtypeStruct((1, 1), f32)),
        in_specs=[pl.BlockSpec(memory_space=pltpu.SMEM)] + [any_spec] * 5 + [vmem_spec] * 2,
        out_specs=(any_spec, any_spec, vmem_spec, any_spec, any_spec, vmem_spec),
        scratch_shapes=[
            pltpu.VMEM((2, blocks, GROUP, hidden), bf16),
            pltpu.VMEM((2, blocks, GROUP, tile), bf16),
            pltpu.VMEM((2, hidden, tile), f32),
            pltpu.VMEM((2, rows, hidden), f32),
            dma((2,)), dma((2,)), dma((2,)), dma((2,)),
        ],
        compiler_params=pltpu.CompilerParams(vmem_limit_bytes=VMEM_LIMIT),
        name="lstm_weight_grads",
    )(spans, useq, hseq, dz, dh, dc, db, sq)


def solution(mesh):
    n_stages = mesh.shape["stage"]

    def local_program(inputs, targets, lengths, w_in, w_rec, gate_bias, h_init, c_init):
        useq, tseq, win_t, wrec_t = run_prepare(n_stages, inputs, targets, w_in, w_rec)
        useq, hseq, gates, cseq = run_forward(n_stages, useq, w_in, w_rec, gate_bias, h_init, c_init, lengths)
        win_t, wrec_t = run_late_turn(n_stages, w_in, w_rec, cseq, win_t, wrec_t)
        dz, dh0, dc0, db, sq = run_backward(n_stages, hseq, tseq, gates, cseq, win_t, wrec_t, lengths)
        grad_in, grad_rec, grad_bias, dh0, dc0, loss = run_grads(useq, hseq, dz, dh0, dc0, db, sq, lengths)
        return loss.reshape(1), grad_in, grad_rec, grad_bias, dh0, dc0

    row_spec = P("data", None, None)
    layer_spec = P("stage", None, None)
    state_spec = P("stage", "data", None)
    grad_spec = P(("data", "stage"), None, None)
    return jax.shard_map(local_program, mesh=mesh,
                         in_specs=(row_spec, row_spec, P("data"), layer_spec, layer_spec, P("stage", None), state_spec, state_spec),
                         out_specs=(P("data"), grad_spec, grad_spec, P(("data", "stage"), None), state_spec, state_spec),
                         check_vma=False)
```

```python
import functools

import jax
import jax.numpy as jnp
from jax import lax
from jax.experimental import pallas as pl
from jax.experimental.pallas import tpu as pltpu
from jax.sharding import PartitionSpec as P

MESH = pl.DeviceIdType.MESH
NB = 8
FWIN = 2
WIN = 2
FUNITS = 5
UNITS = 5
RING = 4
GROUP = 16
VMEM_LIMIT = 67043328
f32 = jnp.float32
bf16 = jnp.bfloat16


def sigmoid(x):
    return 0.5 * jnp.tanh(0.5 * x) + 0.5


def copy_of(src, dst, sem):
    return pltpu.make_async_copy(src, dst, sem)


def entry_signal(stage, n_stages):
    barrier = pltpu.get_barrier_semaphore()

    @pl.when(stage > 0)
    def _():
        pl.semaphore_signal(barrier, inc=1, device_id={"stage": lax.rem(stage + n_stages - 1, n_stages)}, device_id_type=MESH)

    @pl.when(stage < n_stages - 1)
    def _():
        pl.semaphore_signal(barrier, inc=1, device_id={"stage": lax.rem(stage + 1, n_stages)}, device_id_type=MESH)


def entry_wait(stage, n_stages):
    peers = jnp.minimum(stage, 1) + jnp.minimum(n_stages - 1 - stage, 1)
    pl.semaphore_wait(pltpu.get_barrier_semaphore(), peers)


def fill_lens(spans, lens):
    for r in range(lens.shape[0]):
        lens[r:r + 1, :] = jnp.full((1, lens.shape[1]), spans[r], jnp.int32)


def turn_weights(w_in, w_rec, win_t, wrec_t, src, dst, in_sem, out_sem):
    hidden = w_rec.shape[1]
    bw = hidden // NB
    per_half = NB // 2
    n_parts = win_t.shape[1]
    part = hidden // n_parts
    n_slots = src.shape[0]

    def load(i):
        slot = lax.rem(i, n_slots)
        j, g = lax.rem(i, 4 * NB) // 4, lax.rem(i, 4)
        cols = pl.ds(pl.multiple_of(g * hidden + j * bw, 128), bw)
        return (copy_of(w_rec.at[0, :, cols], src.at[slot], in_sem.at[slot]),
                copy_of(w_in.at[0, :, cols], src.at[slot], in_sem.at[slot]))

    def save(i):
        slot = lax.rem(i, n_slots)
        j, g = lax.rem(i, 4 * NB) // 4, lax.rem(i, 4)
        rec = copy_of(dst.at[slot], wrec_t.at[j, pl.ds(pl.multiple_of(g * bw, 8), bw)], out_sem.at[slot, 0])
        at = pl.multiple_of(g * per_half * bw + lax.rem(j, per_half) * bw, 8)
        ins = [copy_of(dst.at[slot, :, pl.ds(q * part, part)], win_t.at[j // per_half, q, pl.ds(at, bw)], out_sem.at[slot, q])
               for q in range(n_parts)]
        return [rec], ins

    units = 8 * NB

    def both(i, rec_do, in_do):
        @pl.when(i < 4 * NB)
        def _():
            rec_do()

        @pl.when(i >= 4 * NB)
        def _():
            in_do()

    def start_load(i):
        both(i, lambda: load(i)[0].start(), lambda: load(i)[1].start())

    def each_save(i, act):
        both(i, lambda: [act(c) for c in save(i)[0]], lambda: [act(c) for c in save(i)[1]])

    for i in range(n_slots):
        start_load(i)

    def unit(i, _):
        slot = lax.rem(i, n_slots)
        load(i)[0].wait()

        @pl.when(i >= n_slots)
        def _():
            each_save(i - n_slots, lambda c: c.wait())

        dst[slot] = src[slot].T
        each_save(i, lambda c: c.start())

        @pl.when(i + n_slots < units)
        def _():
            start_load(i + n_slots)

        return 0

    lax.fori_loop(0, units, unit, 0)
    for i in range(units - n_slots, units):
        each_save(i, lambda c: c.wait())


def early_turn(n_stages, stage):
    return stage >= n_stages // 2


def prepare_kernel(n_stages, inputs, targets, w_in, w_rec, useq, tseq, win_t, wrec_t,
                   src, dst, wsrc, wdst, in_sem, out_sem, win_sem, wout_sem):
    rows, steps, _ = inputs.shape
    stage = lax.axis_index("stage")
    n_slots = src.shape[0]
    n_cols = steps // GROUP
    units = rows // GROUP * n_cols

    def turn(x, y):
        def load(i):
            slot = lax.rem(i, n_slots)
            return copy_of(x.at[pl.ds(pl.multiple_of(i // n_cols * GROUP, GROUP), GROUP),
                                pl.ds(pl.multiple_of(lax.rem(i, n_cols) * GROUP, GROUP), GROUP)], src.at[slot], in_sem.at[slot])

        def save(i):
            slot = lax.rem(i, n_slots)
            return copy_of(dst.at[slot], y.at[i // n_cols, pl.ds(lax.rem(i, n_cols) * GROUP, GROUP)], out_sem.at[slot])

        for i in range(min(n_slots, units)):
            load(i).start()

        def unit(i, _):
            slot = lax.rem(i, n_slots)
            load(i).wait()

            @pl.when(i >= n_slots)
            def _():
                save(i).wait()

            dst[slot] = jnp.swapaxes(src[slot], 0, 1)
            save(i).start()

            @pl.when(i + n_slots < units)
            def _():
                load(i + n_slots).start()

            return 0

        lax.fori_loop(0, units, unit, 0)
        for i in range(max(0, units - n_slots), units):
            save(i).wait()

    @pl.when(stage == 0)
    def _():
        turn(inputs, useq)

    @pl.when(stage == n_stages - 1)
    def _():
        turn(targets, tseq)

    @pl.when(early_turn(n_stages, stage))
    def _():
        turn_weights(w_in, w_rec, win_t, wrec_t, wsrc, wdst, win_sem, wout_sem)


def weight_scratch(hidden):
    dma = pltpu.SemaphoreType.DMA
    slots = 4
    return ([pltpu.VMEM((slots, hidden, hidden // NB), bf16), pltpu.VMEM((slots, hidden // NB, hidden), bf16)],
            [dma((slots,)), dma((slots, WIN))])


def run_prepare(n_stages, inputs, targets, w_in, w_rec):
    rows, steps, hidden = inputs.shape
    any_spec = pl.BlockSpec(memory_space=pl.ANY)
    dma = pltpu.SemaphoreType.DMA
    seq = jax.ShapeDtypeStruct((rows // GROUP, steps, GROUP, hidden), bf16)
    buffers, sems = weight_scratch(hidden)
    return pl.pallas_call(
        functools.partial(prepare_kernel, n_stages),
        out_shape=(seq, seq, jax.ShapeDtypeStruct((2, WIN, 2 * hidden, hidden // WIN), bf16),
                   jax.ShapeDtypeStruct((NB, hidden // 2, hidden), bf16)),
        in_specs=[any_spec] * 4, out_specs=(any_spec,) * 4,
        scratch_shapes=[pltpu.VMEM((4, GROUP, GROUP, hidden), bf16), pltpu.VMEM((4, GROUP, GROUP, hidden), bf16), *buffers,
                        dma((4,)), dma((4,)), *sems],
        compiler_params=pltpu.CompilerParams(vmem_limit_bytes=VMEM_LIMIT),
        name="lstm_prepare",
    )(inputs, targets, w_in, w_rec)


def late_turn_kernel(n_stages, w_in, w_rec, after, win_old, wrec_old, win_t, wrec_t, wsrc, wdst, win_sem, wout_sem):
    del after, win_old, wrec_old

    @pl.when(jnp.logical_not(early_turn(n_stages, lax.axis_index("stage"))))
    def _():
        turn_weights(w_in, w_rec, win_t, wrec_t, wsrc, wdst, win_sem, wout_sem)


def run_late_turn(n_stages, w_in, w_rec, after, win_t, wrec_t):
    any_spec = pl.BlockSpec(memory_space=pl.ANY)
    buffers, sems = weight_scratch(w_rec.shape[1])
    return pl.pallas_call(
        functools.partial(late_turn_kernel, n_stages),
        out_shape=(jax.ShapeDtypeStruct(win_t.shape, bf16), jax.ShapeDtypeStruct(wrec_t.shape, bf16)),
        in_specs=[any_spec] * 5, out_specs=(any_spec,) * 2, input_output_aliases={3: 0, 4: 1},
        scratch_shapes=[*buffers, *sems],
        compiler_params=pltpu.CompilerParams(vmem_limit_bytes=VMEM_LIMIT),
        name="lstm_late_turn",
    )(w_in, w_rec, after, win_t, wrec_t)


def forward_kernel(n_stages, steps, rows, hidden,
                   seq_ref, w_in, w_rec, bias, h_start, c_start, spans,
                   useq, hseq, gates, cseq,
                   wr, wi, uring, zin, gst, cst, hst, lens,
                   wr_sem, wi_sem, u_sem, g_sem, c_sem, h_sem, send_sem, recv_sem, keep_sem, credit):
    bw = hidden // NB
    half = NB // 2
    hw = half * bw
    per = 4 // FWIN
    stage = lax.axis_index("stage")
    first = stage == 0
    sends = stage < n_stages - 1
    entry_signal(stage, n_stages)

    def wr_copies(hf):
        return [copy_of(w_rec.at[0, :, pl.ds(g * hidden + j * bw, bw)], wr.at[j, :, pl.ds(g * bw, bw)], wr_sem.at[j, g])
                for j in range(hf * half, (hf + 1) * half) for g in range(4)]

    first_m = 2 - 2 * FWIN
    last_m = 2 * steps - 1

    def gate_of(t, i):
        return lax.rem(t + FWIN, FWIN) * per + i

    def slot_of(n):
        return lax.rem(n + 4 * FUNITS, FUNITS)

    def wi_copy(n):
        m = (n + 2 * FWIN * per) // per - 2 * FWIN
        t, hf = (m + 2 * FWIN) // 2 - FWIN, lax.rem(m + 2 * FWIN, 2)
        first_col = gate_of(t, n - per * m) * hidden + hf * hw
        return copy_of(w_in.at[0, :, pl.ds(pl.multiple_of(first_col, 128), hw)], wi.at[slot_of(n)], wi_sem.at[slot_of(n)])

    def turn_units(m):
        for i in range(per):
            wi_copy(per * m + i).wait()
        for k in range(per):
            n = per * (m - 1) + FUNITS + k

            @pl.when(n < per * (last_m + 1))
            def _(n=n):
                wi_copy(n).start()

    def u_slot(t):
        return lax.rem(t + 2 * RING, RING)

    def u_copy(t):
        return copy_of(useq.at[:, t], uring.at[u_slot(t)], u_sem.at[0])

    def u_keep(t):
        return copy_of(uring.at[u_slot(t)], useq.at[:, t], keep_sem.at[u_slot(t)])

    def g_copy(t, hf):
        return copy_of(gst.at[pl.ds(hf * half, half)], gates.at[t, pl.ds(hf * half, half)], g_sem.at[hf])

    def c_copy(slot, t):
        return copy_of(cst.at[slot], cseq.at[t], c_sem.at[slot])

    def h_copy(slot, t):
        return copy_of(hst.at[slot], hseq.at[:, t], h_sem.at[slot])

    def send(slot, t):
        return pltpu.make_async_remote_copy(
            src_ref=hst.at[slot], dst_ref=uring.at[u_slot(t)], send_sem=send_sem.at[slot], recv_sem=recv_sem.at[t],
            device_id={"stage": lax.rem(stage + 1, n_stages)}, device_id_type=MESH)

    def fetch_u(t):
        @pl.when(jnp.logical_and(first, t < steps))
        def _():
            u_copy(t).start()

    def await_u(t):
        @pl.when(jnp.logical_and(first, t < steps))
        def _():
            u_copy(t).wait()

        @pl.when(jnp.logical_and(jnp.logical_not(first), t < steps))
        def _():
            send(0, t).wait_recv()
            u_keep(t).start()

    def release_u(t):
        @pl.when(jnp.logical_not(first))
        def _():
            u_keep(t).wait()

            @pl.when(t < steps - RING)
            def _():
                pl.semaphore_signal(credit, inc=1, device_id={"stage": lax.rem(stage + n_stages - 1, n_stages)},
                                    device_id_type=MESH)

    def project(t, hf):
        u = jnp.concatenate([uring[u_slot(jnp.maximum(t + i, 0))].reshape(rows, hidden) for i in range(FWIN)], axis=0)
        for i in range(per):
            g = gate_of(t, i)
            z = jnp.dot(u, wi[slot_of(per * (2 * t + hf) + i)], preferred_element_type=f32)
            z += bias[0:1, pl.ds(pl.multiple_of(g * hidden + hf * hw, 128), hw)]
            for k in range(FWIN):
                zin[4 * hf + g, lax.rem(t + k + 2 * FWIN, FWIN)] = z[k * rows:(k + 1) * rows]

    def recur(t, hf):
        cur, nxt = lax.rem(t, 2), lax.rem(t + 1, 2)
        live = lens[...] > t
        h = hst[cur].reshape(rows, hidden)
        h_twice = jnp.concatenate([h, h], axis=0)
        for j in range(hf * half, (hf + 1) * half):
            cols = slice(j * bw, (j + 1) * bw)
            z = jnp.dot(h_twice, wr[j], preferred_element_type=f32)
            z = jnp.maximum(z[:rows], z[rows:])
            at = (j - hf * half) * bw
            zi, zf, zg, zo = (z[:, g * bw:(g + 1) * bw] + zin[4 * hf + g, lax.rem(t, FWIN), :, at:at + bw] for g in range(4))
            gi = sigmoid(zi)
            gf = sigmoid(zf)
            gg = jnp.tanh(zg)
            go = sigmoid(zo)
            c_prev = cst[cur, :, cols]
            c_new = gf * c_prev + gi * gg
            h_new = go * jnp.tanh(c_new)
            cst[nxt, :, cols] = jnp.where(live, c_new, c_prev)
            hst[nxt, :, :, cols] = jnp.where(live, h_new, h[:, cols].astype(f32)).astype(bf16).reshape(rows // GROUP, GROUP, bw)
            gst[j, :, :bw] = gi
            gst[j, :, bw:2 * bw] = gf
            gst[j, :, 2 * bw:3 * bw] = gg
            gst[j, :, 3 * bw:] = go

    for n in range(per * first_m, per * (first_m - 1) + FUNITS):
        wi_copy(n).start()
    for c in wr_copies(0):
        c.start()
    fill_lens(spans, lens)
    entry_wait(stage, n_stages)
    begin = [copy_of(h_start.at[0, :, pl.ds(i * hw, hw)], gst.at[i], g_sem.at[i]) for i in range(2)]
    begin.append(copy_of(c_start.at[0], cst.at[0], c_sem.at[0]))
    for c in begin:
        c.start()
    for c in begin:
        c.wait()
    for i in range(2):
        hst[0, :, :, i * hw:(i + 1) * hw] = gst[i].astype(bf16).reshape(rows // GROUP, GROUP, hw)
    c_copy(0, 0).start()
    h_copy(0, 0).start()

    def warm(v, _):
        m = v + first_m
        t, hf = (m + 2 * FWIN) // 2 - FWIN, lax.rem(m + 2 * FWIN, 2)
        turn_units(m)

        @pl.when(v == 1)
        def _():
            for c in wr_copies(1):
                c.start()

        @pl.when(hf == 0)
        def _():
            fetch_u(t + FWIN - 1)
            await_u(t + FWIN - 1)

        project(t, hf)
        return 0

    lax.fori_loop(0, -first_m, warm, 0)
    fetch_u(jnp.int32(FWIN - 1))

    def step(t, _):
        nxt = lax.rem(t + 1, 2)
        await_u(t + FWIN - 1)
        turn_units(2 * t)

        @pl.when(t == 0)
        def _():
            for c in wr_copies(0):
                c.wait()

        @pl.when(t >= 1)
        def _():
            release_u(t - 1)
            c_copy(nxt, t).wait()
            h_copy(nxt, t).wait()
            g_copy(t, 0).wait()

        @pl.when(jnp.logical_and(t >= 2, sends))
        def _():
            send(nxt, t).wait_send()

        project(t, 0)
        recur(t, 0)

        g_copy(t, 0).start()
        turn_units(2 * t + 1)
        fetch_u(t + FWIN)

        @pl.when(t == 0)
        def _():
            for c in wr_copies(1):
                c.wait()

        @pl.when(t >= 1)
        def _():
            g_copy(t, 1).wait()

        project(t, 1)
        recur(t, 1)

        g_copy(t, 1).start()
        c_copy(nxt, t + 1).start()
        h_copy(nxt, t + 1).start()

        @pl.when(sends)
        def _():
            @pl.when(t >= RING)
            def _():
                pl.semaphore_wait(credit, 1)

            send(nxt, t).start()

        return 0

    lax.fori_loop(0, steps, step, 0)
    release_u(jnp.int32(steps - 1))
    for hf in range(2):
        g_copy(0, hf).wait()
        c_copy(hf, 0).wait()
        h_copy(hf, 0).wait()

        @pl.when(sends)
        def _():
            send(hf, 0).wait_send()


def run_forward(n_stages, seq, w_in, w_rec, bias, h_start, c_start, spans):
    n_groups, steps, _, hidden = seq.shape
    rows = n_groups * GROUP
    bw = hidden // NB
    any_spec = pl.BlockSpec(memory_space=pl.ANY)
    vmem_spec = pl.BlockSpec(memory_space=pltpu.VMEM)
    dma = pltpu.SemaphoreType.DMA
    return pl.pallas_call(
        functools.partial(forward_kernel, n_stages, steps, rows, hidden),
        out_shape=(jax.ShapeDtypeStruct((n_groups, steps, GROUP, hidden), bf16),
                   jax.ShapeDtypeStruct((n_groups, steps + 1, GROUP, hidden), bf16),
                   jax.ShapeDtypeStruct((steps, NB, rows, 4 * bw), f32),
                   jax.ShapeDtypeStruct((steps + 1, rows, hidden), f32)),
        in_specs=[any_spec, any_spec, any_spec, vmem_spec, any_spec, any_spec, pl.BlockSpec(memory_space=pltpu.SMEM)],
        out_specs=(any_spec,) * 4,
        input_output_aliases={0: 0},
        scratch_shapes=[
            pltpu.VMEM((NB, hidden, 4 * bw), bf16),
            pltpu.VMEM((FUNITS, hidden, hidden // 2), bf16),
            pltpu.VMEM((RING, n_groups, GROUP, hidden), bf16),
            pltpu.VMEM((8, FWIN, rows, hidden // 2), f32),
            pltpu.VMEM((NB, rows, 4 * bw), f32),
            pltpu.VMEM((2, rows, hidden), f32),
            pltpu.VMEM((2, n_groups, GROUP, hidden), bf16),
            pltpu.VMEM((rows, bw), jnp.int32),
            dma((NB, 4)), dma((FUNITS,)), dma((1,)), dma((2,)), dma((2,)), dma((2,)), dma((2,)), dma((steps,)),
            dma((RING,)), pltpu.SemaphoreType.REGULAR,
        ],
        compiler_params=pltpu.CompilerParams(collective_id=0, has_side_effects=True, vmem_limit_bytes=VMEM_LIMIT),
        name="lstm_forward",
    )(seq, w_in, w_rec, bias, h_start, c_start, spans)


def backward_kernel(n_stages, steps, rows, hidden,
                    hseq, tseq, gates, cseq, win_t, wrec_t, spans,
                    dz_out, dh_out, dc_out, db_out, loss_out,
                    wt, wi, gin, cring, dbuf, ybuf, dzr, dh, dc, dbacc, lossacc, duacc, dust, lsend, lrecv, lens, scale,
                    wt_sem, wi_sem, g_sem, c_sem, d_sem, y_sem, dz_sem, out_sem, send_sem, recv_sem, lsend_sem, lrecv_sem, credit):
    bw = hidden // NB
    n_groups = rows // GROUP
    half = NB // 2
    hw = half * bw
    part = hidden // WIN
    ring = WIN
    pad = WIN - 1
    stage = lax.axis_index("stage")
    top = stage == n_stages - 1
    sends = stage > 0
    last = steps - 1
    halves = jnp.where(sends, 2 * (steps + pad), 2 * steps)
    entry_signal(stage, n_stages)

    def wt_copies(hf):
        return [copy_of(wrec_t.at[j], wt.at[j], wt_sem.at[j]) for j in range(hf * half, (hf + 1) * half)]

    def part_of(t):
        return lax.rem(t + WIN, WIN)

    def wi_copy(m, i):
        n = 2 * m + i
        t, hf = last - m // 2, lax.rem(m, 2)
        return copy_of(win_t.at[hf, part_of(t), pl.ds(i * hidden, hidden)], wi.at[lax.rem(n, UNITS)], wi_sem.at[lax.rem(n, UNITS)])

    def turn_units(m):
        for i in range(2):
            wi_copy(m, i).wait()

        @pl.when(m + 1 < halves)
        def _():
            wi_copy(m + 1, 1).start()

        @pl.when(m + 2 < halves)
        def _():
            wi_copy(m + 2, 0).start()

    def g_copy(t, hf):
        return copy_of(gates.at[t, pl.ds(hf * half, half)], gin.at[pl.ds(hf * half, half)], g_sem.at[hf])

    def c_copy(i):
        slot = lax.rem(i, 3)
        return copy_of(cseq.at[i], cring.at[slot], c_sem.at[slot])

    def d_slot(t):
        return lax.rem(t + RING, RING)

    def own_copies(t):
        return [copy_of(hseq.at[:, t + 1, :, pl.ds(q * part, part)], dbuf.at[d_slot(t), q], d_sem.at[q])
                for q in range(WIN)]

    def y_copy(t):
        return copy_of(tseq.at[:, t], ybuf.at[lax.rem(t, 2)], y_sem.at[0])

    def dz_copy(t):
        slot = lax.rem(t, ring)
        return copy_of(dzr.at[slot], dz_out.at[:, :, t], dz_sem.at[slot])

    def send(t, k):
        return pltpu.make_async_remote_copy(
            src_ref=dust.at[k], dst_ref=dbuf.at[d_slot(t + k), part_of(t)],
            send_sem=send_sem.at[k], recv_sem=recv_sem.at[k, t + pad],
            device_id={"stage": lax.rem(stage + n_stages - 1, n_stages)}, device_id_type=MESH)

    def each_send(t, act):
        @pl.when(t >= 0)
        def _():
            act(send(t, 0))

        @pl.when(t < last)
        def _():
            act(send(t, 1))

    def fetch_d(t):
        @pl.when(top)
        def _():
            for c in own_copies(t):
                c.start()
            y_copy(t).start()

    def await_d(t):
        @pl.when(top)
        def _():
            for c in own_copies(t):
                c.wait()
            y_copy(t).wait()

        @pl.when(jnp.logical_not(top))
        def _():
            send(t, 0).wait_recv()
            send(t - 1, 1).wait_recv()

    def release_d(t):
        @pl.when(jnp.logical_and(jnp.logical_not(top), t >= RING))
        def _():
            pl.semaphore_signal(credit, inc=1, device_id={"stage": lax.rem(stage + 1, n_stages)}, device_id_type=MESH)

    def input_grad(t, hf):
        d = jnp.concatenate([dzr[lax.rem(t + i + ring, ring), hf].reshape(rows, 2 * hidden) for i in range(WIN)], axis=0)
        n = 2 * (2 * (last - t) + hf)
        du = jnp.dot(d[:, :hidden], wi[lax.rem(n, UNITS)], preferred_element_type=f32)
        du += jnp.dot(d[:, hidden:], wi[lax.rem(n + 1, UNITS)], preferred_element_type=f32)
        if hf == 0:
            duacc[...] = du
        else:
            du = (du + duacc[...]).astype(bf16)
            for i in range(WIN):
                dust[i] = du[i * rows:(i + 1) * rows].reshape(n_groups, GROUP, part)

    def flat(x):
        return x.reshape(rows, x.shape[-1])

    def fold(x):
        return x.reshape(rows // 8, 8, x.shape[-1]).sum(axis=0)

    def recur(t, hf):
        cur, nxt = lax.rem(t, 2), lax.rem(t + 1, 2)
        slot = d_slot(t)
        live = lens[...] > t
        sc = scale[0:1, :]
        total = None
        for j in range(hf * half, (hf + 1) * half):
            cols = slice(j * bw, (j + 1) * bw)
            q, off = j * bw // part, j * bw % part
            gi, gf = gin[j, :, :bw], gin[j, :, bw:2 * bw]
            gg, go = gin[j, :, 2 * bw:3 * bw], gin[j, :, 3 * bw:]
            err = jnp.where(live, flat(dbuf[slot, q, :, :, off:off + bw]).astype(f32) - flat(ybuf[cur, :, :, cols]).astype(f32), 0.0)
            lossacc[:, cols] += fold(err * err)
            d_total = dh[cur, :, cols] + err * sc
            c_prev = cring[lax.rem(t, 3), :, cols]
            tanh_c = jnp.tanh(cring[lax.rem(t + 1, 3), :, cols])
            dc_old = dc[:, cols]
            d_c = dc_old + d_total * go * (1.0 - tanh_c * tanh_c)
            gates_d = (d_c * gg * gi * (1.0 - gi),
                     d_c * c_prev * gf * (1.0 - gf),
                     d_c * gi * (1.0 - gg * gg),
                     d_total * tanh_c * go * (1.0 - go))
            low = []
            for g in range(4):
                dz = jnp.where(live, gates_d[g], 0.0)
                dbacc[j, :, g * bw:(g + 1) * bw] += fold(dz)
                dz = dz.astype(bf16)
                at = g * hw + (j - hf * half) * bw
                dzr[lax.rem(t, ring), hf, :, :, at:at + bw] = dz.reshape(n_groups, GROUP, bw)
                low.append(dz)
            dc[:, cols] = jnp.where(live, d_c * gf, dc_old)
            keep = jnp.where(live, 0.0, d_total)
            if hf == 0:
                dh[nxt, :, cols] = keep
            else:
                dh[nxt, :, cols] += keep
            low = jnp.concatenate(low, axis=1)
            low = jnp.concatenate([low, low], axis=0)
            r = jnp.dot(low, wt[j], preferred_element_type=f32)
            total = r if total is None else total + r
        total = jnp.maximum(total[:rows], total[rows:])
        if hf == 0:
            dh[nxt, :, :hw] += total[:, :hw]
            dh[nxt, :, hw:] = total[:, hw:]
        else:
            dh[nxt] += total

    for c in wt_copies(0):
        c.start()
    g_copy(last, 0).start()
    c_copy(last + 1).start()
    c_copy(last).start()
    wi_copy(0, 0).start()
    wi_copy(0, 1).start()
    for c in wt_copies(1):
        c.start()
    wi_copy(1, 0).start()
    fill_lens(spans, lens)
    entry_wait(stage, n_stages)
    n_active = spans[0]
    for r in range(1, rows):
        n_active += spans[r]
    share = 1.0 / jnp.full(scale.shape, n_active.astype(f32))
    scale[...] = jnp.where(top, share, 1.0)
    dh[...] = jnp.zeros_like(dh)
    dc[...] = jnp.zeros_like(dc)
    dbacc[...] = jnp.zeros_like(dbacc)
    lossacc[...] = jnp.zeros_like(lossacc)
    ybuf[...] = jnp.zeros_like(ybuf)
    for i in range(ring):
        dzr[i] = jnp.zeros_like(dzr[i])

    fetch_d(last)
    c_copy(last + 1).wait()

    def step(v, _):
        t = last - v
        await_d(t)
        g_copy(t, 0).wait()
        c_copy(t).wait()

        @pl.when(v == 0)
        def _():
            for c in wt_copies(0):
                c.wait()

        @pl.when(v >= ring)
        def _():
            dz_copy(t + ring).wait()

        g_copy(t, 1).start()
        turn_units(2 * v)

        @pl.when(t >= 1)
        def _():
            c_copy(t - 1).start()

        recur(t, 0)
        input_grad(t, 0)

        g_copy(t, 1).wait()

        @pl.when(v == 0)
        def _():
            for c in wt_copies(1):
                c.wait()

        @pl.when(jnp.logical_and(v >= 1, sends))
        def _():
            each_send(t + 1, lambda c: c.wait_send())

        turn_units(2 * v + 1)

        @pl.when(t >= 1)
        def _():
            g_copy(t - 1, 0).start()
            fetch_d(t - 1)

        recur(t, 1)
        input_grad(t, 1)
        dz_copy(t).start()
        release_d(t)

        @pl.when(sends)
        def _():
            @pl.when(t <= last - RING)
            def _():
                pl.semaphore_wait(credit, 1)

            each_send(t, lambda c: c.start())

        return 0

    lax.fori_loop(0, steps, step, 0)

    for i in range(ring):
        dz_copy(i).wait()
    outs = [copy_of(dh.at[1], dh_out, out_sem.at[0]), copy_of(dc, dc_out, out_sem.at[1]),
            copy_of(dbacc, db_out, out_sem.at[2])]
    for c in outs:
        c.start()

    def tell():
        return pltpu.make_async_remote_copy(
            src_ref=lsend, dst_ref=lrecv, send_sem=lsend_sem.at[0], recv_sem=lrecv_sem.at[0],
            device_id={"stage": lax.rem(stage + n_stages - 1, n_stages)}, device_id_type=MESH)

    @pl.when(top)
    def _():
        lsend[...] = sum(lossacc[:, i * 128:(i + 1) * 128] for i in range(hidden // 128))

    @pl.when(sends)
    def _():
        def drain(v, _):
            t = -1 - v
            turn_units(2 * (last - t))
            input_grad(t, 0)
            turn_units(2 * (last - t) + 1)
            each_send(t + 1, lambda c: c.wait_send())
            input_grad(t, 1)
            each_send(t, lambda c: c.start())
            return 0

        lax.fori_loop(0, pad, drain, 0)
        each_send(jnp.int32(-pad), lambda c: c.wait_send())

    @pl.when(jnp.logical_not(top))
    def _():
        tell().wait_recv()
        lsend[...] = lrecv[...]

    for c in outs:
        c.wait()
    loss_copy = copy_of(lsend, loss_out, out_sem.at[3])
    loss_copy.start()
    loss_copy.wait()

    @pl.when(sends)
    def _():
        tell().start()
        tell().wait_send()


def run_backward(n_stages, hseq, tseq, gates, cseq, win_t, wrec_t, spans):
    n_groups, steps, _, hidden = tseq.shape
    rows = n_groups * GROUP
    bw = hidden // NB
    part = hidden // WIN
    any_spec = pl.BlockSpec(memory_space=pl.ANY)
    dma = pltpu.SemaphoreType.DMA
    return pl.pallas_call(
        functools.partial(backward_kernel, n_stages, steps, rows, hidden),
        out_shape=(jax.ShapeDtypeStruct((2, n_groups, steps, GROUP, 2 * hidden), bf16),
                   jax.ShapeDtypeStruct((rows, hidden), f32),
                   jax.ShapeDtypeStruct((rows, hidden), f32),
                   jax.ShapeDtypeStruct((NB, 8, 4 * bw), f32),
                   jax.ShapeDtypeStruct((8, 128), f32)),
        in_specs=[any_spec] * 6 + [pl.BlockSpec(memory_space=pltpu.SMEM)],
        out_specs=(any_spec,) * 5,
        scratch_shapes=[
            pltpu.VMEM((NB, 4 * bw, hidden), bf16),
            pltpu.VMEM((UNITS, hidden, part), bf16),
            pltpu.VMEM((NB, rows, 4 * bw), f32),
            pltpu.VMEM((3, rows, hidden), f32),
            pltpu.VMEM((RING, WIN, n_groups, GROUP, part), bf16),
            pltpu.VMEM((2, n_groups, GROUP, hidden), bf16),
            pltpu.VMEM((WIN, 2, n_groups, GROUP, 2 * hidden), bf16),
            pltpu.VMEM((2, rows, hidden), f32),
            pltpu.VMEM((rows, hidden), f32),
            pltpu.VMEM((NB, 8, 4 * bw), f32),
            pltpu.VMEM((8, hidden), f32),
            pltpu.VMEM((WIN * rows, part), f32),
            pltpu.VMEM((WIN, n_groups, GROUP, part), bf16),
            pltpu.VMEM((8, 128), f32),
            pltpu.VMEM((8, 128), f32),
            pltpu.VMEM((rows, bw), jnp.int32),
            pltpu.VMEM((8, bw), f32),
            dma((NB,)), dma((UNITS,)), dma((2,)), dma((3,)), dma((WIN,)), dma((1,)), dma((WIN,)), dma((4,)), dma((WIN,)),
            dma((WIN, steps + WIN - 1)), dma((1,)), dma((1,)), pltpu.SemaphoreType.REGULAR,
        ],
        compiler_params=pltpu.CompilerParams(collective_id=1, has_side_effects=True, vmem_limit_bytes=VMEM_LIMIT),
        name="lstm_backward",
    )(hseq, tseq, gates, cseq, win_t, wrec_t, spans)


def grads_kernel(steps, hidden, spans, useq, hseq, dz, dh, dc, db, sq,
                 g_in, g_rec, g_bias, dh_out, dc_out, loss_out,
                 xs, dzb, acc, state, x_sem, z_sem, o_sem, s_sem):
    n_groups = useq.shape[0]
    tile = dzb.shape[-1]
    n_tiles = 2 * dz.shape[-1] // tile
    per = hidden // 2 // tile
    bw = hidden // NB
    seen = [spans[i * GROUP] for i in range(n_groups)]
    first = [0]
    for i in range(n_groups):
        first.append(first[-1] + seen[i])
    total = first[-1]
    least = steps // 4
    sizes = []
    size = 1
    while size <= steps - least:
        sizes.insert(0, size)
        size *= 2

    def pieces(make, act):
        act(make(0, pl.ds(0, steps), pl.ds(0, steps)))
        for i in range(1, n_groups):
            act(make(i, pl.ds(0, least), pl.ds(first[i], least)))
            more = seen[i] - least
            for size in sizes:
                done = least + more // (2 * size) * (2 * size)

                @pl.when(more // size % 2 == 1)
                def _(i=i, size=size, done=done):
                    act(make(i, pl.ds(done, size), pl.ds(first[i] + done, size)))

    def load_x(w, act):
        src = useq if w == 0 else hseq
        pieces(lambda i, at, to: copy_of(src.at[i, at], xs.at[w, to], x_sem.at[w]), act)

    def load_z(n, slot, act):
        gate, hf = n // (2 * per), lax.rem(n, 2 * per) // per
        cols = pl.ds(pl.multiple_of((gate * per + lax.rem(n, per)) * tile, tile), tile)
        pieces(lambda i, at, to: copy_of(dz.at[hf, i, at, :, cols], dzb.at[slot, to], z_sem.at[slot]), act)

    def start(c):
        c.start()

    def wait(c):
        c.wait()

    def store(w, n, act):
        cols = pl.ds(pl.multiple_of(n * tile, tile), tile)

        @pl.when(w == 0)
        def _():
            act(copy_of(acc.at[0], g_in.at[0, :, cols], o_sem.at[0]))

        @pl.when(w == 1)
        def _():
            act(copy_of(acc.at[1], g_rec.at[0, :, cols], o_sem.at[1]))

    load_z(0, 0, start)
    load_x(0, start)
    load_x(1, start)
    for slot in range(2):
        xs[slot, pl.ds(total, GROUP)] = jnp.zeros((GROUP, GROUP, hidden), bf16)
        dzb[slot, pl.ds(total, GROUP)] = jnp.zeros((GROUP, GROUP, tile), bf16)
    states = [(copy_of(x, state.at[i], s_sem.at[i]), copy_of(state.at[i], y.at[0], s_sem.at[i]))
              for i, (x, y) in enumerate(((dh, dh_out), (dc, dc_out)))]
    for c, _ in states:
        c.start()
    for j in range(NB):
        for g in range(4):
            g_bias[0:1, g * hidden + j * bw:g * hidden + (j + 1) * bw] = jnp.sum(
                db[j, :, g * bw:(g + 1) * bw], axis=0, keepdims=True)
    n_active = spans[0]
    for r in range(1, n_groups * GROUP):
        n_active += spans[r]
    loss_out[...] = jnp.full((1, 1), jnp.sum(sq[...]) / (2.0 * n_active.astype(f32)))

    def product(w, slot, at, depth, begin):
        rhs = dzb[slot, pl.ds(at, depth)].reshape(depth * GROUP, tile)
        mc = min(512, hidden)
        for m in range(hidden // mc):
            lhs = xs[w, pl.ds(at, depth), :, m * mc:(m + 1) * mc].reshape(depth * GROUP, mc)
            r = lax.dot_general(lhs, rhs, (((0,), (0,)), ((), ())), preferred_element_type=f32)
            acc[w, m * mc:(m + 1) * mc] = r if begin else acc[w, m * mc:(m + 1) * mc] + r

    units = (total + 15) // 16

    def one_tile(v, _):
        n, w = v // 2, lax.rem(v, 2)
        slot = lax.rem(n, 2)

        @pl.when(w == 0)
        def _():
            @pl.when(n + 1 < n_tiles)
            def _():
                load_z(n + 1, 1 - slot, start)

            load_z(n, slot, wait)

        @pl.when(v == 0)
        def _():
            load_x(0, wait)

        @pl.when(v == 1)
        def _():
            load_x(1, wait)

        @pl.when(n >= 1)
        def _():
            store(w, n, wait)

        product(w, slot, 0, 128, True)

        def more(b, _):
            product(w, slot, 128 + b * 64, 64, False)
            return 0

        rest = jnp.maximum(units - 8, 0)
        lax.fori_loop(0, rest // 4, more, 0)

        @pl.when(rest // 2 % 2 == 1)
        def _():
            product(w, slot, 128 + rest // 4 * 64, 32, False)

        @pl.when(rest % 2 == 1)
        def _():
            product(w, slot, 128 + rest // 2 * 32, 16, False)

        store(w, n, start)
        return 0

    lax.fori_loop(0, 2 * n_tiles, one_tile, 0)
    for c, d in states:
        c.wait()
        d.start()
    store(0, 0, wait)
    store(1, 0, wait)
    for _, d in states:
        d.wait()


def run_grads(useq, hseq, dz, dh, dc, db, sq, spans):
    n_groups, steps, _, hidden = useq.shape
    rows = n_groups * GROUP
    any_spec = pl.BlockSpec(memory_space=pl.ANY)
    vmem_spec = pl.BlockSpec(memory_space=pltpu.VMEM)
    blocks = n_groups * steps + GROUP
    tile = 512
    dma = pltpu.SemaphoreType.DMA
    out = jax.ShapeDtypeStruct((1, hidden, 4 * hidden), f32)
    state = jax.ShapeDtypeStruct((1, rows, hidden), f32)
    return pl.pallas_call(
        functools.partial(grads_kernel, steps, hidden),
        out_shape=(out, out, jax.ShapeDtypeStruct((1, 4 * hidden), f32), state, state, jax.ShapeDtypeStruct((1, 1), f32)),
        in_specs=[pl.BlockSpec(memory_space=pltpu.SMEM)] + [any_spec] * 5 + [vmem_spec] * 2,
        out_specs=(any_spec, any_spec, vmem_spec, any_spec, any_spec, vmem_spec),
        scratch_shapes=[
            pltpu.VMEM((2, blocks, GROUP, hidden), bf16),
            pltpu.VMEM((2, blocks, GROUP, tile), bf16),
            pltpu.VMEM((2, hidden, tile), f32),
            pltpu.VMEM((2, rows, hidden), f32),
            dma((2,)), dma((2,)), dma((2,)), dma((2,)),
        ],
        compiler_params=pltpu.CompilerParams(vmem_limit_bytes=VMEM_LIMIT),
        name="lstm_weight_grads",
    )(spans, useq, hseq, dz, dh, dc, db, sq)


def solution(mesh):
    n_stages = mesh.shape["stage"]

    def local_program(inputs, targets, lengths, w_in, w_rec, gate_bias, h_init, c_init):
        useq, tseq, win_t, wrec_t = run_prepare(n_stages, inputs, targets, w_in, w_rec)
        useq, hseq, gates, cseq = run_forward(n_stages, useq, w_in, w_rec, gate_bias, h_init, c_init, lengths)
        win_t, wrec_t = run_late_turn(n_stages, w_in, w_rec, cseq, win_t, wrec_t)
        dz, dh0, dc0, db, sq = run_backward(n_stages, hseq, tseq, gates, cseq, win_t, wrec_t, lengths)
        grad_in, grad_rec, grad_bias, dh0, dc0, loss = run_grads(useq, hseq, dz, dh0, dc0, db, sq, lengths)
        return loss.reshape(1), grad_in, grad_rec, grad_bias, dh0, dc0

    row_spec = P("data", None, None)
    layer_spec = P("stage", None, None)
    state_spec = P("stage", "data", None)
    grad_spec = P(("data", "stage"), None, None)
    return jax.shard_map(local_program, mesh=mesh,
                         in_specs=(row_spec, row_spec, P("data"), layer_spec, layer_spec, P("stage", None), state_spec, state_spec),
                         out_specs=(P("data"), grad_spec, grad_spec, P(("data", "stage"), None), state_spec, state_spec),
                         check_vma=False)
```
